32 devices in a mesh: gx: 4 (over y, x), gy: 4 (over z), gz: 2 (over core).
Axes of the slice: x: 2, y: 2, z: 4, core: 2. Of those that a mesh axis runs over, the one named last changes fastest.
Arguments:
- charges: float32 [128, 256, 256], P('gx', 'gy', 'gz'), may hold values from -8 to 8
- kernel_taps: float32 [5, 3, 17], replicated, may hold values from 0.08 to 0.4
Outputs:
- potential: float32 [128, 256, 256], P('gx', 'gy', 'gz')
The draws below stay inside these ranges and needn't reach their ends.
All inputs are finite; a program needn't handle non-finite values.
Results may differ from the reference program's by a relative error of at most 0.00029.
Values sent between devices are 32-bit elements; how exact they have to be, the bound alone decides.
No kernel may reach another device: no remote copies, remote signals or barrier semaphores. Data moves between devices by JAX's collectives and lax.ppermute only.
A program may use at most 128 MiB of HBM per device.

```python
import math
import jax
import jax.numpy as jnp
from jax import lax

LEVELS = 5
TAPS = 17
NX = 128
NY = 256
NZ = 256


def block_levels(stream_key, shape, cuts, smallest, top_value):
    def one(dim, blocks):
        steps = jax.random.uniform(jax.random.fold_in(jax.random.fold_in(stream_key, 6), dim), (blocks,), jnp.float32, smallest / len(cuts), top_value / len(cuts))
        return jnp.repeat(jnp.exp(steps), shape[dim] // blocks).reshape((-1,) + (1,) * (len(shape) - dim - 1))

    loudness = one(*cuts[0])
    for cut in cuts[1:]:
        loudness = loudness * one(*cut)
    return loudness


def normal_values(stream_key, shape, width, most, shards=(), kind=jnp.bfloat16):
    factor_of = block_levels(stream_key, shape, shards, -0.22, 0.18) if shards else 1.0
    values = jax.random.normal(stream_key, shape, jnp.float32) * width * factor_of
    return jnp.minimum(jnp.maximum(values, -most), most).astype(kind)


def setup_inputs(seed: int = 0) -> dict:
    arg_keys = jax.random.split(jax.random.key(seed), 3)
    charges = normal_values(arg_keys[0], (NX, NY, NZ), 1.0, 8.0, ((0, 4), (1, 4), (2, 2)), jnp.float32)
    kernel_taps = jnp.clip(jnp.exp(jax.random.uniform(arg_keys[1], (LEVELS, 3, TAPS), jnp.float32, math.log(0.08), math.log(0.4))), 0.08, 0.4)
    return dict(charges=charges, kernel_taps=kernel_taps)


CUBIC = (-0.0625, 0.0, 0.5625, 1.0, 0.5625, 0.0, -0.0625)
PATTERNS = ("ij,jbc->ibc", "ij,ajc->aic", "ij,abj->abi")


def picks_matrix(weights, offsets):
    count = weights.shape[0]
    picks = (offsets[None, :, :] == jnp.arange(count, dtype=jnp.int32)[:, None, None]).astype(jnp.float32)
    return jnp.sum(weights.astype(jnp.float32)[:, None, None] * picks, axis=0)


def apply_axis(matrix, values, axis):
    return jnp.einsum(PATTERNS[axis], matrix, values, precision=lax.Precision.HIGHEST)


def stencil_padded(padded, taps_level):
    for axis in range(3):
        length = padded.shape[axis] - 16
        total = jnp.zeros(padded.shape[:axis] + (length,) + padded.shape[axis + 1:], jnp.float32)
        for offset in range(17):
            total = total + taps_level[axis, offset] * lax.slice_in_dim(padded, offset, offset + length, 1, axis)
        padded = total
    return padded


def restrict_padded(padded):
    cubic = jnp.array(CUBIC, jnp.float32)
    for axis in range(3):
        length = padded.shape[axis] - 6
        offsets = jnp.arange(length + 6, dtype=jnp.int32)[None, :] - 2 * jnp.arange(length // 2, dtype=jnp.int32)[:, None]
        padded = apply_axis(picks_matrix(cubic, offsets), padded, axis)
    return padded


def prolong_padded(padded):
    cubic = jnp.array(CUBIC, jnp.float32)
    for axis in range(3):
        length = padded.shape[axis] - 4
        offsets = 7 + jnp.arange(2 * length, dtype=jnp.int32)[:, None] - 2 * jnp.arange(length + 4, dtype=jnp.int32)[None, :]
        padded = apply_axis(picks_matrix(cubic, offsets), padded, axis)
    return padded


def reference(charges, kernel_taps):
    levels_charge = [charges]
    for level in range(1, LEVELS):
        levels_charge.append(restrict_padded(jnp.pad(levels_charge[-1], 3)))
    result = stencil_padded(jnp.pad(levels_charge[LEVELS - 1], 8), kernel_taps[LEVELS - 1])
    for level in range(LEVELS - 2, -1, -1):
        result = stencil_padded(jnp.pad(levels_charge[level], 8), kernel_taps[level]) + prolong_padded(jnp.pad(result, 2))
    return result
```

```python
import functools

import jax
import jax.numpy as jnp
import numpy as np
from jax import lax
from jax.experimental import pallas as pl
from jax.experimental.pallas import tpu as pltpu
from jax.sharding import PartitionSpec as P

LEVELS = 5
TAPS = 17
REACH = 8
LANES = 128
CUBIC = {-3: -0.0625, -1: 0.5625, 0: 1.0, 1: 0.5625, 3: -0.0625}
LOW = (0, 1, 2, 2, 2)
HIGH = (0, 2, 3, 3, 3)
F32 = jnp.float32
BF16 = jnp.bfloat16


def sizes(block):
    return [block // 2**l + LOW[l] + HIGH[l] for l in range(LEVELS)]


def pad8(n):
    return -(-n // 8) * 8


def pad16(n):
    return -(-n // 16) * 16


def restrictions(whole):
    composite, out = np.eye(whole), [np.eye(whole)]
    for _ in range(1, LEVELS):
        fine = composite.shape[0]
        step = np.zeros((fine // 2, fine))
        for i in range(fine // 2):
            for k, w in CUBIC.items():
                if 0 <= 2 * i + k < fine:
                    step[i, 2 * i + k] = w
        composite = step @ composite
        out.append(composite)
    return out


def rows_padded(block):
    n = sizes(block)
    return [block] + [max(16, pad8(n[l])) for l in range(1, LEVELS)]


def lane_offsets(block):
    n = sizes(block)
    return [0, 0, n[1], n[1] + n[2], n[1] + n[2]]


def split_rows_const(whole, count):
    block = whole // count
    full, n, padded = restrictions(whole), sizes(block), rows_padded(block)
    out = np.zeros((count, sum(padded[1:]), block), np.float32)
    for d in range(count):
        row0 = 0
        for l in range(1, LEVELS):
            for r in range(n[l]):
                g = d * (block >> l) - LOW[l] + r
                if 0 <= g < whole >> l:
                    out[d, row0 + r] = full[l][g, d * block : (d + 1) * block]
            row0 += padded[l]
    hi = out.astype(BF16)
    lo = (out - hi.astype(np.float32)).astype(BF16)
    return np.concatenate([hi, hi, lo], axis=2)


def prolong_entries(whole, count, d, l):
    block = whole // count
    n = sizes(block)
    for i in range(n[l]):
        g_out = d * (block >> l) - LOW[l] + i
        for j in range(n[l + 1]):
            g_in = d * (block >> (l + 1)) - LOW[l + 1] + j
            ok = 0 <= g_out < whole >> l and 0 <= g_in < whole >> (l + 1)
            if ok and g_out - 2 * g_in in CUBIC:
                yield i, j, CUBIC[g_out - 2 * g_in]


def prolong_rows_const(whole, count):
    padded = rows_padded(whole // count)
    out = np.zeros((count, sum(padded[:4]), 2 * padded[1]), np.float32)
    for d in range(count):
        row0 = 0
        for l in range(LEVELS - 1):
            for i, j, w in prolong_entries(whole, count, d, l):
                out[d, row0 + i, j] = w
                out[d, row0 + i, padded[l + 1] + j] = w
            row0 += padded[l]
    return out.astype(BF16)


def prolong_lanes_const(whole, count):
    off = lane_offsets(whole // count)
    out = np.zeros((count, LEVELS - 1, LANES, LANES), np.float32)
    for d in range(count):
        for l in range(LEVELS - 1):
            for i, j, w in prolong_entries(whole, count, d, l):
                out[d, l, off[l + 1] + j, off[l] + i] = w
    return out.astype(BF16)


def lanes_restrict_const(whole):
    full = restrictions(whole)
    out = np.concatenate([full[l].T for l in range(1, LEVELS)], axis=1)
    extra = -out.shape[1] % LANES
    return np.pad(out, ((0, 0), (0, extra))).astype(np.float32)


def toeplitz(taps_ref, row, g_in, g_out, mask):
    diff = g_in - g_out + REACH
    value = jnp.zeros(diff.shape, F32)
    for k in range(TAPS):
        value = jnp.where(diff == k, taps_ref[row, k], value)
    return jnp.where(mask, value, 0.0)


def iota(shape, axis):
    return lax.broadcasted_iota(jnp.int32, shape, axis)


def xor(a, b):
    return jnp.bitwise_xor(a, jnp.int32(b))


def halves(value):
    scaled = value * 65537.0
    hi = scaled - (scaled - value)
    return hi, value - hi


def mm(a, b):
    return jnp.dot(a, b, preferred_element_type=F32)


def setup_kernel(by, ny, nz, whole_y, taps_ref, idx_ref, rz_ref, w_ref, *rest):
    ty_refs, tb_ref = rest[:LEVELS], rest[LEVELS]
    whole_z = rz_ref.shape[0]
    bz = LANES
    dy, dz = idx_ref[1], idx_ref[2]
    n, off = sizes(bz), lane_offsets(bz)
    tb_ref[...] = jnp.zeros_like(tb_ref)
    row0 = 0
    for l in range(1, LEVELS):
        rows = whole_z >> l
        tile = 0 if l < LEVELS - 1 else 1
        col = iota((rows, LANES), 1)
        g_out = dz * (bz >> l) - LOW[l] + col - off[l]
        mask = (col >= off[l]) & (col < off[l] + n[l]) & (g_out >= 0) & (g_out < rows)
        tb_ref[row0 : row0 + rows, tile * LANES : (tile + 1) * LANES] = toeplitz(
            taps_ref, 3 * l + 2, iota((rows, LANES), 0), g_out, mask
        )
        row0 += rows
    order = [dz, 1 - dz] if nz == 2 else list(range(nz))
    for j, source in enumerate(order):
        start = pl.multiple_of(source * bz, bz) if nz == 2 else source * bz
        part = jnp.dot(
            rz_ref[pl.ds(start, bz), :],
            tb_ref[...],
            precision=lax.Precision.HIGHEST,
            preferred_element_type=F32,
        )
        g_in = source * bz + iota((bz, bz), 0)
        g_out = dz * bz + iota((bz, bz), 1)
        first = toeplitz(taps_ref, 2, g_in, g_out, g_out >= 0)
        hi, lo = halves(jnp.concatenate([first, part], axis=1))
        w_ref[j * bz : (j + 1) * bz] = hi.astype(BF16)
        w_ref[(nz + j) * bz : (nz + j + 1) * bz] = hi.astype(BF16)
        w_ref[(2 * nz + j) * bz : (2 * nz + j + 1) * bz] = lo.astype(BF16)
    even = (dy % 2) == 0
    sizes_y, padded = sizes(by), rows_padded(by)
    for l, ty_ref in enumerate(ty_refs):
        m, wide = ty_ref.shape
        k = wide // 3
        block = by >> l
        j = iota((m, wide), 1)
        j = jnp.where(j >= 2 * k, j - 2 * k, jnp.where(j >= k, j - k, j))
        if l < 3:
            window = 8 if l == 0 else 16
            right = (dy + 1) * block - LOW[l]
            left = (dy - 1) * block - LOW[l] + padded[l] - window
            base_a = jnp.where(even, right, left)
            base_b = jnp.where(even, left, right)
            own = dy * block - LOW[l] + j
            g_in = jnp.where(
                j < padded[l],
                own,
                jnp.where(
                    j < padded[l] + window,
                    base_a + j - padded[l],
                    base_b + j - padded[l] - window,
                ),
            )
        else:
            g_in = j
            for b in range(ny):
                source = xor(dy, b) if ny == 4 else b
                here = (j >= b * 16) & (j < (b + 1) * 16)
                g_in = jnp.where(here, source * block - LOW[l] + j - b * 16, g_in)
        i = iota((m, wide), 0)
        g_out = dy * block - LOW[l] + i
        mask = (i < sizes_y[l]) & (g_out >= 0) & (g_out < whole_y >> l)
        hi, lo = halves(toeplitz(taps_ref, 3 * l + 1, g_in, g_out, mask))
        ty_ref[...] = jnp.where(iota((m, wide), 1) < 2 * k, hi, lo).astype(BF16)


def masked(value, index, block, place):
    if 0 <= index < block:
        return value
    cell = place[0] * block + index
    inside = (cell >= 0) & (cell < place[1] * block)
    return value * jnp.where(inside, 1.0, 0.0).astype(F32)


def restrict_planes(src, dst, level, block_out, place):
    lo_in, count_in = LOW[level - 1], src.shape[0]
    for r in range(dst.shape[0]):
        i = r - LOW[level]
        total = None
        for k, w in CUBIC.items():
            p = 2 * i + k + lo_in
            if 0 <= p < count_in:
                term = src[p] if w == 1.0 else src[p] * w
                total = term if total is None else total + term
        dst[r] = masked(total, i, block_out, place)


def stacked(value):
    hi, lo = halves(value)
    return jnp.concatenate([hi, lo, hi], axis=0).astype(BF16)


def z_kernel(nx, nz, idx_ref, *refs):
    src = refs[: (2 if nz == 2 else 1)]
    w_ref, sy_ref = refs[len(src) : len(src) + 2]
    g0_ref, ma_ref, mb_ref, y1_ref, y2_ref, y34_ref = refs[len(src) + 2 : len(src) + 8]
    g1, g2, x1, x2, x3, t1, t2, t3, x4 = refs[len(src) + 8 :]
    bx, by, bz = g0_ref.shape
    dx, dy = idx_ref[0], idx_ref[1]
    chunk = 4

    def step(c, carry):
        planes = pl.ds(c * chunk, chunk)
        if nz == 2:
            blocks = [s[planes].reshape(chunk * by, bz) for s in src]
        else:
            blocks = [src[0][s, planes].reshape(chunk * by, bz) for s in range(nz)]
        his, los = zip(*[halves(b) for b in blocks])
        lhs = jnp.concatenate([h.astype(BF16) for h in his + los + his], axis=1)
        acc = mm(lhs, w_ref[...])
        g0_ref[planes] = acc[:, :LANES].reshape(chunk, by, bz)
        g1[planes] = acc[:, LANES : 2 * LANES].reshape(chunk, by, bz)
        g2[planes] = acc[:, 2 * LANES :].reshape(chunk, by, bz)
        return carry

    lax.fori_loop(0, bx // chunk, step, 0)
    place = (dx, nx)
    for source, first, second, third, fourth in (
        (g1, x1, x2, x3, None),
        (g2, t1, t2, t3, x4),
    ):
        restrict_planes(source, first, 1, bx >> 1, place)
        restrict_planes(first, second, 2, bx >> 2, place)
        restrict_planes(second, third, 3, bx >> 3, place)
        if fourth is not None:
            restrict_planes(third, fourth, 4, bx >> 4, place)
    padded = rows_padded(by)
    n3 = x3.shape[0]
    row0 = 0
    for l, (source, target, first) in enumerate(
        ((x1, y1_ref, 0), (x2, y2_ref, 0), (x3, y34_ref, 0), (x4, y34_ref, n3)), 1
    ):
        sy = sy_ref[row0 : row0 + padded[l], :]
        for p in range(source.shape[0]):
            target[first + p] = mm(sy, stacked(source[p]))
        row0 += padded[l]
    off = lane_offsets(bz)
    lane = iota((16, LANES), 1)
    even = (dy % 2) == 0
    for m_ref, rightward in ((ma_ref, even), (mb_ref, jnp.logical_not(even))):
        start0 = pl.multiple_of(jnp.where(rightward, by - 8, 0), 8)
        start1 = pl.multiple_of(jnp.where(rightward, padded[1] - 16, 0), 8)
        start2 = pl.multiple_of(jnp.where(rightward, padded[2] - 16, 0), 8)
        m_ref[0:bx] = g0_ref[:, pl.ds(start0, 8), :]
        for p in range(y1_ref.shape[0]):
            value = y1_ref[p, pl.ds(start1, 16), :]
            if p < y2_ref.shape[0]:
                value = jnp.where(lane < off[2], value, y2_ref[p, pl.ds(start2, 16), :])
            if p < y34_ref.shape[0]:
                value = jnp.where(lane < off[3], value, y34_ref[p])
            m_ref[bx + 2 * p : bx + 2 * p + 2] = value.reshape(2, 8, LANES)


def pack_y_kernel(off3, bx, own_ref, got_ref, out_ref):
    lane = iota((16, LANES), 1)
    for p in range(out_ref.shape[0]):
        got = got_ref[bx + 2 * p : bx + 2 * p + 2].reshape(16, LANES)
        out_ref[p] = jnp.where(lane >= off3, own_ref[p], pltpu.roll(got, LANES - 32, 1))


def y_kernel(ny, idx_ref, g0_ref, ra_ref, rb_ref, y1_ref, y2_ref, y34_ref, c_ref, *refs):
    ty0, ty1, ty2, ty3, ty4, h0_ref, ma_ref, mb_ref, h1_ref, h2_ref, h3_ref, h4_ref = refs
    bx, by, bz = g0_ref.shape
    dx = idx_ref[0]
    off = lane_offsets(bz)

    def plane0(p, carry):
        value = jnp.concatenate([g0_ref[p], ra_ref[p], rb_ref[p]], axis=0)
        h0_ref[p] = mm(ty0[...], stacked(value))
        return carry

    lax.fori_loop(0, bx, plane0, 0, unroll=4)

    def got(ref, p):
        return ref[bx + 2 * p : bx + 2 * p + 2].reshape(16, LANES)

    for own, ty, h in ((y1_ref, ty1, h1_ref), (y2_ref, ty2, h2_ref)):
        for p in range(h.shape[0]):
            value = jnp.concatenate([own[p], got(ra_ref, p), got(rb_ref, p)], axis=0)
            h[p] = mm(ty[...], stacked(value))
    n3 = h3_ref.shape[0]
    for p in range(y34_ref.shape[0]):
        if ny == 4:
            far = c_ref[p]
            parts = [y34_ref[p], got(ra_ref, p), far, pltpu.roll(far, 32, 1)]
        else:
            parts = [c_ref[s, p] for s in range(ny)]
        value = stacked(jnp.concatenate(parts, axis=0))
        if p < n3:
            h3_ref[p] = mm(ty3[...], value)
        else:
            h4_ref[p - n3] = mm(ty4[...], value)

    even = (dx % 2) == 0
    tiles = by // 8
    n2, rows1 = h2_ref.shape[0], h1_ref.shape[1]
    n1 = REACH + 3
    lane = iota((rows1, LANES), 1)
    for m_ref, rightward, coarse in ((ma_ref, even, True), (mb_ref, jnp.logical_not(even), False)):
        start0 = jnp.where(rightward, bx - REACH, 0)
        start1 = jnp.where(rightward, (bx >> 1) - REACH, 0)
        for p in range(REACH):
            m_ref[p * tiles : (p + 1) * tiles] = h0_ref[start0 + p].reshape(tiles, 8, LANES)
        base, each = REACH * tiles, rows1 // 8
        for p in range(n2 if coarse else n1):
            if coarse:
                zero = jnp.zeros((16, LANES), F32)
                t2 = jnp.concatenate(
                    [h2_ref[p], jnp.zeros((rows1 - h2_ref.shape[1], LANES), F32)], axis=0
                )
                t34 = jnp.concatenate(
                    [
                        h3_ref[p] if p < n3 else zero,
                        h4_ref[p] if p < h4_ref.shape[0] else zero,
                        jnp.zeros((rows1 - 32, LANES), F32),
                    ],
                    axis=0,
                )
                value = jnp.where(lane < off[3], t2, t34)
                if p < n1:
                    value = jnp.where(lane < off[2], h1_ref[start1 + p], value)
            else:
                value = h1_ref[start1 + p]
            m_ref[base + p * each : base + (p + 1) * each] = value.reshape(each, 8, LANES)


def pack_x_kernel(base, each, own_ref, got_ref, out_ref):
    lane = iota((4, 8, LANES), 2)
    for p in range(out_ref.shape[0] // 4):
        rows = slice(base + p * each, base + p * each + 4)
        got = pltpu.roll(got_ref[rows].reshape(32, LANES), 64, 1).reshape(4, 8, LANES)
        out_ref[4 * p : 4 * p + 4] = jnp.where(lane >= 64, own_ref[rows], got)


def x_kernel(nx, taps_ref, idx_ref, h0, h1, h2, h3, h4, ra, rb, rc, py_ref, pz_ref, out_ref, *scratch):
    ext0, e1, e2, e3, e4, f1, f2, f3, f4, s1, s2 = scratch
    bx, by, bz = h0.shape
    dx = idx_ref[0]
    even = (dx % 2) == 0
    place = (dx, nx)
    tiles, padded = by // 8, rows_padded(by)
    each = h1.shape[1] // 8
    base = REACH * tiles
    sa = jnp.where(even, bx + REACH, 0)
    sb = jnp.where(even, 0, bx + REACH)
    ext0[REACH : REACH + bx] = h0[...]
    for p in range(REACH):
        ext0[sa + p] = ra[p * tiles : (p + 1) * tiles].reshape(by, LANES)
        ext0[sb + p] = rb[p * tiles : (p + 1) * tiles].reshape(by, LANES)

    def rows0(t, carry):
        at = pl.ds(pl.multiple_of(t * 8, 8), 8)
        for i in range(bx):
            total = ext0[i, at, :] * taps_ref[0, 0]
            for k in range(1, TAPS):
                total = total + ext0[i + k, at, :] * taps_ref[0, k]
            out_ref[i, at, :] = total
        return carry

    lax.fori_loop(0, tiles, rows0, 0)

    n1 = REACH + 3
    high = (bx >> 1) + REACH
    e1[...] = jnp.zeros_like(e1)
    e1[REACH : REACH + h1.shape[0]] = h1[...]
    sa = jnp.where(even, high, 0)
    sb = jnp.where(even, 0, high)
    for p in range(n1):
        rows = slice(base + p * each, base + (p + 1) * each)
        e1[sa + p] = e1[sa + p] + ra[rows].reshape(each * 8, LANES)
        e1[sb + p] = e1[sb + p] + rb[rows].reshape(each * 8, LANES)
    for e, h, row, l in ((e2, h2, 0, 2), (e3, h3, 0, 3), (e4, h4, 16, 4)):
        e[...] = jnp.zeros_like(e)
        rows = h.shape[1]
        t0, t1 = row // 8, (row + rows) // 8
        for b in range(nx):
            source = xor(dx, b) if nx == 4 else b
            at = source * (bx >> l) - LOW[l] + 12
            for p in range(h.shape[0]):
                if nx != 4:
                    value = rc[b, p * each + t0 : p * each + t1].reshape(rows, LANES)
                elif b == 0:
                    value = h[p]
                elif b == 1:
                    value = ra[base + p * each + t0 : base + p * each + t1].reshape(rows, LANES)
                else:
                    value = rc[4 * p + t0 : 4 * p + t1].reshape(rows, LANES)
                    if b == 3:
                        value = pltpu.roll(value, 64, 1)
                e[at + p] = e[at + p] + value
    for e, f, l in ((e1, f1, 1), (e2, f2, 2), (e3, f3, 3), (e4, f4, 4)):
        start = 0 if l == 1 else dx * (bx >> l) - LOW[l] - REACH + 12
        for r in range(f.shape[0]):
            total = e[start + r] * taps_ref[3 * l, 0]
            for k in range(1, TAPS):
                total = total + e[start + r + k] * taps_ref[3 * l, k]
            f[r] = masked(total, r - LOW[l], bx >> l, place)
    row0 = [sum(padded[:l]) for l in range(LEVELS)]
    for l, f, target in ((3, f4, f3), (2, f3, f2), (1, f2, f1), (0, f1, out_ref)):
        rows, k = padded[l], 2 * padded[l + 1]
        matrix = py_ref[row0[l] : row0[l] + rows, :k]
        count = f.shape[0]
        for p in range(count):
            hi, lo = halves(f[p])
            s1[p, 0:rows] = mm(matrix, jnp.concatenate([hi, lo], axis=0).astype(BF16))
        pz = jnp.concatenate([pz_ref[l], pz_ref[l]], axis=0)
        for p in range(count):
            hi, lo = halves(s1[p, 0:rows])
            s2[p, 0:rows] = mm(jnp.concatenate([hi, lo], axis=1).astype(BF16), pz)
        for r in range(target.shape[0]):
            j = r - LOW[l]
            total = None
            for kk, w in CUBIC.items():
                if (j - kk) % 2 == 0:
                    p = (j - kk) // 2 + LOW[l + 1]
                    if 0 <= p < count:
                        value = s2[p, 0:rows]
                        term = value if w == 1.0 else value * w
                        total = term if total is None else total + term
            target[r] = target[r] + masked(total, j, bx >> l, place)


def call(kernel, out_shape, args, n_smem, scratch=()):
    vmem, smem = pl.BlockSpec(memory_space=pltpu.VMEM), pl.BlockSpec(memory_space=pltpu.SMEM)
    many = isinstance(out_shape, (tuple, list))
    return pl.pallas_call(
        kernel,
        out_shape=out_shape,
        in_specs=[smem] * n_smem + [vmem] * (len(args) - n_smem),
        out_specs=[vmem] * len(out_shape) if many else vmem,
        scratch_shapes=scratch,
        compiler_params=pltpu.CompilerParams(vmem_limit_bytes=48 * 2**20),
    )(*args)


def swaps(count, distance, first=0):
    pairs = []
    for i in range(first, count):
        j = i + distance
        if j < count and (distance > 1 and (i ^ distance) == j or distance == 1 and (i - first) % 2 == 0):
            pairs += [(i, j), (j, i)]
    return pairs


def per_device(charges, kernel_taps):
    nx, ny, nz = (lax.axis_size(a) for a in ("gx", "gy", "gz"))
    bx, by, bz = charges.shape
    assert bz == LANES and nx % 2 == 0 and ny % 2 == 0
    xs, ys, padded, off = sizes(bx), sizes(by), rows_padded(by), lane_offsets(bz)
    dx, dy, dz = (lax.axis_index(a) for a in ("gx", "gy", "gz"))
    taps = kernel_taps.reshape(3 * LEVELS, TAPS)
    idx = jnp.stack([dx, dy, dz]).astype(jnp.int32)

    def shape(*dims, dtype=F32):
        return jax.ShapeDtypeStruct(dims, dtype)

    if nz == 2:
        sources = (charges, lax.ppermute(charges, "gz", swaps(2, 1)))
    else:
        sources = (lax.all_gather(charges, "gz"),)
    rz = jnp.asarray(lanes_restrict_const(nz * bz))
    in_y = [padded[0] + 16, padded[1] + 32, padded[2] + 32, 16 * ny, 16 * ny]
    w, *ty = call(
        functools.partial(setup_kernel, by, ny, nz, ny * by),
        [shape(3 * nz * bz, 3 * LANES, dtype=BF16)]
        + [shape(padded[l], 3 * in_y[l], dtype=BF16) for l in range(LEVELS)],
        (taps, idx, rz),
        2,
        [pltpu.VMEM((rz.shape[1], 2 * LANES), F32)],
    )
    sy = jnp.asarray(split_rows_const(ny * by, ny))[dy]
    n34 = xs[3] + xs[4]
    message = shape(bx + 2 * xs[1], 8, LANES)
    plane = lambda n: pltpu.VMEM((n, by, bz), F32)
    g0, ma, mb, y1, y2, y34 = call(
        functools.partial(z_kernel, nx, nz),
        [
            shape(bx, by, bz),
            message,
            message,
            shape(xs[1], padded[1], LANES),
            shape(xs[2], padded[2], LANES),
            shape(n34, 16, LANES),
        ],
        (idx, *sources, w, sy),
        1,
        [plane(bx), plane(bx), plane(xs[1]), plane(xs[2]), plane(xs[3])]
        + [plane(xs[1]), plane(xs[2]), plane(xs[3]), plane(xs[4])],
    )
    ra = lax.ppermute(ma, "gy", swaps(ny, 1))
    rb = lax.ppermute(mb, "gy", swaps(ny, 1, 1))
    if ny == 4:
        packed = call(
            functools.partial(pack_y_kernel, off[3], bx), shape(n34, 16, LANES), (y34, ra), 0
        )
        rc = lax.ppermute(packed, "gy", swaps(ny, 2))
    else:
        rc = lax.all_gather(y34, "gy")
    tiles, each = by // 8, padded[1] // 8
    h0, ma, mb, h1, h2, h3, h4 = call(
        functools.partial(y_kernel, ny),
        [
            shape(bx, by, bz),
            shape(REACH * tiles + xs[2] * each, 8, LANES),
            shape(REACH * tiles + (REACH + 3) * each, 8, LANES),
        ]
        + [shape(xs[l], padded[l], LANES) for l in range(1, LEVELS)],
        (idx, g0, ra, rb, y1, y2, y34, rc, *ty),
        1,
    )
    ra = lax.ppermute(ma, "gx", swaps(nx, 1))
    rb = lax.ppermute(mb, "gx", swaps(nx, 1, 1))
    if nx == 4:
        packed = call(
            functools.partial(pack_x_kernel, REACH * tiles, each),
            shape(4 * xs[2], 8, LANES),
            (ma, ra),
            0,
        )
        rc = lax.ppermute(packed, "gx", swaps(nx, 2))
    else:
        rc = lax.all_gather(ma[REACH * tiles :], "gx")
    py = jnp.asarray(prolong_rows_const(ny * by, ny))[dy]
    pz = jnp.asarray(prolong_lanes_const(nz * bz, nz))[dz]
    buf = lambda n, rows: pltpu.VMEM((n, rows, LANES), F32)
    return call(
        functools.partial(x_kernel, nx),
        shape(bx, by, bz),
        (taps, idx, h0, h1, h2, h3, h4, ra, rb, rc, py, pz),
        2,
        [buf(bx + 2 * REACH, by), buf(xs[1] + 2 * REACH, padded[1])]
        + [buf((nx * bx >> l) + 24, padded[l]) for l in range(2, LEVELS)]
        + [buf(xs[l], padded[l]) for l in range(1, LEVELS)]
        + [buf(xs[1], by), buf(xs[1], by)],
    )


def solution(mesh):
    in_specs = (P("gx", "gy", "gz"), P())
    out_specs = P("gx", "gy", "gz")
    return jax.shard_map(
        per_device, mesh=mesh, in_specs=in_specs, out_specs=out_specs, check_vma=False
    )
```

```python
import functools

import jax
import jax.numpy as jnp
import numpy as np
from jax import lax
from jax.experimental import pallas as pl
from jax.experimental.pallas import tpu as pltpu
from jax.sharding import PartitionSpec as P

LEVELS = 5
TAPS = 17
REACH = 8
LANES = 128
CUBIC = {-3: -0.0625, -1: 0.5625, 0: 1.0, 1: 0.5625, 3: -0.0625}
LOW = (0, 1, 2, 2, 2)
HIGH = (0, 2, 3, 3, 3)
F32 = jnp.float32
BF16 = jnp.bfloat16
GATHER = (0, 1, 3, 2)


def sizes(block):
    return [block // 2**l + LOW[l] + HIGH[l] for l in range(LEVELS)]


def pad8(n):
    return -(-n // 8) * 8


def pad16(n):
    return -(-n // 16) * 16


def restrictions(whole):
    composite, out = np.eye(whole), [np.eye(whole)]
    for _ in range(1, LEVELS):
        fine = composite.shape[0]
        step = np.zeros((fine // 2, fine))
        for i in range(fine // 2):
            for k, w in CUBIC.items():
                if 0 <= 2 * i + k < fine:
                    step[i, 2 * i + k] = w
        composite = step @ composite
        out.append(composite)
    return out


def rows_padded(block):
    n = sizes(block)
    return [block] + [max(16, pad8(n[l])) for l in range(1, LEVELS)]


def lane_offsets(block):
    n = sizes(block)
    return [0, 0, n[1], n[1] + n[2], n[1] + n[2]]


def split_rows_const(whole, count):
    block = whole // count
    full, n, padded = restrictions(whole), sizes(block), rows_padded(block)
    out = np.zeros((count, sum(padded[1:]), block), np.float32)
    for d in range(count):
        row0 = 0
        for l in range(1, LEVELS):
            for r in range(n[l]):
                g = d * (block >> l) - LOW[l] + r
                if 0 <= g < whole >> l:
                    out[d, row0 + r] = full[l][g, d * block : (d + 1) * block]
            row0 += padded[l]
    hi = out.astype(BF16)
    lo = (out - hi.astype(np.float32)).astype(BF16)
    return np.concatenate([hi, hi, lo], axis=2)


def prolong_entries(whole, count, d, l):
    block = whole // count
    n = sizes(block)
    for i in range(n[l]):
        g_out = d * (block >> l) - LOW[l] + i
        for j in range(n[l + 1]):
            g_in = d * (block >> (l + 1)) - LOW[l + 1] + j
            ok = 0 <= g_out < whole >> l and 0 <= g_in < whole >> (l + 1)
            if ok and g_out - 2 * g_in in CUBIC:
                yield i, j, CUBIC[g_out - 2 * g_in]


def prolong_rows_const(whole, count):
    padded = rows_padded(whole // count)
    out = np.zeros((count, sum(padded[:4]), 2 * padded[1]), np.float32)
    for d in range(count):
        row0 = 0
        for l in range(LEVELS - 1):
            for i, j, w in prolong_entries(whole, count, d, l):
                out[d, row0 + i, j] = w
                out[d, row0 + i, padded[l + 1] + j] = w
            row0 += padded[l]
    return out.astype(BF16)


def prolong_lanes_const(whole, count):
    off = lane_offsets(whole // count)
    out = np.zeros((count, LEVELS - 1, LANES, LANES), np.float32)
    for d in range(count):
        for l in range(LEVELS - 1):
            for i, j, w in prolong_entries(whole, count, d, l):
                out[d, l, off[l + 1] + j, off[l] + i] = w
    return out.astype(BF16)


def lanes_restrict_const(whole):
    full = restrictions(whole)
    out = np.concatenate([full[l].T for l in range(1, LEVELS)], axis=1)
    extra = -out.shape[1] % LANES
    return np.pad(out, ((0, 0), (0, extra))).astype(np.float32)


def toeplitz(taps_ref, row, g_in, g_out, mask):
    diff = g_in - g_out + REACH
    value = jnp.zeros(diff.shape, F32)
    for k in range(TAPS):
        value = jnp.where(diff == k, taps_ref[row, k], value)
    return jnp.where(mask, value, 0.0)


def iota(shape, axis):
    return lax.broadcasted_iota(jnp.int32, shape, axis)


def xor(a, b):
    return jnp.bitwise_xor(a, jnp.int32(b))


def halves(value):
    scaled = value * 65537.0
    hi = scaled - (scaled - value)
    return hi, value - hi


def mm(a, b):
    return jnp.dot(a, b, preferred_element_type=F32)


def setup_kernel(
    by, ny, nz, whole_y, taps_ref, idx_ref, q_hbm, rz_ref, q_ref, w_ref, ty0_ref, tyh_ref, *rest
):
    ty_refs, tb_ref, sem = rest[:4], rest[4], rest[5]
    copy = pltpu.make_async_copy(q_hbm, q_ref, sem)
    copy.start()
    whole_z = rz_ref.shape[0]
    bz = LANES
    dy, dz = idx_ref[1], idx_ref[2]
    n, off = sizes(bz), lane_offsets(bz)
    tb_ref[...] = jnp.zeros_like(tb_ref)
    row0 = 0
    for l in range(1, LEVELS):
        rows = whole_z >> l
        tile = 0 if l < LEVELS - 1 else 1
        col = iota((rows, LANES), 1)
        g_out = dz * (bz >> l) - LOW[l] + col - off[l]
        mask = (col >= off[l]) & (col < off[l] + n[l]) & (g_out >= 0) & (g_out < rows)
        tb_ref[row0 : row0 + rows, tile * LANES : (tile + 1) * LANES] = toeplitz(
            taps_ref, 3 * l + 2, iota((rows, LANES), 0), g_out, mask
        )
        row0 += rows
    order = [dz, 1 - dz] if nz == 2 else list(range(nz))
    for j, source in enumerate(order):
        start = pl.multiple_of(source * bz, bz) if nz == 2 else source * bz
        part = jnp.dot(
            rz_ref[pl.ds(start, bz), :],
            tb_ref[...],
            precision=lax.Precision.HIGHEST,
            preferred_element_type=F32,
        )
        g_in = source * bz + iota((bz, bz), 0)
        g_out = dz * bz + iota((bz, bz), 1)
        first = toeplitz(taps_ref, 2, g_in, g_out, g_out >= 0)
        hi, lo = halves(jnp.concatenate([first, part], axis=1))
        w_ref[j * bz : (j + 1) * bz] = hi.astype(BF16)
        w_ref[(nz + j) * bz : (nz + j + 1) * bz] = hi.astype(BF16)
        w_ref[(2 * nz + j) * bz : (2 * nz + j + 1) * bz] = lo.astype(BF16)
    even = (dy % 2) == 0
    sizes_y, padded = sizes(by), rows_padded(by)

    def column(shape):
        k = shape[1] // 3
        j = iota(shape, 1)
        return k, jnp.where(j >= 2 * k, j - 2 * k, jnp.where(j >= k, j - k, j))

    def store(ref, k, value):
        hi, lo = halves(value)
        ref[...] = jnp.where(iota(ref.shape, 1) < 2 * k, hi, lo).astype(BF16)

    def windows(l, j, own, window):
        block = by >> l
        right = (dy + 1) * block - LOW[l]
        left = (dy - 1) * block - LOW[l] + padded[l] - window
        base_a = jnp.where(even, right, left)
        base_b = jnp.where(even, left, right)
        second = jnp.where(j < own + window, base_a + j - own, base_b + j - own - window)
        return jnp.where(j < own, dy * block - LOW[l] + j, second)

    k, j = column(ty0_ref.shape)
    i = iota(ty0_ref.shape, 0)
    store(ty0_ref, k, toeplitz(taps_ref, 1, j, i, i >= 0))
    k, j = column(tyh_ref.shape)
    i = iota(tyh_ref.shape, 0)
    i = dy * by + jnp.where(i < 8, i, i + by - 16)
    g_in = windows(0, j, 0, 8)
    store(tyh_ref, k, toeplitz(taps_ref, 1, g_in, i, (g_in >= 0) & (g_in < whole_y)))
    for l, ty_ref in enumerate(ty_refs, 1):
        block = by >> l
        k, j = column(ty_ref.shape)
        if l < 3:
            g_in = windows(l, j, padded[l], 16)
        else:
            g_in = j
            for b in range(ny):
                source = xor(dy, GATHER[b]) if ny == 4 else b
                here = (j >= b * 16) & (j < (b + 1) * 16)
                g_in = jnp.where(here, source * block - LOW[l] + j - b * 16, g_in)
        i = iota(ty_ref.shape, 0)
        g_out = dy * block - LOW[l] + i
        mask = (i < sizes_y[l]) & (g_out >= 0) & (g_out < whole_y >> l)
        mask = mask & (g_in >= 0) & (g_in < whole_y >> l)
        store(ty_ref, k, toeplitz(taps_ref, 3 * l + 1, g_in, g_out, mask))
    copy.wait()


def masked(value, index, block, place):
    if 0 <= index < block:
        return value
    cell = place[0] * block + index
    inside = (cell >= 0) & (cell < place[1] * block)
    return value * jnp.where(inside, 1.0, 0.0).astype(F32)


def restrict_planes(src, dst, level, block_out, place):
    lo_in, count_in = LOW[level - 1], src.shape[0]
    for r in range(dst.shape[0]):
        i = r - LOW[level]
        total = None
        for k, w in CUBIC.items():
            p = 2 * i + k + lo_in
            if 0 <= p < count_in:
                term = src[p] if w == 1.0 else src[p] * w
                total = term if total is None else total + term
        dst[r] = masked(total, i, block_out, place)


def stacked(value):
    hi, lo = halves(value)
    return jnp.concatenate([hi, lo, hi], axis=0).astype(BF16)


def z_kernel(nx, nz, idx_ref, *refs):
    src = refs[: (2 if nz == 2 else 1)]
    w_ref, sy_ref, g0_ref, xa_ref, xb_ref, ma_ref, mb_ref, mc_ref, y1_ref, y2_ref, y34_ref = refs[
        len(src) : len(src) + 11
    ]
    g1, g2, x1, x2, x3, t1, t2, t3, x4 = refs[len(src) + 11 :]
    bx, by, bz = g0_ref.shape
    dx, dy = idx_ref[0], idx_ref[1]
    chunk = 4

    def step(c, carry):
        planes = pl.ds(c * chunk, chunk)
        if nz == 2:
            blocks = [s[planes].reshape(chunk * by, bz) for s in src]
        else:
            blocks = [src[0][s, planes].reshape(chunk * by, bz) for s in range(nz)]
        his, los = zip(*[halves(b) for b in blocks])
        lhs = jnp.concatenate([h.astype(BF16) for h in his + los + his], axis=1)
        acc = mm(lhs, w_ref[...])
        g0_ref[planes] = acc[:, :LANES].reshape(chunk, by, bz)
        g1[planes] = acc[:, LANES : 2 * LANES].reshape(chunk, by, bz)
        g2[planes] = acc[:, 2 * LANES :].reshape(chunk, by, bz)
        return carry

    lax.fori_loop(0, bx // chunk, step, 0)
    even = (dx % 2) == 0
    xa_ref[...] = g0_ref[pl.ds(jnp.where(even, bx - REACH, 0), REACH)]
    xb_ref[...] = g0_ref[pl.ds(jnp.where(even, 0, bx - REACH), REACH)]
    place = (dx, nx)
    for source, first, second, third, fourth in (
        (g1, x1, x2, x3, None),
        (g2, t1, t2, t3, x4),
    ):
        restrict_planes(source, first, 1, bx >> 1, place)
        restrict_planes(first, second, 2, bx >> 2, place)
        restrict_planes(second, third, 3, bx >> 3, place)
        if fourth is not None:
            restrict_planes(third, fourth, 4, bx >> 4, place)
    padded = rows_padded(by)
    n3 = x3.shape[0]
    row0 = 0
    for l, (source, target, first) in enumerate(
        ((x1, y1_ref, 0), (x2, y2_ref, 0), (x3, y34_ref, 0), (x4, y34_ref, n3)), 1
    ):
        sy = sy_ref[dy, row0 : row0 + padded[l], :]
        for p in range(source.shape[0]):
            target[first + p] = mm(sy, stacked(source[p]))
        row0 += padded[l]
    off = lane_offsets(bz)
    lane = iota((16, LANES), 1)
    even = (dy % 2) == 0
    for m_ref, rightward in ((ma_ref, even), (mb_ref, jnp.logical_not(even))):
        start1 = pl.multiple_of(jnp.where(rightward, padded[1] - 16, 0), 8)
        start2 = pl.multiple_of(jnp.where(rightward, padded[2] - 16, 0), 8)
        for p in range(y1_ref.shape[0]):
            value = y1_ref[p, pl.ds(start1, 16), :]
            if p < y2_ref.shape[0]:
                value = jnp.where(lane < off[2], value, y2_ref[p, pl.ds(start2, 16), :])
            if p < y34_ref.shape[0]:
                value = jnp.where(lane < off[3], value, y34_ref[p])
            m_ref[2 * p : 2 * p + 2] = value.reshape(2, 8, LANES)
    for p in range(4):
        value = y34_ref[p]
        for g in range(1, 4):
            moved = pltpu.roll(y34_ref[4 * g + p], LANES - 32 * g, 1)
            value = jnp.where(lane >= off[3] - 32 * (g - 1), value, moved)
        mc_ref[2 * p : 2 * p + 2] = value.reshape(2, 8, LANES)


def conv_own_kernel(taps_ref, g_ref, h_ref):
    bx, by, bz = g_ref.shape

    def rows(t, carry):
        at = pl.ds(pl.multiple_of(t * 8, 8), 8)
        for i in range(bx):
            total = None
            for k in range(TAPS):
                j = i + k - REACH
                if 0 <= j < bx:
                    term = g_ref[j, at, :] * taps_ref[0, k]
                    total = term if total is None else total + term
            h_ref[i, at, :] = total
        return carry

    lax.fori_loop(0, by // 8, rows, 0)


def x_slots(n1, n2, each, rows2):
    free = [(p, b) for p in range(n1) for b in range(rows2, each)]
    where = {}
    for q in range(n2):
        for b in range(rows2):
            where[q, b] = (q, b) if q < n1 else free[(q - n1) * rows2 + b]
    return where


def mid_kernel(nx, ny, taps_ref, idx_ref, h_in, xa, xb, ra, rb, rc, y1, y2, y34, *refs):
    ty1, ty2, ty3, ty4, h0, ya_ref, yb_ref, ma_ref, mb_ref, mc_ref, h1, h2, h3, h4, halo = refs
    bx, by, bz = h0.shape
    dx, dy = idx_ref[0], idx_ref[1]
    off = lane_offsets(bz)

    def got(ref, p):
        return ref[2 * p : 2 * p + 2].reshape(16, LANES)

    for own, ty, h in ((y1, ty1, h1), (y2, ty2, h2)):
        for p in range(h.shape[0]):
            value = jnp.concatenate([own[p], got(ra, p), got(rb, p)], axis=0)
            h[p] = mm(ty[...], stacked(value))
    n3 = h3.shape[0]
    for p in range(y34.shape[0]):
        if ny == 4:
            far = rc[2 * (p % 4) : 2 * (p % 4) + 2].reshape(16, LANES)
            if p >= 4:
                far = pltpu.roll(far, 32 * (p // 4), 1)
            parts = [y34[p], got(ra, p), got(rb, p), far]
        else:
            parts = [rc[s, p] for s in range(ny)]
        value = stacked(jnp.concatenate(parts, axis=0))
        if p < n3:
            h3[p] = mm(ty3[...], value)
        else:
            h4[p - n3] = mm(ty4[...], value)

    even = (dx % 2) == 0
    n2, each = h2.shape[0], h1.shape[1] // 8
    n1 = REACH + 3
    slots = x_slots(n1, n2, each, h2.shape[1] // 8)
    at2 = {v: k for k, v in slots.items()}
    lane = iota((8, LANES), 1)

    def block34(pp, b):
        ref, p = (h3, pp) if pp < n3 else (h4, pp - n3)
        return ref[p, 8 * b : 8 * b + 8, :]

    for m_ref, rightward in ((ma_ref, even), (mb_ref, jnp.logical_not(even))):
        start1 = jnp.where(rightward, (bx >> 1) - REACH, 0)
        for p in range(n1):
            for b in range(each):
                value = h1[start1 + p, 8 * b : 8 * b + 8, :]
                if (p, b) in at2:
                    q, bb = at2[p, b]
                    value = jnp.where(lane < off[2], value, h2[q, 8 * bb : 8 * bb + 8, :])
                if b < 2 and p < n3:
                    value = jnp.where(lane < off[3], value, block34(p, b))
                elif 2 <= b < 4 and p < h4.shape[0]:
                    value = jnp.where(lane < off[3], value, block34(n3 + p, b - 2))
                m_ref[p * each + b] = value
    start2 = jnp.where(dx < 2, n2 - 5, 0)
    rows2 = h2.shape[1] // 8
    for s in range(16):
        near = block34(s // 2, s % 2)
        far = pltpu.roll(block34((16 + s) // 2, s % 2), LANES - 32, 1)
        value = jnp.where(lane >= off[3], near, far)
        if s < 5 * rows2:
            b = s % rows2
            two = pltpu.roll(h2[start2 + s // rows2, 8 * b : 8 * b + 8, :], 64, 1)
            value = jnp.where(lane >= off[3] - 32, value, two)
        mc_ref[s] = value

    halo[jnp.where(even, 1, 0)] = xa[...]
    halo[jnp.where(even, 0, 1)] = xb[...]

    def rows(t, carry):
        at = pl.ds(pl.multiple_of(t * 8, 8), 8)
        for i in range(REACH):
            low, high = h_in[i, at, :], h_in[bx - REACH + i, at, :]
            for m in range(i, REACH):
                low = low + halo[0, m, at, :] * taps_ref[0, m - i]
            for m in range(i + 1):
                high = high + halo[1, m, at, :] * taps_ref[0, 2 * REACH + m - i]
            h0[i, at, :] = low
            h0[bx - REACH + i, at, :] = high
        return carry

    lax.fori_loop(0, by // 8, rows, 0)
    even = (dy % 2) == 0
    for m_ref, rightward in ((ya_ref, even), (yb_ref, jnp.logical_not(even))):
        m_ref[...] = h0[:, pl.ds(pl.multiple_of(jnp.where(rightward, by - 8, 0), 8), 8), :]


def last_own_kernel(taps_ref, h0, h1, ty0, f0, f1):
    bx, by, bz = h0.shape

    def plane(p, carry):
        f0[p] = mm(ty0[...], stacked(h0[p]))
        return carry

    lax.fori_loop(0, bx, plane, 0, unroll=4)
    count = h1.shape[0]
    for i in range(count):
        total = None
        for k in range(TAPS):
            j = i + k - REACH
            if 0 <= j < count:
                term = h1[j] * taps_ref[3, k]
                total = term if total is None else total + term
        f1[i] = total


def last_kernel(nx, taps_ref, idx_ref, f0, f1o, h2, h3, h4, ya, yb, ra, rb, rc, *refs):
    tyh, py_ref, pz_ref, out_ref, side, e2, e3, e4, f1, f2, f3, f4, s1, s2 = refs
    bx, by, bz = f0.shape
    dx, dy, dz = idx_ref[0], idx_ref[1], idx_ref[2]
    even = (dx % 2) == 0
    place = (dx, nx)
    padded = rows_padded(by)
    each = f1o.shape[1] // 8
    n1, n2, n3, n4 = REACH + 3, h2.shape[0], h3.shape[0], h4.shape[0]
    rows2 = h2.shape[1] // 8
    slots = x_slots(n1, n2, each, rows2)

    side[jnp.where(even, 1, 0)] = ra[...].reshape(n1, each * 8, LANES)
    partner = jnp.where(even, dx > 0, dx < nx - 1)
    side[jnp.where(even, 0, 1)] = rb[...].reshape(n1, each * 8, LANES) * jnp.where(
        partner, 1.0, 0.0
    ).astype(F32)
    block = bx >> 1
    for r in range(f1.shape[0]):
        total, i = f1o[r], r - LOW[1]
        for m in range(n1):
            for s, j in ((0, m - REACH - 1), (1, block - 1 + m)):
                k = j - i + REACH
                if 0 <= k < TAPS:
                    total = total + side[s, m] * taps_ref[3, k]
        f1[r] = masked(total, i, block, place)

    def near(ref, l, p):
        if l == 2:
            return jnp.concatenate(
                [ref[slots[p, b][0] * each + slots[p, b][1]] for b in range(rows2)], axis=0
            )
        first = p * each + (0 if l == 3 else 2)
        return ref[first : first + 2].reshape(16, LANES)

    def far(l, p):
        if l == 2:
            value = rc[p * rows2 : (p + 1) * rows2].reshape(8 * rows2, LANES)
            return pltpu.roll(value, 64, 1)
        first = 2 * p if l == 3 else 2 * (n3 + p)
        value = rc[first % 16 : first % 16 + 2].reshape(16, LANES)
        return value if first < 16 else pltpu.roll(value, 32, 1)

    for e, h, l in ((e2, h2, 2), (e3, h3, 3), (e4, h4, 4)):
        e[...] = jnp.zeros_like(e)
        for b in range(nx):
            source = xor(dx, GATHER[b]) if nx == 4 else b
            at = source * (bx >> l) - LOW[l] + 12
            count = h.shape[0]
            if nx == 4 and b == 3 and l == 2:
                at, count = at + jnp.where(source < 2, n2 - 5, 0), 5
            for p in range(count):
                if nx != 4:
                    value = near(rc.at[b], l, p)
                else:
                    value = far(l, p) if b == 3 else near(rb, l, p) if b == 2 else h[p]
                    if b == 1:
                        value = near(ra, l, p)
                e[at + p] = e[at + p] + value
    for e, f, l in ((e2, f2, 2), (e3, f3, 3), (e4, f4, 4)):
        start = dx * (bx >> l) - LOW[l] - REACH + 12
        for r in range(f.shape[0]):
            total = e[start + r] * taps_ref[3 * l, 0]
            for k in range(1, TAPS):
                total = total + e[start + r + k] * taps_ref[3 * l, k]
            f[r] = masked(total, r - LOW[l], bx >> l, place)
    for p in range(bx):
        value = mm(tyh[...], stacked(jnp.concatenate([ya[p], yb[p]], axis=0)))
        out_ref[p, 0:8] = f0[p, 0:8] + value[0:8]
        out_ref[p, 8 : by - 8] = f0[p, 8 : by - 8]
        out_ref[p, by - 8 : by] = f0[p, by - 8 : by] + value[8:16]
    row0 = [sum(padded[:l]) for l in range(LEVELS)]
    for l, f, target in ((3, f4, f3), (2, f3, f2), (1, f2, f1), (0, f1, out_ref)):
        rows, k = padded[l], 2 * padded[l + 1]
        matrix = py_ref[dy, row0[l] : row0[l] + rows, :k]
        count = f.shape[0]
        for p in range(count):
            hi, lo = halves(f[p])
            s1[p, 0:rows] = mm(matrix, jnp.concatenate([hi, lo], axis=0).astype(BF16))
        pz = jnp.concatenate([pz_ref[dz, l], pz_ref[dz, l]], axis=0)
        for p in range(count):
            hi, lo = halves(s1[p, 0:rows])
            s2[p, 0:rows] = mm(jnp.concatenate([hi, lo], axis=1).astype(BF16), pz)
        for r in range(target.shape[0]):
            j = r - LOW[l]
            total = None
            for kk, w in CUBIC.items():
                if (j - kk) % 2 == 0:
                    p = (j - kk) // 2 + LOW[l + 1]
                    if 0 <= p < count:
                        value = s2[p, 0:rows]
                        term = value if w == 1.0 else value * w
                        total = term if total is None else total + term
            target[r] = target[r] + masked(total, j, bx >> l, place)


def call(kernel, out_shape, args, n_smem, scratch=(), flops=0, aliases={}, hbm=()):
    vmem, smem = pl.BlockSpec(memory_space=pltpu.VMEM), pl.BlockSpec(memory_space=pltpu.SMEM)
    anywhere = pl.BlockSpec(memory_space=pl.ANY)
    many = isinstance(out_shape, (tuple, list))
    return pl.pallas_call(
        kernel,
        out_shape=out_shape,
        in_specs=[
            smem if i < n_smem else anywhere if i in hbm else vmem for i in range(len(args))
        ],
        out_specs=[vmem] * len(out_shape) if many else vmem,
        scratch_shapes=scratch,
        input_output_aliases=aliases,
        cost_estimate=pl.CostEstimate(flops=flops, bytes_accessed=2**20, transcendentals=0),
        compiler_params=pltpu.CompilerParams(vmem_limit_bytes=20 * 2**20),
    )(*args)


def swaps(count, flip):
    return [(i, i ^ flip) for i in range(count)]


def middle_swaps(count):
    if count == 4:
        return swaps(count, 3)
    return [p for i in range(1, count - 1, 2) for p in ((i, i + 1), (i + 1, i))]


def per_device(charges, kernel_taps):
    nx, ny, nz = (lax.axis_size(a) for a in ("gx", "gy", "gz"))
    bx, by, bz = charges.shape
    assert bz == LANES and nx % 2 == 0 and ny % 2 == 0
    xs, ys, padded = sizes(bx), sizes(by), rows_padded(by)
    dx, dy, dz = (lax.axis_index(a) for a in ("gx", "gy", "gz"))
    taps = kernel_taps.reshape(3 * LEVELS, TAPS)
    idx = jnp.stack([dx, dy, dz]).astype(jnp.int32)

    def shape(*dims, dtype=F32):
        return jax.ShapeDtypeStruct(dims, dtype)

    def neighbours(count):
        return [(i, j) for i, j in middle_swaps(count) if abs(i - j) == 1]

    if nz == 2:
        others = (lax.ppermute(charges, "gz", swaps(2, 1)),)
    else:
        others = (lax.all_gather(charges, "gz"),)
    rz = jnp.asarray(lanes_restrict_const(nz * bz))
    in_y = [0, padded[1] + 32, padded[2] + 32, 16 * ny, 16 * ny]
    q, w, ty0, tyh, *ty = call(
        functools.partial(setup_kernel, by, ny, nz, ny * by),
        [
            shape(bx, by, bz),
            shape(3 * nz * bz, 3 * LANES, dtype=BF16),
            shape(by, 3 * by, dtype=BF16),
            shape(16, 48, dtype=BF16),
        ]
        + [shape(padded[l], 3 * in_y[l], dtype=BF16) for l in range(1, LEVELS)],
        (taps, idx, charges, rz),
        2,
        [pltpu.VMEM((rz.shape[1], 2 * LANES), F32), pltpu.SemaphoreType.DMA],
        flops=10**8,
        hbm=(2,),
    )
    sy = jnp.asarray(split_rows_const(ny * by, ny))
    sources = (q, *others) if nz == 2 else others
    n34 = xs[3] + xs[4]
    face, coarse = shape(REACH, by, bz), shape(2 * xs[1], 8, LANES)
    plane = lambda n: pltpu.VMEM((n, by, bz), F32)
    g0, xa, xb, ma, mb, mc, y1, y2, y34 = call(
        functools.partial(z_kernel, nx, nz),
        [
            shape(bx, by, bz),
            face,
            face,
            coarse,
            coarse,
            shape(8, 8, LANES),
            shape(xs[1], padded[1], LANES),
            shape(xs[2], padded[2], LANES),
            shape(n34, 16, LANES),
        ],
        (idx, *sources, w, sy),
        1,
        [plane(bx), plane(bx), plane(xs[1]), plane(xs[2]), plane(xs[3])]
        + [plane(xs[1]), plane(xs[2]), plane(xs[3]), plane(xs[4])],
        flops=10**9,
    )
    xa = lax.ppermute(xa, "gx", swaps(nx, 1))
    xb = lax.ppermute(xb, "gx", neighbours(nx))
    ra = lax.ppermute(ma, "gy", swaps(ny, 1))
    rb = lax.ppermute(mb, "gy", middle_swaps(ny))
    rc = lax.ppermute(mc, "gy", swaps(ny, 2)) if ny == 4 else lax.all_gather(y34, "gy")
    h0 = call(conv_own_kernel, shape(bx, by, bz), (taps, g0), 1, flops=10**9)
    each = padded[1] // 8
    strip, coarse = shape(bx, 8, LANES), shape((REACH + 3) * each, 8, LANES)
    h0, ya, yb, ma, mb, mc, h1, h2, h3, h4 = call(
        functools.partial(mid_kernel, nx, ny),
        [shape(bx, by, bz), strip, strip, coarse, coarse, shape(16, 8, LANES)]
        + [shape(xs[l], padded[l], LANES) for l in range(1, LEVELS)],
        (taps, idx, h0, xa, xb, ra, rb, rc, y1, y2, y34, *ty),
        2,
        [pltpu.VMEM((2, REACH, by, bz), F32)],
        flops=10**9,
        aliases={2: 0},
    )
    ra = lax.ppermute(ma, "gx", swaps(nx, 1))
    rb = lax.ppermute(mb, "gx", middle_swaps(nx))
    rc = lax.ppermute(mc, "gx", swaps(nx, 2)) if nx == 4 else lax.all_gather(ma, "gx")
    ya = lax.ppermute(ya, "gy", swaps(ny, 1))
    yb = lax.ppermute(yb, "gy", neighbours(ny))
    f0, f1 = call(
        last_own_kernel,
        [shape(bx, by, bz), shape(xs[1], padded[1], LANES)],
        (taps, h0, h1, ty0),
        1,
        flops=10**9,
    )
    py = jnp.asarray(prolong_rows_const(ny * by, ny))
    pz = jnp.asarray(prolong_lanes_const(nz * bz, nz))
    buf = lambda n, rows: pltpu.VMEM((n, rows, LANES), F32)
    return call(
        functools.partial(last_kernel, nx),
        shape(bx, by, bz),
        (taps, idx, f0, f1, h2, h3, h4, ya, yb, ra, rb, rc, tyh, py, pz),
        2,
        [pltpu.VMEM((2, REACH + 3, padded[1], LANES), F32)]
        + [buf((nx * bx >> l) + 24, padded[l]) for l in range(2, LEVELS)]
        + [buf(xs[l], padded[l]) for l in range(1, LEVELS)]
        + [buf(xs[1], by), buf(xs[1], by)],
        flops=10**9,
    )


def solution(mesh):
    in_specs = (P("gx", "gy", "gz"), P())
    out_specs = P("gx", "gy", "gz")
    return jax.shard_map(
        per_device, mesh=mesh, in_specs=in_specs, out_specs=out_specs, check_vma=False
    )
```

```python
import functools

import jax
import jax.numpy as jnp
import numpy as np
from jax import lax
from jax.experimental import pallas as pl
from jax.experimental.pallas import tpu as pltpu
from jax.sharding import PartitionSpec as P

LEVELS = 5
TAPS = 17
REACH = 8
LANES = 128
CUBIC = {-3: -0.0625, -1: 0.5625, 0: 1.0, 1: 0.5625, 3: -0.0625}
LOW = (0, 1, 2, 2, 2)
HIGH = (0, 2, 3, 3, 3)
F32 = jnp.float32
BF16 = jnp.bfloat16
GATHER = (0, 1, 3, 2)
FLOPS = 10**9


def sizes(block):
    return [block // 2**l + LOW[l] + HIGH[l] for l in range(LEVELS)]


def pad8(n):
    return -(-n // 8) * 8


def pad16(n):
    return -(-n // 16) * 16


def restrictions(whole):
    composite, out = np.eye(whole), [np.eye(whole)]
    for _ in range(1, LEVELS):
        fine = composite.shape[0]
        step = np.zeros((fine // 2, fine))
        for i in range(fine // 2):
            for k, w in CUBIC.items():
                if 0 <= 2 * i + k < fine:
                    step[i, 2 * i + k] = w
        composite = step @ composite
        out.append(composite)
    return out


def rows_padded(block):
    n = sizes(block)
    return [block] + [max(16, pad8(n[l])) for l in range(1, LEVELS)]


def lane_offsets(block):
    n = sizes(block)
    return [0, 0, n[1], n[1] + n[2], n[1] + n[2]]


def split_rows_const(whole, count):
    block = whole // count
    full, n, padded = restrictions(whole), sizes(block), rows_padded(block)
    out = np.zeros((count, sum(padded[1:]), block), np.float32)
    for d in range(count):
        row0 = 0
        for l in range(1, LEVELS):
            for r in range(n[l]):
                g = d * (block >> l) - LOW[l] + r
                if 0 <= g < whole >> l:
                    out[d, row0 + r] = full[l][g, d * block : (d + 1) * block]
            row0 += padded[l]
    hi = out.astype(BF16)
    lo = (out - hi.astype(np.float32)).astype(BF16)
    return np.concatenate([hi, hi, lo], axis=2)


def prolong_entries(whole, count, d, l):
    block = whole // count
    n = sizes(block)
    for i in range(n[l]):
        g_out = d * (block >> l) - LOW[l] + i
        for j in range(n[l + 1]):
            g_in = d * (block >> (l + 1)) - LOW[l + 1] + j
            ok = 0 <= g_out < whole >> l and 0 <= g_in < whole >> (l + 1)
            if ok and g_out - 2 * g_in in CUBIC:
                yield i, j, CUBIC[g_out - 2 * g_in]


def prolong_rows_const(whole, count):
    padded = rows_padded(whole // count)
    out = np.zeros((count, sum(padded[:4]), 2 * padded[1]), np.float32)
    for d in range(count):
        row0 = 0
        for l in range(LEVELS - 1):
            for i, j, w in prolong_entries(whole, count, d, l):
                out[d, row0 + i, j] = w
                out[d, row0 + i, padded[l + 1] + j] = w
            row0 += padded[l]
    return out.astype(BF16)


def prolong_lanes_const(whole, count):
    off = lane_offsets(whole // count)
    out = np.zeros((count, LEVELS - 1, LANES, LANES), np.float32)
    for d in range(count):
        for l in range(LEVELS - 1):
            for i, j, w in prolong_entries(whole, count, d, l):
                out[d, l, off[l + 1] + j, off[l] + i] = w
    return out.astype(BF16)


def toeplitz(taps_ref, row, g_in, g_out, mask):
    diff = g_in - g_out + REACH
    value = jnp.zeros(diff.shape, F32)
    for k in range(TAPS):
        value = jnp.where(diff == k, taps_ref[row, k], value)
    return jnp.where(mask, value, 0.0)


def iota(shape, axis):
    return lax.broadcasted_iota(jnp.int32, shape, axis)


def xor(a, b):
    return jnp.bitwise_xor(a, jnp.int32(b))


def halves(value):
    scaled = value * 65537.0
    hi = scaled - (scaled - value)
    return hi, value - hi


def mm(a, b):
    return jnp.dot(a, b, preferred_element_type=F32)


def spread(fine, coarse):
    k = fine - 2 * iota(fine.shape, 1)
    step = jnp.where(k == 0, 1.0, 0.0)
    step = jnp.where((k == 1) | (k == -1), 0.5625, step)
    step = jnp.where((k == 3) | (k == -3), -0.0625, step).astype(BF16)
    hi, lo = halves(coarse)
    low, rest = halves(lo)
    total = mm(step, rest.astype(BF16)) + mm(step, low.astype(BF16))
    return total + mm(step, hi.astype(BF16))


def setup_kernel(
    by, ny, nz, whole_y, taps_ref, idx_ref, w0_ref, w_ref, ty0_ref, *rest
):
    tyh_ref, ty_refs = rest[0], rest[1:5]
    bz = LANES
    whole_z = nz * bz
    dy, dz = idx_ref[1], idx_ref[2]
    n, off = sizes(bz), lane_offsets(bz)
    below = None
    for l in range(LEVELS - 1, 0, -1):
        rows = whole_z >> l
        col = iota((rows, LANES), 1)
        g_out = dz * (bz >> l) - LOW[l] + col - off[l]
        mask = (col >= off[l]) & (col < off[l] + n[l]) & (g_out >= 0) & (g_out < rows)
        here = toeplitz(taps_ref, 3 * l + 2, iota((rows, LANES), 0), g_out, mask)
        none = jnp.zeros((rows, LANES), F32)
        here = jnp.concatenate([none, here] if l == LEVELS - 1 else [here, none], axis=1)
        if below is not None:
            here = here + spread(iota((rows, rows // 2), 0), below)
        below = here
    order = [dz, 1 - dz] if nz == 2 else list(range(nz))

    def store_rows(ref, j, value):
        hi, lo = halves(value)
        ref[j * bz : (j + 1) * bz] = hi.astype(BF16)
        ref[(nz + j) * bz : (nz + j + 1) * bz] = hi.astype(BF16)
        ref[(2 * nz + j) * bz : (2 * nz + j + 1) * bz] = lo.astype(BF16)

    for j, source in enumerate(order):
        g_in = source * bz + iota((bz, bz), 0)
        g_out = dz * bz + iota((bz, bz), 1)
        store_rows(w0_ref, j, toeplitz(taps_ref, 2, g_in, g_out, g_out >= 0))
    even = (dy % 2) == 0
    sizes_y, padded = sizes(by), rows_padded(by)

    def column(shape):
        k = shape[1] // 3
        j = iota(shape, 1)
        return k, jnp.where(j >= 2 * k, j - 2 * k, jnp.where(j >= k, j - k, j))

    def store(ref, k, value):
        hi, lo = halves(value)
        ref[...] = jnp.where(iota(ref.shape, 1) < 2 * k, hi, lo).astype(BF16)

    def windows(l, j, own, window):
        block = by >> l
        right = (dy + 1) * block - LOW[l]
        left = (dy - 1) * block - LOW[l] + padded[l] - window
        base_a = jnp.where(even, right, left)
        base_b = jnp.where(even, left, right)
        second = jnp.where(j < own + window, base_a + j - own, base_b + j - own - window)
        return jnp.where(j < own, dy * block - LOW[l] + j, second)

    k, j = column(ty0_ref.shape)
    i = iota(ty0_ref.shape, 0)
    store(ty0_ref, k, toeplitz(taps_ref, 1, j, i, i >= 0))
    k, j = column(tyh_ref.shape)
    i = iota(tyh_ref.shape, 0)
    i = dy * by + jnp.where(i < 8, i, i + by - 16)
    g_in = windows(0, j, 0, 8)
    store(tyh_ref, k, toeplitz(taps_ref, 1, g_in, i, (g_in >= 0) & (g_in < whole_y)))
    for l, ty_ref in enumerate(ty_refs, 1):
        block = by >> l
        k, j = column(ty_ref.shape)
        if l < 3:
            g_in = windows(l, j, padded[l], 16)
        else:
            g_in = j
            for b in range(ny):
                source = xor(dy, GATHER[b]) if ny == 4 else b
                here = (j >= b * 16) & (j < (b + 1) * 16)
                g_in = jnp.where(here, source * block - LOW[l] + j - b * 16, g_in)
        i = iota(ty_ref.shape, 0)
        g_out = dy * block - LOW[l] + i
        mask = (i < sizes_y[l]) & (g_out >= 0) & (g_out < whole_y >> l)
        mask = mask & (g_in >= 0) & (g_in < whole_y >> l)
        store(ty_ref, k, toeplitz(taps_ref, 3 * l + 1, g_in, g_out, mask))
    for j, source in enumerate(order):
        store_rows(w_ref, j, spread(source * bz + iota((bz, whole_z // 2), 0), below))


def masked(value, index, block, place):
    if 0 <= index < block:
        return value
    cell = place[0] * block + index
    inside = (cell >= 0) & (cell < place[1] * block)
    return value * jnp.where(inside, 1.0, 0.0).astype(F32)


def restrict_planes(src, dst, level, block_out, place):
    lo_in, count_in = LOW[level - 1], src.shape[0]
    for r in range(dst.shape[0]):
        i = r - LOW[level]
        total = None
        for k, w in CUBIC.items():
            p = 2 * i + k + lo_in
            if 0 <= p < count_in:
                term = src[p] if w == 1.0 else src[p] * w
                total = term if total is None else total + term
        dst[r] = masked(total, i, block_out, place)


def stacked(value):
    hi, lo = halves(value)
    return jnp.concatenate([hi, lo, hi], axis=0).astype(BF16)


def y_slots(n1, n2, n3, n4):
    half = -(-n1 // 2)
    ones = [[(p, 0)] for p in range(n1)]
    ones += [[(p, 1)] + ([(p + half, 1)] if p + half < n1 else []) for p in range(half)]
    twos = [(p, 0) for p in range(n2)] + [(p, 1) for p in range(n2)]
    threes = [[(p, 0)] for p in range(n3 + n4)]
    threes += [[(p, 1)] + ([(n3 + p, 1)] if p < n4 else []) for p in range(n3)]
    assert max(len(twos), len(threes)) <= len(ones)
    return ones, twos, threes


def put(ref, first, p, value):
    ref[first + p] = value


def batched(matrix, values, store, form=stacked, group=4):
    for p in range(0, len(values), group):
        some = values[p : p + group]
        out = mm(matrix, jnp.concatenate([form(v()) for v in some], axis=1))
        for q in range(len(some)):
            store(p + q, out[:, q * LANES : (q + 1) * LANES])


def z_rows(src, nz, planes, count):
    if nz == 2:
        blocks = [s[planes] for s in src]
    else:
        blocks = [src[0][s, planes] for s in range(nz)]
    his, los = zip(*[halves(b.reshape(count * b.shape[1], b.shape[2])) for b in blocks])
    return jnp.concatenate([h.astype(BF16) for h in his + los + his], axis=1)


def z0_kernel(nz, idx_ref, *refs):
    src = refs[: (2 if nz == 2 else 1)]
    w_ref, g0_ref, xa_ref, xb_ref = refs[len(src) :]
    bx, by, bz = g0_ref.shape
    chunk = 8

    def step(c, carry):
        planes = pl.ds(c * chunk, chunk)
        out = mm(z_rows(src, nz, planes, chunk), w_ref[...])
        g0_ref[planes] = out.reshape(chunk, by, bz)
        return carry

    lax.fori_loop(0, bx // chunk, step, 0)
    even = (idx_ref[0] % 2) == 0
    xa_ref[...] = g0_ref[pl.ds(jnp.where(even, bx - REACH, 0), REACH)]
    xb_ref[...] = g0_ref[pl.ds(jnp.where(even, 0, bx - REACH), REACH)]


def z_kernel(nx, nz, idx_ref, *refs):
    src = refs[: (2 if nz == 2 else 1)]
    w_ref, sy_ref, ma_ref, mb_ref, mc_ref, y1_ref, y2_ref, y34_ref = refs[
        len(src) : len(src) + 8
    ]
    g1, g2, x1, x2, x3, t1, t2, t3, x4 = refs[len(src) + 8 :]
    bx, by, bz = g1.shape
    dx, dy = idx_ref[0], idx_ref[1]
    chunk = 8

    def step(c, carry):
        planes = pl.ds(c * chunk, chunk)
        out = mm(z_rows(src, nz, planes, chunk), w_ref[...])
        g1[planes] = out[:, :LANES].reshape(chunk, by, bz)
        g2[planes] = out[:, LANES:].reshape(chunk, by, bz)
        return carry

    lax.fori_loop(0, bx // chunk, step, 0)
    place = (dx, nx)
    for source, first, second, third, fourth in (
        (g1, x1, x2, x3, None),
        (g2, t1, t2, t3, x4),
    ):
        restrict_planes(source, first, 1, bx >> 1, place)
        restrict_planes(first, second, 2, bx >> 2, place)
        restrict_planes(second, third, 3, bx >> 3, place)
        if fourth is not None:
            restrict_planes(third, fourth, 4, bx >> 4, place)
    padded = rows_padded(by)
    n3 = x3.shape[0]
    row0 = 0
    for l, (source, target, first) in enumerate(
        ((x1, y1_ref, 0), (x2, y2_ref, 0), (x3, y34_ref, 0), (x4, y34_ref, n3)), 1
    ):
        sy = sy_ref[dy, row0 : row0 + padded[l], :]
        planes = [functools.partial(lambda ref, p: ref[p], source, p) for p in range(source.shape[0])]
        batched(sy, planes, functools.partial(put, target, first))
        row0 += padded[l]
    off = lane_offsets(bz)
    even = (dy % 2) == 0
    n1, n2 = y1_ref.shape[0], y2_ref.shape[0]
    ones, twos, threes = y_slots(n1, n2, n3, y34_ref.shape[0] - n3)
    lane8, row8 = iota((8, LANES), 1), iota((8, LANES), 0)
    for m_ref, rightward in ((ma_ref, even), (mb_ref, jnp.logical_not(even))):
        start1 = pl.multiple_of(jnp.where(rightward, padded[1] - 16, 0), 8)
        start2 = pl.multiple_of(jnp.where(rightward, padded[2] - 16, 0), 8)

        def first(p, b):
            return y1_ref[p, pl.ds(start1 + 8 * b, 8), :]

        for s in range(m_ref.shape[0]):
            value = first(*ones[s][0])
            if len(ones[s]) == 2:
                value = jnp.where(row8 < 4, value, pltpu.roll(first(*ones[s][1]), 4, 0))
            if s < len(twos):
                p, b = twos[s]
                value = jnp.where(lane8 < off[2], value, y2_ref[p, pl.ds(start2 + 8 * b, 8), :])
            if s < len(threes):
                p, b = threes[s][0]
                three = y34_ref[p, 8 * b : 8 * b + 8, :]
                if len(threes[s]) == 2:
                    p, b = threes[s][1]
                    four = pltpu.roll(y34_ref[p, 8 * b : 8 * b + 8, :], 5, 0)
                    three = jnp.where(row8 < 5, three, four)
                value = jnp.where(lane8 < off[3], value, three)
            m_ref[s] = value
    lane = iota((16, LANES), 1)
    for p in range(4):
        value = y34_ref[p]
        for g in range(1, 4):
            moved = pltpu.roll(y34_ref[4 * g + p], LANES - 32 * g, 1)
            value = jnp.where(lane >= off[3] - 32 * (g - 1), value, moved)
        mc_ref[2 * p : 2 * p + 2] = value.reshape(2, 8, LANES)


def conv_own_kernel(taps_ref, g_ref, h_ref):
    bx, by, bz = g_ref.shape

    def rows(t, carry):
        at = pl.ds(pl.multiple_of(t * 8, 8), 8)
        for i in range(bx):
            total = None
            for k in range(TAPS):
                j = i + k - REACH
                if 0 <= j < bx:
                    term = g_ref[j, at, :] * taps_ref[0, k]
                    total = term if total is None else total + term
            h_ref[i, at, :] = total
        return carry

    lax.fori_loop(0, by // 8, rows, 0)


def x_slots(n1, n2, rows1, rows2):
    whole = rows1 - 1
    free = [whole * p + b for p in range(n1) for b in range(rows2, whole)]
    twos = {}
    for q in range(n2):
        for b in range(rows2):
            slot = whole * q + b if q < n1 else free[(q - n1) * rows2 + b]
            twos[slot] = (q, b)
    return twos


def mid_kernel(nx, ny, taps_ref, idx_ref, h_in, xa, xb, ra, rb, rc, y1, y2, y34, *refs):
    ty1, ty2, ty3, ty4, h0, ya_ref, yb_ref, ma_ref, mb_ref, mc_ref, h1, h2, h3, h4, halo = refs
    bx, by, bz = h0.shape
    dx, dy = idx_ref[0], idx_ref[1]
    off = lane_offsets(bz)

    ones, twos, threes = y_slots(y1.shape[0], y2.shape[0], h3.shape[0], h4.shape[0])
    row8 = iota((8, LANES), 0)
    found = {}
    for l, slots in ((1, ones), (2, [[v] for v in twos]), (3, threes)):
        for s, held in enumerate(slots):
            for place, (p, b) in enumerate(held):
                used = 8 if b == 0 else {1: 3, 2: 5}.get(l, 5 if p < h3.shape[0] else 1)
                found[l, p, b] = (s, 0 if place == 0 else 4 if l == 1 else 3, used)

    def block(ref, l, p, b):
        s, turn, used = found[l, p, b]
        value = ref[s] if turn == 0 else pltpu.roll(ref[s], turn, 0)
        return value if used == 8 else jnp.where(row8 < used, value, 0.0)

    def got(ref, l, p):
        return jnp.concatenate([block(ref, l, p, 0), block(ref, l, p, 1)], axis=0)

    def joined(own, l, p):
        return jnp.concatenate([own[p], got(ra, l, p), got(rb, l, p)], axis=0)

    def gathered(p):
        if ny == 4:
            far = rc[2 * (p % 4) : 2 * (p % 4) + 2].reshape(16, LANES)
            if p >= 4:
                far = pltpu.roll(far, 32 * (p // 4), 1)
            parts = [y34[p], got(ra, 3, p), got(rb, 3, p), far]
        else:
            parts = [rc[s, p] for s in range(ny)]
        return jnp.concatenate(parts, axis=0)

    for own, ty, h, l in ((y1, ty1, h1, 1), (y2, ty2, h2, 2)):
        planes = [functools.partial(joined, own, l, p) for p in range(h.shape[0])]
        batched(ty[...], planes, functools.partial(put, h, 0))
    n3 = h3.shape[0]
    planes = [functools.partial(gathered, p) for p in range(y34.shape[0])]
    batched(ty3[...], planes[:n3], functools.partial(put, h3, 0))
    batched(ty4[...], planes[n3:], functools.partial(put, h4, 0))

    even = (dx % 2) == 0
    n2, n1 = h2.shape[0], REACH + 3
    each = h1.shape[1] // 8 - 1
    twos = x_slots(n1, n2, each + 1, h2.shape[1] // 8)
    half = -(-n1 // 2)
    lane = iota((8, LANES), 1)

    def block34(pp, b):
        ref, p = (h3, pp) if pp < n3 else (h4, pp - n3)
        return ref[p, 8 * b : 8 * b + 8, :]

    for m_ref, rightward in ((ma_ref, even), (mb_ref, jnp.logical_not(even))):
        start1 = jnp.where(rightward, (bx >> 1) - REACH, 0)
        for p in range(n1):
            for b in range(each):
                value = h1[start1 + p, 8 * b : 8 * b + 8, :]
                if each * p + b in twos:
                    q, bb = twos[each * p + b]
                    value = jnp.where(lane < off[2], value, h2[q, 8 * bb : 8 * bb + 8, :])
                if b < 2 and p < n3:
                    value = jnp.where(lane < off[3], value, block34(p, b))
                elif 2 <= b < 4 and p < h4.shape[0]:
                    value = jnp.where(lane < off[3], value, block34(n3 + p, b - 2))
                m_ref[each * p + b] = value
        for p in range(half):
            value = h1[start1 + p, 8 * each : 8 * each + 8, :]
            if p + half < n1:
                other = pltpu.roll(h1[start1 + p + half, 8 * each : 8 * each + 8, :], 4, 0)
                value = jnp.where(row8 < 4, value, other)
            m_ref[each * n1 + p] = value
    start2 = jnp.where(dx < 2, n2 - 5, 0)
    rows2 = h2.shape[1] // 8
    for s in range(16):
        near = block34(s // 2, s % 2)
        far = pltpu.roll(block34((16 + s) // 2, s % 2), LANES - 32, 1)
        value = jnp.where(lane >= off[3], near, far)
        if s < 5 * rows2:
            b = s % rows2
            two = pltpu.roll(h2[start2 + s // rows2, 8 * b : 8 * b + 8, :], 64, 1)
            value = jnp.where(lane >= off[3] - 32, value, two)
        mc_ref[s] = value

    halo[jnp.where(even, 1, 0)] = xa[...]
    halo[jnp.where(even, 0, 1)] = xb[...]

    def rows(t, carry):
        at = pl.ds(pl.multiple_of(t * 8, 8), 8)
        for i in range(REACH):
            low, high = h_in[i, at, :], h_in[bx - REACH + i, at, :]
            for m in range(i, REACH):
                low = low + halo[0, m, at, :] * taps_ref[0, m - i]
            for m in range(i + 1):
                high = high + halo[1, m, at, :] * taps_ref[0, 2 * REACH + m - i]
            h0[i, at, :] = low
            h0[bx - REACH + i, at, :] = high
        return carry

    lax.fori_loop(0, by // 8, rows, 0)
    even = (dy % 2) == 0
    for m_ref, rightward in ((ya_ref, even), (yb_ref, jnp.logical_not(even))):
        m_ref[...] = h0[:, pl.ds(pl.multiple_of(jnp.where(rightward, by - 8, 0), 8), 8), :]


def last_own_kernel(taps_ref, h0, h1, ty0, f0, f1):
    bx, by, bz = h0.shape

    def planes(c, carry):
        some = [functools.partial(lambda p: h0[p], 4 * c + q) for q in range(4)]
        batched(ty0[...], some, lambda q, value: put(f0, 4 * c, q, value))
        return carry

    lax.fori_loop(0, bx // 4, planes, 0)
    count = h1.shape[0]
    for i in range(count):
        total = None
        for k in range(TAPS):
            j = i + k - REACH
            if 0 <= j < count:
                term = h1[j] * taps_ref[3, k]
                total = term if total is None else total + term
        f1[i] = total


def last_kernel(nx, taps_ref, idx_ref, f0, f1o, h2, h3, h4, ya, yb, ra, rb, rc, *refs):
    tyh, py_ref, pz_ref, out_ref, side, e2, e3, e4, f1, f2, f3, f4 = refs[:12]
    stage = refs[12:]
    bx, by, bz = f0.shape
    dx, dy, dz = idx_ref[0], idx_ref[1], idx_ref[2]
    even = (dx % 2) == 0
    place = (dx, nx)
    padded = rows_padded(by)
    each = f1o.shape[1] // 8 - 1
    n1, n2, n3, n4 = REACH + 3, h2.shape[0], h3.shape[0], h4.shape[0]
    rows2 = h2.shape[1] // 8
    twos = {v: k for k, v in x_slots(n1, n2, each + 1, rows2).items()}
    half = -(-n1 // 2)

    partner = jnp.where(even, dx > 0, dx < nx - 1)
    okay = jnp.where(partner, 1.0, 0.0).astype(F32)
    for ref, place_of, scale in ((ra, jnp.where(even, 1, 0), None), (rb, jnp.where(even, 0, 1), okay)):
        for p in range(n1):
            final = ref[each * n1 + p % half]
            final = pltpu.roll(final, 4, 0) if p >= half else final
            value = jnp.concatenate(
                [ref[each * p : each * p + each].reshape(8 * each, LANES), final], axis=0
            )
            side[place_of, p] = value if scale is None else value * scale
    block = bx >> 1
    for r in range(f1.shape[0]):
        total, i = f1o[r], r - LOW[1]
        for m in range(n1):
            for s, j in ((0, m - REACH - 1), (1, block - 1 + m)):
                k = j - i + REACH
                if 0 <= k < TAPS:
                    total = total + side[s, m] * taps_ref[3, k]
        f1[r] = masked(total, i, block, place)

    def near(ref, l, p):
        if l == 2:
            return jnp.concatenate(
                [ref[twos[p, b]] for b in range(rows2)], axis=0
            )
        first = p * each + (0 if l == 3 else 2)
        return ref[first : first + 2].reshape(16, LANES)

    def far(l, p):
        if l == 2:
            value = rc[p * rows2 : (p + 1) * rows2].reshape(8 * rows2, LANES)
            return pltpu.roll(value, 64, 1)
        first = 2 * p if l == 3 else 2 * (n3 + p)
        value = rc[first % 16 : first % 16 + 2].reshape(16, LANES)
        return value if first < 16 else pltpu.roll(value, 32, 1)

    for e, h, l in ((e2, h2, 2), (e3, h3, 3), (e4, h4, 4)):
        e[...] = jnp.zeros_like(e)
        for b in range(nx):
            source = xor(dx, GATHER[b]) if nx == 4 else b
            at = source * (bx >> l) - LOW[l] + 12
            count = h.shape[0]
            if nx == 4 and b == 3 and l == 2:
                at, count = at + jnp.where(source < 2, n2 - 5, 0), 5
            for p in range(count):
                if nx != 4:
                    value = near(rc.at[b], l, p)
                else:
                    value = far(l, p) if b == 3 else near(rb, l, p) if b == 2 else h[p]
                    if b == 1:
                        value = near(ra, l, p)
                e[at + p] = e[at + p] + value
    for e, f, l in ((e2, f2, 2), (e3, f3, 3), (e4, f4, 4)):
        start = dx * (bx >> l) - LOW[l] - REACH + 12
        for r in range(f.shape[0]):
            total = e[start + r] * taps_ref[3 * l, 0]
            for k in range(1, TAPS):
                total = total + e[start + r + k] * taps_ref[3 * l, k]
            f[r] = masked(total, r - LOW[l], bx >> l, place)
    def strips(p):
        return jnp.concatenate([ya[p], yb[p]], axis=0)

    def add_strips(p, value):
        out_ref[p, 0:8] = f0[p, 0:8] + value[0:8]
        out_ref[p, 8 : by - 8] = f0[p, 8 : by - 8]
        out_ref[p, by - 8 : by] = f0[p, by - 8 : by] + value[8:16]

    batched(tyh[...], [functools.partial(strips, p) for p in range(bx)], add_strips)

    def doubled(value):
        return jnp.concatenate(halves(value), axis=0).astype(BF16)

    row0 = [sum(padded[:l]) for l in range(LEVELS)]
    for l, f, target in ((3, f4, f3), (2, f3, f2), (1, f2, f1), (0, f1, out_ref)):
        rows, k = padded[l], 2 * padded[l + 1]
        matrix = py_ref[dy, row0[l] : row0[l] + rows, :k]
        s1, s2 = stage[2 * l], stage[2 * l + 1]
        count = f.shape[0]
        planes = [functools.partial(lambda ref, p: ref[p], f, p) for p in range(count)]
        batched(matrix, planes, functools.partial(put, s1, 0), doubled)
        pz = jnp.concatenate([pz_ref[dz, l], pz_ref[dz, l]], axis=0)
        hi, lo = halves(s1[...].reshape(count * rows, LANES))
        both = jnp.concatenate([hi.astype(BF16), lo.astype(BF16)], axis=1)
        s2[...] = mm(both, pz).reshape(count, rows, LANES)
        for r in range(target.shape[0]):
            j = r - LOW[l]
            total = None
            for kk, w in CUBIC.items():
                if (j - kk) % 2 == 0:
                    p = (j - kk) // 2 + LOW[l + 1]
                    if 0 <= p < count:
                        term = s2[p] if w == 1.0 else s2[p] * w
                        total = term if total is None else total + term
            target[r] = target[r] + masked(total, j, bx >> l, place)


def call(kernel, out_shape, args, n_smem, scratch=(), flops=0, aliases={}, hbm=(), limit=20):
    vmem, smem = pl.BlockSpec(memory_space=pltpu.VMEM), pl.BlockSpec(memory_space=pltpu.SMEM)
    anywhere = pl.BlockSpec(memory_space=pltpu.HBM)
    many = isinstance(out_shape, (tuple, list))
    return pl.pallas_call(
        kernel,
        out_shape=out_shape,
        in_specs=[
            smem if i < n_smem else anywhere if i in hbm else vmem for i in range(len(args))
        ],
        out_specs=[vmem] * len(out_shape) if many else vmem,
        scratch_shapes=scratch,
        input_output_aliases=aliases,
        cost_estimate=pl.CostEstimate(flops=flops, bytes_accessed=2**20, transcendentals=0),
        compiler_params=pltpu.CompilerParams(vmem_limit_bytes=limit * 2**20),
    )(*args)


def swaps(count, flip):
    return [(i, i ^ flip) for i in range(count)]


def middle_swaps(count):
    if count == 4:
        return swaps(count, 3)
    return [p for i in range(1, count - 1, 2) for p in ((i, i + 1), (i + 1, i))]


def per_device(charges, kernel_taps):
    nx, ny, nz = (lax.axis_size(a) for a in ("gx", "gy", "gz"))
    bx, by, bz = charges.shape
    assert bz == LANES and nx % 2 == 0 and ny % 2 == 0
    xs, ys, padded = sizes(bx), sizes(by), rows_padded(by)
    dx, dy, dz = (lax.axis_index(a) for a in ("gx", "gy", "gz"))
    taps = kernel_taps.reshape(3 * LEVELS, TAPS)
    idx = jnp.stack([dx, dy, dz]).astype(jnp.int32)

    def shape(*dims, dtype=F32):
        return jax.ShapeDtypeStruct(dims, dtype)

    def neighbours(count):
        return [(i, j) for i, j in middle_swaps(count) if abs(i - j) == 1]

    if nz == 2:
        others = (lax.ppermute(charges, "gz", swaps(2, 1)),)
    else:
        others = (lax.all_gather(charges, "gz"),)
    in_y = [0, padded[1] + 32, padded[2] + 32, 16 * ny, 16 * ny]
    w0, w, ty0, tyh, *ty = call(
        functools.partial(setup_kernel, by, ny, nz, ny * by),
        [
            shape(3 * nz * bz, LANES, dtype=BF16),
            shape(3 * nz * bz, 2 * LANES, dtype=BF16),
            shape(by, 3 * by, dtype=BF16),
            shape(16, 48, dtype=BF16),
        ]
        + [shape(padded[l], 3 * in_y[l], dtype=BF16) for l in range(1, LEVELS)],
        (taps, idx),
        2,
        flops=FLOPS,
    )
    sy = jnp.asarray(split_rows_const(ny * by, ny))
    sources = (charges, *others) if nz == 2 else others
    n34 = xs[3] + xs[4]
    face, coarse = shape(REACH, by, bz), shape(xs[1] + -(-xs[1] // 2), 8, LANES)
    plane = lambda n: pltpu.VMEM((n, by, bz), F32)
    g0, xa, xb = call(
        functools.partial(z0_kernel, nz),
        [shape(bx, by, bz), face, face],
        (idx, *sources, w0),
        1,
        flops=10**8,
    )
    xa = lax.ppermute(xa, "gx", swaps(nx, 1))
    xb = lax.ppermute(xb, "gx", neighbours(nx))
    ma, mb, mc, y1, y2, y34 = call(
        functools.partial(z_kernel, nx, nz),
        [
            coarse,
            coarse,
            shape(8, 8, LANES),
            shape(xs[1], padded[1], LANES),
            shape(xs[2], padded[2], LANES),
            shape(n34, 16, LANES),
        ],
        (idx, *sources, w, sy),
        1,
        [plane(bx), plane(bx), plane(xs[1]), plane(xs[2]), plane(xs[3])]
        + [plane(xs[1]), plane(xs[2]), plane(xs[3]), plane(xs[4])],
        flops=10**9,
    )
    ra = lax.ppermute(ma, "gy", swaps(ny, 1))
    rb = lax.ppermute(mb, "gy", middle_swaps(ny))
    rc = lax.ppermute(mc, "gy", swaps(ny, 2)) if ny == 4 else lax.all_gather(y34, "gy")
    h0 = call(conv_own_kernel, shape(bx, by, bz), (taps, g0), 1, flops=10**9)
    n1, strip = REACH + 3, shape(bx, 8, LANES)
    coarse = shape((padded[1] // 8 - 1) * n1 + -(-n1 // 2), 8, LANES)
    h0, ya, yb, ma, mb, mc, h1, h2, h3, h4 = call(
        functools.partial(mid_kernel, nx, ny),
        [shape(bx, by, bz), strip, strip, coarse, coarse, shape(16, 8, LANES)]
        + [shape(xs[l], padded[l], LANES) for l in range(1, LEVELS)],
        (taps, idx, h0, xa, xb, ra, rb, rc, y1, y2, y34, *ty),
        2,
        [pltpu.VMEM((2, REACH, by, bz), F32)],
        flops=10**9,
        aliases={2: 0},
    )
    ra = lax.ppermute(ma, "gx", swaps(nx, 1))
    rb = lax.ppermute(mb, "gx", middle_swaps(nx))
    rc = lax.ppermute(mc, "gx", swaps(nx, 2)) if nx == 4 else lax.all_gather(ma, "gx")
    ya = lax.ppermute(ya, "gy", swaps(ny, 1))
    yb = lax.ppermute(yb, "gy", neighbours(ny))
    f0, f1 = call(
        last_own_kernel,
        [shape(bx, by, bz), shape(xs[1], padded[1], LANES)],
        (taps, h0, h1, ty0),
        1,
        flops=10**9,
    )
    py = jnp.asarray(prolong_rows_const(ny * by, ny))
    pz = jnp.asarray(prolong_lanes_const(nz * bz, nz))
    buf = lambda n, rows: pltpu.VMEM((n, rows, LANES), F32)
    return call(
        functools.partial(last_kernel, nx),
        shape(bx, by, bz),
        (taps, idx, f0, f1, h2, h3, h4, ya, yb, ra, rb, rc, tyh, py, pz),
        2,
        [pltpu.VMEM((2, REACH + 3, padded[1], LANES), F32)]
        + [buf((nx * bx >> l) + 24, padded[l]) for l in range(2, LEVELS)]
        + [buf(xs[l], padded[l]) for l in range(1, LEVELS)]
        + [buf(xs[l + 1], padded[l]) for l in range(LEVELS - 1) for _ in range(2)],
        flops=10**9,
    )


def solution(mesh):
    in_specs = (P("gx", "gy", "gz"), P())
    out_specs = P("gx", "gy", "gz")
    return jax.shard_map(
        per_device, mesh=mesh, in_specs=in_specs, out_specs=out_specs, check_vma=False
    )
```

```python
import functools

import jax
import jax.numpy as jnp
import numpy as np
from jax import lax
from jax.experimental import pallas as pl
from jax.experimental.pallas import tpu as pltpu
from jax.sharding import PartitionSpec as P

LEVELS = 5
TAPS = 17
REACH = 8
LANES = 128
CUBIC = {-3: -0.0625, -1: 0.5625, 0: 1.0, 1: 0.5625, 3: -0.0625}
LOW = (0, 1, 2, 2, 2)
HIGH = (0, 2, 3, 3, 3)
F32 = jnp.float32
BF16 = jnp.bfloat16
GATHER = (0, 1, 3, 2)
FLOPS = 10**9


def sizes(block):
    return [block // 2**l + LOW[l] + HIGH[l] for l in range(LEVELS)]


def pad8(n):
    return -(-n // 8) * 8


def pad16(n):
    return -(-n // 16) * 16


def restrictions(whole):
    composite, out = np.eye(whole), [np.eye(whole)]
    for _ in range(1, LEVELS):
        fine = composite.shape[0]
        step = np.zeros((fine // 2, fine))
        for i in range(fine // 2):
            for k, w in CUBIC.items():
                if 0 <= 2 * i + k < fine:
                    step[i, 2 * i + k] = w
        composite = step @ composite
        out.append(composite)
    return out


def rows_padded(block):
    n = sizes(block)
    return [block] + [max(16, pad8(n[l])) for l in range(1, LEVELS)]


def lane_offsets(block):
    n = sizes(block)
    return [0, 0, n[1], n[1] + n[2], n[1] + n[2]]


def split_rows_const(whole, count):
    block = whole // count
    full, n, padded = restrictions(whole), sizes(block), rows_padded(block)
    out = np.zeros((count, sum(padded[1:]), block), np.float32)
    for d in range(count):
        row0 = 0
        for l in range(1, LEVELS):
            for r in range(n[l]):
                g = d * (block >> l) - LOW[l] + r
                if 0 <= g < whole >> l:
                    out[d, row0 + r] = full[l][g, d * block : (d + 1) * block]
            row0 += padded[l]
    hi = out.astype(BF16)
    lo = (out - hi.astype(np.float32)).astype(BF16)
    return np.concatenate([hi, hi, lo], axis=2)


def prolong_entries(whole, count, d, l):
    block = whole // count
    n = sizes(block)
    for i in range(n[l]):
        g_out = d * (block >> l) - LOW[l] + i
        for j in range(n[l + 1]):
            g_in = d * (block >> (l + 1)) - LOW[l + 1] + j
            ok = 0 <= g_out < whole >> l and 0 <= g_in < whole >> (l + 1)
            if ok and g_out - 2 * g_in in CUBIC:
                yield i, j, CUBIC[g_out - 2 * g_in]


def prolong_rows_const(whole, count):
    padded = rows_padded(whole // count)
    out = np.zeros((count, sum(padded[:4]), 2 * padded[1]), np.float32)
    for d in range(count):
        row0 = 0
        for l in range(LEVELS - 1):
            for i, j, w in prolong_entries(whole, count, d, l):
                out[d, row0 + i, j] = w
                out[d, row0 + i, padded[l + 1] + j] = w
            row0 += padded[l]
    return out.astype(BF16)


def prolong_lanes_const(whole, count):
    off = lane_offsets(whole // count)
    out = np.zeros((count, LEVELS - 1, LANES, LANES), np.float32)
    for d in range(count):
        for l in range(LEVELS - 1):
            for i, j, w in prolong_entries(whole, count, d, l):
                out[d, l, off[l + 1] + j, off[l] + i] = w
    return out.astype(BF16)


def toeplitz(taps_ref, row, g_in, g_out, mask):
    diff = g_in - g_out + REACH
    value = jnp.zeros(diff.shape, F32)
    for k in range(TAPS):
        value = jnp.where(diff == k, taps_ref[row, k], value)
    return jnp.where(mask, value, 0.0)


def iota(shape, axis):
    return lax.broadcasted_iota(jnp.int32, shape, axis)


def xor(a, b):
    return jnp.bitwise_xor(a, jnp.int32(b))


def halves(value):
    scaled = value * 65537.0
    hi = scaled - (scaled - value)
    return hi, value - hi


def mm(a, b):
    return jnp.dot(a, b, preferred_element_type=F32)


def spread(fine, coarse):
    k = fine - 2 * iota(fine.shape, 1)
    step = jnp.where(k == 0, 1.0, 0.0)
    step = jnp.where((k == 1) | (k == -1), 0.5625, step)
    step = jnp.where((k == 3) | (k == -3), -0.0625, step).astype(BF16)
    hi, lo = halves(coarse)
    low, rest = halves(lo)
    total = mm(step, rest.astype(BF16)) + mm(step, low.astype(BF16))
    return total + mm(step, hi.astype(BF16))


def setup_kernel(
    nz, taps_ref, idx_ref, w0_ref, w_ref
):
    bz = LANES
    whole_z = nz * bz
    dz = idx_ref[2]
    n, off = sizes(bz), lane_offsets(bz)
    below = None
    for l in range(LEVELS - 1, 0, -1):
        rows = whole_z >> l
        col = iota((rows, LANES), 1)
        g_out = dz * (bz >> l) - LOW[l] + col - off[l]
        mask = (col >= off[l]) & (col < off[l] + n[l]) & (g_out >= 0) & (g_out < rows)
        here = toeplitz(taps_ref, 3 * l + 2, iota((rows, LANES), 0), g_out, mask)
        none = jnp.zeros((rows, LANES), F32)
        here = jnp.concatenate([none, here] if l == LEVELS - 1 else [here, none], axis=1)
        if below is not None:
            here = here + spread(iota((rows, rows // 2), 0), below)
        below = here
    order = [dz, 1 - dz] if nz == 2 else list(range(nz))

    def store_rows(ref, j, value):
        hi, lo = halves(value)
        ref[j * bz : (j + 1) * bz] = hi.astype(BF16)
        ref[(nz + j) * bz : (nz + j + 1) * bz] = hi.astype(BF16)
        ref[(2 * nz + j) * bz : (2 * nz + j + 1) * bz] = lo.astype(BF16)

    row, col = iota((bz, bz), 0), iota((bz, bz), 1)
    if nz == 2:
        hi, lo = halves(toeplitz(taps_ref, 2, row, col, row >= 0))
        w0_ref[0:bz] = hi.astype(BF16)
        w0_ref[bz : 2 * bz] = hi.astype(BF16)
        w0_ref[2 * bz : 3 * bz] = lo.astype(BF16)
        hi, lo = halves(toeplitz(taps_ref, 2, (1 - 2 * dz) * bz + row, col, row >= 0))
        w0_ref[3 * bz : 4 * bz] = hi.astype(BF16)
        w0_ref[4 * bz : 5 * bz] = hi.astype(BF16)
        w0_ref[5 * bz : 6 * bz] = lo.astype(BF16)
    else:
        for j in range(nz):
            g_in, g_out = j * bz + row, dz * bz + col
            store_rows(w0_ref, j, toeplitz(taps_ref, 2, g_in, g_out, g_out >= 0))
    for j, source in enumerate(order):
        store_rows(w_ref, j, spread(source * bz + iota((bz, whole_z // 2), 0), below))


def y_matrices(by, ny, whole_y, taps_ref, idx_ref, ty0_ref, tyh_ref, *ty_refs):
    dy = idx_ref[1]
    even = (dy % 2) == 0
    sizes_y, padded = sizes(by), rows_padded(by)

    def column(shape):
        k = shape[1] // 3
        j = iota(shape, 1)
        return k, jnp.where(j >= 2 * k, j - 2 * k, jnp.where(j >= k, j - k, j))

    def store(ref, k, value):
        hi, lo = halves(value)
        ref[...] = jnp.where(iota(ref.shape, 1) < 2 * k, hi, lo).astype(BF16)

    def windows(l, j, own, window):
        block = by >> l
        right = (dy + 1) * block - LOW[l]
        left = (dy - 1) * block - LOW[l] + padded[l] - window
        base_a = jnp.where(even, right, left)
        base_b = jnp.where(even, left, right)
        second = jnp.where(j < own + window, base_a + j - own, base_b + j - own - window)
        return jnp.where(j < own, dy * block - LOW[l] + j, second)

    k, j = column(ty0_ref.shape)
    i = iota(ty0_ref.shape, 0)
    store(ty0_ref, k, toeplitz(taps_ref, 1, j, i, i >= 0))
    k, j = column(tyh_ref.shape)
    i = iota(tyh_ref.shape, 0)
    i = dy * by + jnp.where(i < 8, i, i + by - 16)
    g_in = windows(0, j, 0, 8)
    store(tyh_ref, k, toeplitz(taps_ref, 1, g_in, i, (g_in >= 0) & (g_in < whole_y)))
    for l, ty_ref in enumerate(ty_refs, 1):
        block = by >> l
        k, j = column(ty_ref.shape)
        if l < 3:
            g_in = windows(l, j, padded[l], 16)
        else:
            g_in = j
            for b in range(ny):
                source = xor(dy, GATHER[b]) if ny == 4 else b
                here = (j >= b * 16) & (j < (b + 1) * 16)
                g_in = jnp.where(here, source * block - LOW[l] + j - b * 16, g_in)
        i = iota(ty_ref.shape, 0)
        g_out = dy * block - LOW[l] + i
        mask = (i < sizes_y[l]) & (g_out >= 0) & (g_out < whole_y >> l)
        mask = mask & (g_in >= 0) & (g_in < whole_y >> l)
        store(ty_ref, k, toeplitz(taps_ref, 3 * l + 1, g_in, g_out, mask))


def masked(value, index, block, place):
    if 0 <= index < block:
        return value
    cell = place[0] * block + index
    inside = (cell >= 0) & (cell < place[1] * block)
    return value * jnp.where(inside, 1.0, 0.0).astype(F32)


def restrict_planes(src, dst, level, block_out, place):
    lo_in, count_in = LOW[level - 1], src.shape[0]
    for r in range(dst.shape[0]):
        i = r - LOW[level]
        total = None
        for k, w in CUBIC.items():
            p = 2 * i + k + lo_in
            if 0 <= p < count_in:
                term = src[p] if w == 1.0 else src[p] * w
                total = term if total is None else total + term
        dst[r] = masked(total, i, block_out, place)


def stacked(value):
    hi, lo = halves(value)
    return jnp.concatenate([hi, lo, hi], axis=0).astype(BF16)


def y_slots(n1, n2, n3, n4):
    half = -(-n1 // 2)
    ones = [[(p, 0)] for p in range(n1)]
    ones += [[(p, 1)] + ([(p + half, 1)] if p + half < n1 else []) for p in range(half)]
    twos = [(p, 0) for p in range(n2)] + [(p, 1) for p in range(n2)]
    threes = [[(p, 0)] for p in range(n3 + n4)]
    threes += [[(p, 1)] + ([(n3 + p, 1)] if p < n4 else []) for p in range(n3)]
    assert max(len(twos), len(threes)) <= len(ones)
    return ones, twos, threes


def put(ref, first, p, value):
    ref[first + p] = value


def batched(matrix, values, store, form=stacked, group=4):
    for p in range(0, len(values), group):
        some = values[p : p + group]
        out = mm(matrix, jnp.concatenate([form(v()) for v in some], axis=1))
        for q in range(len(some)):
            store(p + q, out[:, q * LANES : (q + 1) * LANES])


def z_rows(src, nz, planes, count):
    if nz == 2:
        blocks = [s[planes] for s in src]
    else:
        blocks = [src[0][s, planes] for s in range(nz)]
    his, los = zip(*[halves(b.reshape(count * b.shape[1], b.shape[2])) for b in blocks])
    return jnp.concatenate([h.astype(BF16) for h in his + los + his], axis=1)


def z0_own_kernel(q_ref, w_ref, g_ref):
    bx, by, bz = q_ref.shape
    chunk = 8

    def step(c, carry):
        planes = pl.ds(c * chunk, chunk)
        hi, lo = halves(q_ref[planes].reshape(chunk * by, bz))
        lhs = jnp.concatenate([hi.astype(BF16), lo.astype(BF16)], axis=1)
        g_ref[planes] = mm(lhs, w_ref[0 : 2 * bz, :]).reshape(chunk, by, bz)
        return carry

    lax.fori_loop(0, bx // chunk, step, 0, unroll=4)


def z0_rest_kernel(idx_ref, g_in, q_ref, other_ref, w_ref, g0_ref, xa_ref, xb_ref):
    bx, by, bz = q_ref.shape
    chunk = 8

    def step(c, carry):
        planes = pl.ds(c * chunk, chunk)
        own = halves(q_ref[planes].reshape(chunk * by, bz))[0]
        hi, lo = halves(other_ref[planes].reshape(chunk * by, bz))
        lhs = jnp.concatenate([v.astype(BF16) for v in (own, hi, lo, hi)], axis=1)
        out = mm(lhs, w_ref[2 * bz :, :]).reshape(chunk, by, bz)
        g0_ref[planes] = g_in[planes] + out
        return carry

    lax.fori_loop(0, bx // chunk, step, 0, unroll=4)
    even = (idx_ref[0] % 2) == 0
    xa_ref[...] = g0_ref[pl.ds(jnp.where(even, bx - REACH, 0), REACH)]
    xb_ref[...] = g0_ref[pl.ds(jnp.where(even, 0, bx - REACH), REACH)]


def z0_kernel(nz, idx_ref, *refs):
    src = refs[: (2 if nz == 2 else 1)]
    w_ref, g0_ref, xa_ref, xb_ref = refs[len(src) :]
    bx, by, bz = g0_ref.shape
    chunk = 8

    def step(c, carry):
        planes = pl.ds(c * chunk, chunk)
        out = mm(z_rows(src, nz, planes, chunk), w_ref[...])
        g0_ref[planes] = out.reshape(chunk, by, bz)
        return carry

    lax.fori_loop(0, bx // chunk, step, 0, unroll=4)
    even = (idx_ref[0] % 2) == 0
    xa_ref[...] = g0_ref[pl.ds(jnp.where(even, bx - REACH, 0), REACH)]
    xb_ref[...] = g0_ref[pl.ds(jnp.where(even, 0, bx - REACH), REACH)]


def z_kernel(nx, nz, idx_ref, *refs):
    src = refs[: (2 if nz == 2 else 1)]
    w_ref, sy_ref, ma_ref, mb_ref, mc_ref, y1_ref, y2_ref, y34_ref = refs[
        len(src) : len(src) + 8
    ]
    g1, g2, x1, x2, x3, t1, t2, t3, x4 = refs[len(src) + 8 :]
    bx, by, bz = g1.shape
    dx, dy = idx_ref[0], idx_ref[1]
    chunk = 8

    def step(c, carry):
        planes = pl.ds(c * chunk, chunk)
        out = mm(z_rows(src, nz, planes, chunk), w_ref[...])
        g1[planes] = out[:, :LANES].reshape(chunk, by, bz)
        g2[planes] = out[:, LANES:].reshape(chunk, by, bz)
        return carry

    lax.fori_loop(0, bx // chunk, step, 0, unroll=4)
    place = (dx, nx)
    for source, first, second, third, fourth in (
        (g1, x1, x2, x3, None),
        (g2, t1, t2, t3, x4),
    ):
        restrict_planes(source, first, 1, bx >> 1, place)
        restrict_planes(first, second, 2, bx >> 2, place)
        restrict_planes(second, third, 3, bx >> 3, place)
        if fourth is not None:
            restrict_planes(third, fourth, 4, bx >> 4, place)
    padded = rows_padded(by)
    n3 = x3.shape[0]
    row0 = 0
    for l, (source, target, first) in enumerate(
        ((x1, y1_ref, 0), (x2, y2_ref, 0), (x3, y34_ref, 0), (x4, y34_ref, n3)), 1
    ):
        sy = sy_ref[dy, row0 : row0 + padded[l], :]
        planes = [functools.partial(lambda ref, p: ref[p], source, p) for p in range(source.shape[0])]
        batched(sy, planes, functools.partial(put, target, first))
        row0 += padded[l]
    off = lane_offsets(bz)
    even = (dy % 2) == 0
    n1, n2 = y1_ref.shape[0], y2_ref.shape[0]
    ones, twos, threes = y_slots(n1, n2, n3, y34_ref.shape[0] - n3)
    lane8, row8 = iota((8, LANES), 1), iota((8, LANES), 0)
    for m_ref, rightward in ((ma_ref, even), (mb_ref, jnp.logical_not(even))):
        start1 = pl.multiple_of(jnp.where(rightward, padded[1] - 16, 0), 8)
        start2 = pl.multiple_of(jnp.where(rightward, padded[2] - 16, 0), 8)

        def first(p, b):
            return y1_ref[p, pl.ds(start1 + 8 * b, 8), :]

        for s in range(m_ref.shape[0]):
            value = first(*ones[s][0])
            if len(ones[s]) == 2:
                value = jnp.where(row8 < 4, value, pltpu.roll(first(*ones[s][1]), 4, 0))
            if s < len(twos):
                p, b = twos[s]
                value = jnp.where(lane8 < off[2], value, y2_ref[p, pl.ds(start2 + 8 * b, 8), :])
            if s < len(threes):
                p, b = threes[s][0]
                three = y34_ref[p, 8 * b : 8 * b + 8, :]
                if len(threes[s]) == 2:
                    p, b = threes[s][1]
                    four = pltpu.roll(y34_ref[p, 8 * b : 8 * b + 8, :], 5, 0)
                    three = jnp.where(row8 < 5, three, four)
                value = jnp.where(lane8 < off[3], value, three)
            m_ref[s] = value
    lane = iota((16, LANES), 1)
    for p in range(4):
        value = y34_ref[p]
        for g in range(1, 4):
            moved = pltpu.roll(y34_ref[4 * g + p], LANES - 32 * g, 1)
            value = jnp.where(lane >= off[3] - 32 * (g - 1), value, moved)
        mc_ref[2 * p : 2 * p + 2] = value.reshape(2, 8, LANES)


def conv_own_kernel(ny, taps_ref, idx_ref, g_ref, h_ref, *ty_refs):
    bx, by, bz = g_ref.shape
    y_matrices(by, ny, ny * by, taps_ref, idx_ref, *ty_refs)

    def rows(t, carry):
        at = pl.ds(pl.multiple_of(t * 8, 8), 8)
        for i in range(bx):
            total = None
            for k in range(TAPS):
                j = i + k - REACH
                if 0 <= j < bx:
                    term = g_ref[j, at, :] * taps_ref[0, k]
                    total = term if total is None else total + term
            h_ref[i, at, :] = total
        return carry

    lax.fori_loop(0, by // 8, rows, 0)


def x_slots(n1, n2, rows1, rows2):
    whole = rows1 - 1
    free = [whole * p + b for p in range(n1) for b in range(rows2, whole)]
    twos = {}
    for q in range(n2):
        for b in range(rows2):
            slot = whole * q + b if q < n1 else free[(q - n1) * rows2 + b]
            twos[slot] = (q, b)
    return twos


def mid_kernel(nx, ny, taps_ref, idx_ref, h_in, xa, xb, ra, rb, rc, y1, y2, y34, *refs):
    ty1, ty2, ty3, ty4, h0, ya_ref, yb_ref, ma_ref, mb_ref, mc_ref, h1, h2, h3, h4, halo = refs
    bx, by, bz = h0.shape
    dx, dy = idx_ref[0], idx_ref[1]
    off = lane_offsets(bz)

    ones, twos, threes = y_slots(y1.shape[0], y2.shape[0], h3.shape[0], h4.shape[0])
    row8 = iota((8, LANES), 0)
    found = {}
    for l, slots in ((1, ones), (2, [[v] for v in twos]), (3, threes)):
        for s, held in enumerate(slots):
            for place, (p, b) in enumerate(held):
                used = 8 if b == 0 else {1: 3, 2: 5}.get(l, 5 if p < h3.shape[0] else 1)
                found[l, p, b] = (s, 0 if place == 0 else 4 if l == 1 else 3, used)

    def block(ref, l, p, b):
        s, turn, used = found[l, p, b]
        value = ref[s] if turn == 0 else pltpu.roll(ref[s], turn, 0)
        return value if used == 8 else jnp.where(row8 < used, value, 0.0)

    def got(ref, l, p):
        return jnp.concatenate([block(ref, l, p, 0), block(ref, l, p, 1)], axis=0)

    def joined(own, l, p):
        return jnp.concatenate([own[p], got(ra, l, p), got(rb, l, p)], axis=0)

    def gathered(p):
        if ny == 4:
            far = rc[2 * (p % 4) : 2 * (p % 4) + 2].reshape(16, LANES)
            if p >= 4:
                far = pltpu.roll(far, 32 * (p // 4), 1)
            parts = [y34[p], got(ra, 3, p), got(rb, 3, p), far]
        else:
            parts = [rc[s, p] for s in range(ny)]
        return jnp.concatenate(parts, axis=0)

    for own, ty, h, l in ((y1, ty1, h1, 1), (y2, ty2, h2, 2)):
        planes = [functools.partial(joined, own, l, p) for p in range(h.shape[0])]
        batched(ty[...], planes, functools.partial(put, h, 0))
    n3 = h3.shape[0]
    planes = [functools.partial(gathered, p) for p in range(y34.shape[0])]
    batched(ty3[...], planes[:n3], functools.partial(put, h3, 0))
    batched(ty4[...], planes[n3:], functools.partial(put, h4, 0))

    even = (dx % 2) == 0
    n2, n1 = h2.shape[0], REACH + 3
    each = h1.shape[1] // 8 - 1
    twos = x_slots(n1, n2, each + 1, h2.shape[1] // 8)
    half = -(-n1 // 2)
    lane = iota((8, LANES), 1)

    def block34(pp, b):
        ref, p = (h3, pp) if pp < n3 else (h4, pp - n3)
        return ref[p, 8 * b : 8 * b + 8, :]

    for m_ref, rightward in ((ma_ref, even), (mb_ref, jnp.logical_not(even))):
        start1 = jnp.where(rightward, (bx >> 1) - REACH, 0)
        for p in range(n1):
            for b in range(each):
                value = h1[start1 + p, 8 * b : 8 * b + 8, :]
                if each * p + b in twos:
                    q, bb = twos[each * p + b]
                    value = jnp.where(lane < off[2], value, h2[q, 8 * bb : 8 * bb + 8, :])
                if b < 2 and p < n3:
                    value = jnp.where(lane < off[3], value, block34(p, b))
                elif 2 <= b < 4 and p < h4.shape[0]:
                    value = jnp.where(lane < off[3], value, block34(n3 + p, b - 2))
                m_ref[each * p + b] = value
        for p in range(half):
            value = h1[start1 + p, 8 * each : 8 * each + 8, :]
            if p + half < n1:
                other = pltpu.roll(h1[start1 + p + half, 8 * each : 8 * each + 8, :], 4, 0)
                value = jnp.where(row8 < 4, value, other)
            m_ref[each * n1 + p] = value
    start2 = jnp.where(dx < 2, n2 - 5, 0)
    rows2 = h2.shape[1] // 8
    for s in range(16):
        near = block34(s // 2, s % 2)
        far = pltpu.roll(block34((16 + s) // 2, s % 2), LANES - 32, 1)
        value = jnp.where(lane >= off[3], near, far)
        if s < 5 * rows2:
            b = s % rows2
            two = pltpu.roll(h2[start2 + s // rows2, 8 * b : 8 * b + 8, :], 64, 1)
            value = jnp.where(lane >= off[3] - 32, value, two)
        mc_ref[s] = value

    halo[jnp.where(even, 1, 0)] = xa[...]
    halo[jnp.where(even, 0, 1)] = xb[...]

    def rows(t, carry):
        at = pl.ds(pl.multiple_of(t * 8, 8), 8)
        for i in range(REACH):
            low, high = h_in[i, at, :], h_in[bx - REACH + i, at, :]
            for m in range(i, REACH):
                low = low + halo[0, m, at, :] * taps_ref[0, m - i]
            for m in range(i + 1):
                high = high + halo[1, m, at, :] * taps_ref[0, 2 * REACH + m - i]
            h0[i, at, :] = low
            h0[bx - REACH + i, at, :] = high
        return carry

    lax.fori_loop(0, by // 8, rows, 0)
    even = (dy % 2) == 0
    for m_ref, rightward in ((ya_ref, even), (yb_ref, jnp.logical_not(even))):
        m_ref[...] = h0[:, pl.ds(pl.multiple_of(jnp.where(rightward, by - 8, 0), 8), 8), :]


def last_own_kernel(taps_ref, h0, h1, ty0, f0, f1):
    bx, by, bz = h0.shape

    def planes(c, carry):
        some = [functools.partial(lambda p: h0[p], 4 * c + q) for q in range(4)]
        batched(ty0[...], some, lambda q, value: put(f0, 4 * c, q, value))
        return carry

    lax.fori_loop(0, bx // 4, planes, 0, unroll=4)
    count = h1.shape[0]
    for i in range(count):
        total = None
        for k in range(TAPS):
            j = i + k - REACH
            if 0 <= j < count:
                term = h1[j] * taps_ref[3, k]
                total = term if total is None else total + term
        f1[i] = total


def last_kernel(nx, taps_ref, idx_ref, f0, f1o, h2, h3, h4, ya, yb, ra, rb, rc, *refs):
    tyh, py_ref, pz_ref, result, side, e2, e3, e4, f1, f2, f3, f4, out_ref, sem = refs[:14]
    stage = refs[14:]
    group = result.shape[0] // sem.shape[0]
    copies = [
        pltpu.make_async_copy(
            out_ref.at[c * group : (c + 1) * group], result.at[c * group : (c + 1) * group], sem.at[c]
        )
        for c in range(sem.shape[0])
    ]
    bx, by, bz = f0.shape
    dx, dy, dz = idx_ref[0], idx_ref[1], idx_ref[2]
    even = (dx % 2) == 0
    place = (dx, nx)
    padded = rows_padded(by)
    each = f1o.shape[1] // 8 - 1
    n1, n2, n3, n4 = REACH + 3, h2.shape[0], h3.shape[0], h4.shape[0]
    rows2 = h2.shape[1] // 8
    twos = {v: k for k, v in x_slots(n1, n2, each + 1, rows2).items()}
    half = -(-n1 // 2)

    partner = jnp.where(even, dx > 0, dx < nx - 1)
    okay = jnp.where(partner, 1.0, 0.0).astype(F32)
    for ref, place_of, scale in ((ra, jnp.where(even, 1, 0), None), (rb, jnp.where(even, 0, 1), okay)):
        for p in range(n1):
            final = ref[each * n1 + p % half]
            final = pltpu.roll(final, 4, 0) if p >= half else final
            value = jnp.concatenate(
                [ref[each * p : each * p + each].reshape(8 * each, LANES), final], axis=0
            )
            side[place_of, p] = value if scale is None else value * scale
    block = bx >> 1
    for r in range(f1.shape[0]):
        total, i = f1o[r], r - LOW[1]
        for m in range(n1):
            for s, j in ((0, m - REACH - 1), (1, block - 1 + m)):
                k = j - i + REACH
                if 0 <= k < TAPS:
                    total = total + side[s, m] * taps_ref[3, k]
        f1[r] = masked(total, i, block, place)

    def near(ref, l, p):
        if l == 2:
            return jnp.concatenate(
                [ref[twos[p, b]] for b in range(rows2)], axis=0
            )
        first = p * each + (0 if l == 3 else 2)
        return ref[first : first + 2].reshape(16, LANES)

    def far(l, p):
        if l == 2:
            value = rc[p * rows2 : (p + 1) * rows2].reshape(8 * rows2, LANES)
            return pltpu.roll(value, 64, 1)
        first = 2 * p if l == 3 else 2 * (n3 + p)
        value = rc[first % 16 : first % 16 + 2].reshape(16, LANES)
        return value if first < 16 else pltpu.roll(value, 32, 1)

    for e, h, l in ((e2, h2, 2), (e3, h3, 3), (e4, h4, 4)):
        e[...] = jnp.zeros_like(e)
        for b in range(nx):
            source = xor(dx, GATHER[b]) if nx == 4 else b
            at = source * (bx >> l) - LOW[l] + 12
            count = h.shape[0]
            if nx == 4 and b == 3 and l == 2:
                at, count = at + jnp.where(source < 2, n2 - 5, 0), 5
            for p in range(count):
                if nx != 4:
                    value = near(rc.at[b], l, p)
                else:
                    value = far(l, p) if b == 3 else near(rb, l, p) if b == 2 else h[p]
                    if b == 1:
                        value = near(ra, l, p)
                e[at + p] = e[at + p] + value
    for e, f, l in ((e2, f2, 2), (e3, f3, 3), (e4, f4, 4)):
        start = dx * (bx >> l) - LOW[l] - REACH + 12
        for r in range(f.shape[0]):
            total = e[start + r] * taps_ref[3 * l, 0]
            for k in range(1, TAPS):
                total = total + e[start + r + k] * taps_ref[3 * l, k]
            f[r] = masked(total, r - LOW[l], bx >> l, place)
    def strips(p):
        return jnp.concatenate([ya[p], yb[p]], axis=0)

    def add_strips(p, value):
        out_ref[p, 0:8] = f0[p, 0:8] + value[0:8]
        out_ref[p, 8 : by - 8] = f0[p, 8 : by - 8]
        out_ref[p, by - 8 : by] = f0[p, by - 8 : by] + value[8:16]

    batched(tyh[...], [functools.partial(strips, p) for p in range(bx)], add_strips)

    def doubled(value):
        return jnp.concatenate(halves(value), axis=0).astype(BF16)

    row0 = [sum(padded[:l]) for l in range(LEVELS)]
    for l, f, target in ((3, f4, f3), (2, f3, f2), (1, f2, f1), (0, f1, out_ref)):
        rows, k = padded[l], 2 * padded[l + 1]
        matrix = py_ref[dy, row0[l] : row0[l] + rows, :k]
        s1, s2 = stage[2 * l], stage[2 * l + 1]
        count = f.shape[0]
        planes = [functools.partial(lambda ref, p: ref[p], f, p) for p in range(count)]
        batched(matrix, planes, functools.partial(put, s1, 0), doubled)
        pz = jnp.concatenate([pz_ref[dz, l], pz_ref[dz, l]], axis=0)
        hi, lo = halves(s1[...].reshape(count * rows, LANES))
        both = jnp.concatenate([hi.astype(BF16), lo.astype(BF16)], axis=1)
        s2[...] = mm(both, pz).reshape(count, rows, LANES)
        for r in range(target.shape[0]):
            j = r - LOW[l]
            total = None
            for kk, w in CUBIC.items():
                if (j - kk) % 2 == 0:
                    p = (j - kk) // 2 + LOW[l + 1]
                    if 0 <= p < count:
                        term = s2[p] if w == 1.0 else s2[p] * w
                        total = term if total is None else total + term
            target[r] = target[r] + masked(total, j, bx >> l, place)
            if l == 0 and (r + 1) % group == 0:
                copies[r // group].start()
    for copy in copies:
        copy.wait()


def call(kernel, out_shape, args, n_smem, scratch=(), flops=0, aliases={}, limit=20, out_hbm=False):
    vmem, smem = pl.BlockSpec(memory_space=pltpu.VMEM), pl.BlockSpec(memory_space=pltpu.SMEM)
    anywhere = pl.BlockSpec(memory_space=pltpu.HBM)
    many = isinstance(out_shape, (tuple, list))
    return pl.pallas_call(
        kernel,
        out_shape=out_shape,
        in_specs=[smem] * n_smem + [vmem] * (len(args) - n_smem),
        out_specs=[vmem] * len(out_shape) if many else anywhere if out_hbm else vmem,
        scratch_shapes=scratch,
        input_output_aliases=aliases,
        cost_estimate=pl.CostEstimate(flops=flops, bytes_accessed=2**20, transcendentals=0),
        compiler_params=pltpu.CompilerParams(vmem_limit_bytes=limit * 2**20),
    )(*args)


def swaps(count, flip):
    return [(i, i ^ flip) for i in range(count)]


def middle_swaps(count):
    if count == 4:
        return swaps(count, 3)
    return [p for i in range(1, count - 1, 2) for p in ((i, i + 1), (i + 1, i))]


def per_device(charges, kernel_taps):
    nx, ny, nz = (lax.axis_size(a) for a in ("gx", "gy", "gz"))
    bx, by, bz = charges.shape
    assert bz == LANES and nx % 2 == 0 and ny % 2 == 0
    xs, ys, padded = sizes(bx), sizes(by), rows_padded(by)
    dx, dy, dz = (lax.axis_index(a) for a in ("gx", "gy", "gz"))
    taps = kernel_taps.reshape(3 * LEVELS, TAPS)
    idx = jnp.stack([dx, dy, dz]).astype(jnp.int32)

    def shape(*dims, dtype=F32):
        return jax.ShapeDtypeStruct(dims, dtype)

    def neighbours(count):
        return [(i, j) for i, j in middle_swaps(count) if abs(i - j) == 1]

    if nz == 2:
        others = (lax.ppermute(charges, "gz", swaps(2, 1)),)
    else:
        others = (lax.all_gather(charges, "gz"),)
    in_y = [0, padded[1] + 32, padded[2] + 32, 16 * ny, 16 * ny]
    w0, w = call(
        functools.partial(setup_kernel, nz),
        [
            shape(3 * nz * bz, LANES, dtype=BF16),
            shape(3 * nz * bz, 2 * LANES, dtype=BF16),
        ],
        (taps, idx),
        2,
        flops=FLOPS,
    )
    sy = jnp.asarray(split_rows_const(ny * by, ny))
    sources = (charges, *others) if nz == 2 else others
    n34 = xs[3] + xs[4]
    face, coarse = shape(REACH, by, bz), shape(xs[1] + -(-xs[1] // 2), 8, LANES)
    plane = lambda n: pltpu.VMEM((n, by, bz), F32)
    if nz == 2:
        g0 = call(z0_own_kernel, shape(bx, by, bz), (charges, w0), 0, flops=FLOPS)
        g0, xa, xb = call(
            z0_rest_kernel,
            [shape(bx, by, bz), face, face],
            (idx, g0, *sources, w0),
            1,
            flops=10**8,
            aliases={1: 0},
        )
    else:
        g0, xa, xb = call(
            functools.partial(z0_kernel, nz),
            [shape(bx, by, bz), face, face],
            (idx, *sources, w0),
            1,
            flops=10**8,
        )
    xa = lax.ppermute(xa, "gx", swaps(nx, 1))
    xb = lax.ppermute(xb, "gx", neighbours(nx))
    ma, mb, mc, y1, y2, y34 = call(
        functools.partial(z_kernel, nx, nz),
        [
            coarse,
            coarse,
            shape(8, 8, LANES),
            shape(xs[1], padded[1], LANES),
            shape(xs[2], padded[2], LANES),
            shape(n34, 16, LANES),
        ],
        (idx, *sources, w, sy),
        1,
        [plane(bx), plane(bx), plane(xs[1]), plane(xs[2]), plane(xs[3])]
        + [plane(xs[1]), plane(xs[2]), plane(xs[3]), plane(xs[4])],
        flops=10**9,
    )
    ra = lax.ppermute(ma, "gy", swaps(ny, 1))
    rb = lax.ppermute(mb, "gy", middle_swaps(ny))
    rc = lax.ppermute(mc, "gy", swaps(ny, 2)) if ny == 4 else lax.all_gather(y34, "gy")
    h0, ty0, tyh, *ty = call(
        functools.partial(conv_own_kernel, ny),
        [
            shape(bx, by, bz),
            shape(by, 3 * by, dtype=BF16),
            shape(16, 48, dtype=BF16),
        ]
        + [shape(padded[l], 3 * in_y[l], dtype=BF16) for l in range(1, LEVELS)],
        (taps, idx, g0),
        2,
        flops=10**9,
    )
    n1, strip = REACH + 3, shape(bx, 8, LANES)
    coarse = shape((padded[1] // 8 - 1) * n1 + -(-n1 // 2), 8, LANES)
    h0, ya, yb, ma, mb, mc, h1, h2, h3, h4 = call(
        functools.partial(mid_kernel, nx, ny),
        [shape(bx, by, bz), strip, strip, coarse, coarse, shape(16, 8, LANES)]
        + [shape(xs[l], padded[l], LANES) for l in range(1, LEVELS)],
        (taps, idx, h0, xa, xb, ra, rb, rc, y1, y2, y34, *ty),
        2,
        [pltpu.VMEM((2, REACH, by, bz), F32)],
        flops=10**9,
        aliases={2: 0},
    )
    ra = lax.ppermute(ma, "gx", swaps(nx, 1))
    rb = lax.ppermute(mb, "gx", middle_swaps(nx))
    rc = lax.ppermute(mc, "gx", swaps(nx, 2)) if nx == 4 else lax.all_gather(ma, "gx")
    ya = lax.ppermute(ya, "gy", swaps(ny, 1))
    yb = lax.ppermute(yb, "gy", neighbours(ny))
    f0, f1 = call(
        last_own_kernel,
        [shape(bx, by, bz), shape(xs[1], padded[1], LANES)],
        (taps, h0, h1, ty0),
        1,
        flops=10**9,
    )
    py = jnp.asarray(prolong_rows_const(ny * by, ny))
    pz = jnp.asarray(prolong_lanes_const(nz * bz, nz))
    buf = lambda n, rows: pltpu.VMEM((n, rows, LANES), F32)
    return call(
        functools.partial(last_kernel, nx),
        shape(bx, by, bz),
        (taps, idx, f0, f1, h2, h3, h4, ya, yb, ra, rb, rc, tyh, py, pz),
        2,
        [pltpu.VMEM((2, REACH + 3, padded[1], LANES), F32)]
        + [buf((nx * bx >> l) + 24, padded[l]) for l in range(2, LEVELS)]
        + [buf(xs[l], padded[l]) for l in range(1, LEVELS)]
        + [buf(bx, by), pltpu.SemaphoreType.DMA((4,))]
        + [buf(xs[l + 1], padded[l]) for l in range(LEVELS - 1) for _ in range(2)],
        flops=10**9,
        out_hbm=True,
    )


def solution(mesh):
    in_specs = (P("gx", "gy", "gz"), P())
    out_specs = P("gx", "gy", "gz")
    return jax.shard_map(
        per_device, mesh=mesh, in_specs=in_specs, out_specs=out_specs, check_vma=False
    )
```

```python
import functools

import jax
import jax.numpy as jnp
import numpy as np
from jax import lax
from jax.experimental import pallas as pl
from jax.experimental.pallas import tpu as pltpu
from jax.sharding import PartitionSpec as P

LEVELS = 5
TAPS = 17
REACH = 8
LANES = 128
CUBIC = {-3: -0.0625, -1: 0.5625, 0: 1.0, 1: 0.5625, 3: -0.0625}
LOW = (0, 1, 2, 2, 2)
HIGH = (0, 2, 3, 3, 3)
F32 = jnp.float32
BF16 = jnp.bfloat16
GATHER = (0, 1, 3, 2)
FLOPS = 10**9


def sizes(block):
    return [block // 2**l + LOW[l] + HIGH[l] for l in range(LEVELS)]


def pad8(n):
    return -(-n // 8) * 8


def pad16(n):
    return -(-n // 16) * 16


def restrictions(whole):
    composite, out = np.eye(whole), [np.eye(whole)]
    for _ in range(1, LEVELS):
        fine = composite.shape[0]
        step = np.zeros((fine // 2, fine))
        for i in range(fine // 2):
            for k, w in CUBIC.items():
                if 0 <= 2 * i + k < fine:
                    step[i, 2 * i + k] = w
        composite = step @ composite
        out.append(composite)
    return out


def rows_padded(block):
    n = sizes(block)
    return [block] + [max(16, pad8(n[l])) for l in range(1, LEVELS)]


def lane_offsets(block):
    n = sizes(block)
    return [0, 0, n[1], n[1] + n[2], n[1] + n[2]]


def split_rows_const(whole, count):
    block = whole // count
    full, n, padded = restrictions(whole), sizes(block), rows_padded(block)
    out = np.zeros((count, sum(padded[1:]), block), np.float32)
    for d in range(count):
        row0 = 0
        for l in range(1, LEVELS):
            for r in range(n[l]):
                g = d * (block >> l) - LOW[l] + r
                if 0 <= g < whole >> l:
                    out[d, row0 + r] = full[l][g, d * block : (d + 1) * block]
            row0 += padded[l]
    hi = out.astype(BF16)
    lo = (out - hi.astype(np.float32)).astype(BF16)
    return np.concatenate([hi, hi, lo], axis=2)


def prolong_entries(whole, count, d, l):
    block = whole // count
    n = sizes(block)
    for i in range(n[l]):
        g_out = d * (block >> l) - LOW[l] + i
        for j in range(n[l + 1]):
            g_in = d * (block >> (l + 1)) - LOW[l + 1] + j
            ok = 0 <= g_out < whole >> l and 0 <= g_in < whole >> (l + 1)
            if ok and g_out - 2 * g_in in CUBIC:
                yield i, j, CUBIC[g_out - 2 * g_in]


def prolong_rows_const(whole, count):
    padded = rows_padded(whole // count)
    out = np.zeros((count, sum(padded[:4]), 2 * padded[1]), np.float32)
    for d in range(count):
        row0 = 0
        for l in range(LEVELS - 1):
            for i, j, w in prolong_entries(whole, count, d, l):
                out[d, row0 + i, j] = w
                out[d, row0 + i, padded[l + 1] + j] = w
            row0 += padded[l]
    return out.astype(BF16)


def prolong_lanes_const(whole, count):
    off = lane_offsets(whole // count)
    out = np.zeros((count, LEVELS - 1, LANES, LANES), np.float32)
    for d in range(count):
        for l in range(LEVELS - 1):
            for i, j, w in prolong_entries(whole, count, d, l):
                out[d, l, off[l + 1] + j, off[l] + i] = w
    return out.astype(BF16)


def toeplitz(taps_ref, row, g_in, g_out, mask):
    diff = g_in - g_out + REACH
    value = jnp.zeros(diff.shape, F32)
    for k in range(TAPS):
        value = jnp.where(diff == k, taps_ref[row, k], value)
    return jnp.where(mask, value, 0.0)


def iota(shape, axis):
    return lax.broadcasted_iota(jnp.int32, shape, axis)


def xor(a, b):
    return jnp.bitwise_xor(a, jnp.int32(b))


def halves(value):
    scaled = value * 65537.0
    hi = scaled - (scaled - value)
    return hi, value - hi


def mm(a, b):
    return jnp.dot(a, b, preferred_element_type=F32)


def spread(fine, coarse):
    k = fine - 2 * iota(fine.shape, 1)
    step = jnp.where(k == 0, 1.0, 0.0)
    step = jnp.where((k == 1) | (k == -1), 0.5625, step)
    step = jnp.where((k == 3) | (k == -3), -0.0625, step).astype(BF16)
    hi, lo = halves(coarse)
    low, rest = halves(lo)
    total = mm(step, rest.astype(BF16)) + mm(step, low.astype(BF16))
    return total + mm(step, hi.astype(BF16))


def setup_kernel(
    nz, taps_ref, idx_ref, w0_ref, w_ref
):
    bz = LANES
    whole_z = nz * bz
    dz = idx_ref[2]
    n, off = sizes(bz), lane_offsets(bz)
    below = None
    for l in range(LEVELS - 1, 0, -1):
        rows = whole_z >> l
        col = iota((rows, LANES), 1)
        g_out = dz * (bz >> l) - LOW[l] + col - off[l]
        mask = (col >= off[l]) & (col < off[l] + n[l]) & (g_out >= 0) & (g_out < rows)
        here = toeplitz(taps_ref, 3 * l + 2, iota((rows, LANES), 0), g_out, mask)
        none = jnp.zeros((rows, LANES), F32)
        here = jnp.concatenate([none, here] if l == LEVELS - 1 else [here, none], axis=1)
        if below is not None:
            here = here + spread(iota((rows, rows // 2), 0), below)
        below = here
    order = [dz, 1 - dz] if nz == 2 else list(range(nz))

    def store_rows(ref, j, value):
        hi, lo = halves(value)
        ref[j * bz : (j + 1) * bz] = hi.astype(BF16)
        ref[(nz + j) * bz : (nz + j + 1) * bz] = hi.astype(BF16)
        ref[(2 * nz + j) * bz : (2 * nz + j + 1) * bz] = lo.astype(BF16)

    row, col = iota((bz, bz), 0), iota((bz, bz), 1)
    if nz == 2:
        hi, lo = halves(toeplitz(taps_ref, 2, row, col, row >= 0))
        w0_ref[0:bz] = hi.astype(BF16)
        w0_ref[bz : 2 * bz] = hi.astype(BF16)
        w0_ref[2 * bz : 3 * bz] = lo.astype(BF16)
        hi, lo = halves(toeplitz(taps_ref, 2, (1 - 2 * dz) * bz + row, col, row >= 0))
        w0_ref[3 * bz : 4 * bz] = hi.astype(BF16)
        w0_ref[4 * bz : 5 * bz] = hi.astype(BF16)
        w0_ref[5 * bz : 6 * bz] = lo.astype(BF16)
    else:
        for j in range(nz):
            g_in, g_out = j * bz + row, dz * bz + col
            store_rows(w0_ref, j, toeplitz(taps_ref, 2, g_in, g_out, g_out >= 0))
    for j, source in enumerate(order):
        store_rows(w_ref, j, spread(source * bz + iota((bz, whole_z // 2), 0), below))


def y_matrices(by, ny, whole_y, taps_ref, idx_ref, ty0_ref, tyh_ref, *ty_refs):
    dy = idx_ref[1]
    even = (dy % 2) == 0
    sizes_y, padded = sizes(by), rows_padded(by)

    def column(shape):
        k = shape[1] // 3
        j = iota(shape, 1)
        return k, jnp.where(j >= 2 * k, j - 2 * k, jnp.where(j >= k, j - k, j))

    def store(ref, k, value):
        hi, lo = halves(value)
        ref[...] = jnp.where(iota(ref.shape, 1) < 2 * k, hi, lo).astype(BF16)

    def windows(l, j, own, window):
        block = by >> l
        right = (dy + 1) * block - LOW[l]
        left = (dy - 1) * block - LOW[l] + padded[l] - window
        base_a = jnp.where(even, right, left)
        base_b = jnp.where(even, left, right)
        second = jnp.where(j < own + window, base_a + j - own, base_b + j - own - window)
        return jnp.where(j < own, dy * block - LOW[l] + j, second)

    k, j = column(ty0_ref.shape)
    i = iota(ty0_ref.shape, 0)
    store(ty0_ref, k, toeplitz(taps_ref, 1, j, i, i >= 0))
    k, j = column(tyh_ref.shape)
    i = iota(tyh_ref.shape, 0)
    i = dy * by + jnp.where(i < 8, i, i + by - 16)
    g_in = windows(0, j, 0, 8)
    store(tyh_ref, k, toeplitz(taps_ref, 1, g_in, i, (g_in >= 0) & (g_in < whole_y)))
    for l, ty_ref in enumerate(ty_refs, 1):
        block = by >> l
        k, j = column(ty_ref.shape)
        if l < 3:
            g_in = windows(l, j, padded[l], 16)
        else:
            g_in = j
            for b in range(ny):
                source = xor(dy, GATHER[b]) if ny == 4 else b
                here = (j >= b * 16) & (j < (b + 1) * 16)
                g_in = jnp.where(here, source * block - LOW[l] + j - b * 16, g_in)
        i = iota(ty_ref.shape, 0)
        g_out = dy * block - LOW[l] + i
        mask = (i < sizes_y[l]) & (g_out >= 0) & (g_out < whole_y >> l)
        mask = mask & (g_in >= 0) & (g_in < whole_y >> l)
        store(ty_ref, k, toeplitz(taps_ref, 3 * l + 1, g_in, g_out, mask))


def masked(value, index, block, place):
    if 0 <= index < block:
        return value
    cell = place[0] * block + index
    inside = (cell >= 0) & (cell < place[1] * block)
    return value * jnp.where(inside, 1.0, 0.0).astype(F32)


def restrict_planes(src, dst, level, block_out, place):
    lo_in, count_in = LOW[level - 1], src.shape[0]
    for r in range(dst.shape[0]):
        i = r - LOW[level]
        total = None
        for k, w in CUBIC.items():
            p = 2 * i + k + lo_in
            if 0 <= p < count_in:
                term = src[p] if w == 1.0 else src[p] * w
                total = term if total is None else total + term
        dst[r] = masked(total, i, block_out, place)


def stacked(value):
    hi, lo = halves(value)
    return jnp.concatenate([hi, lo, hi], axis=0).astype(BF16)


def y_slots(n1, n2, n3, n4):
    half = -(-n1 // 2)
    ones = [[(p, 0)] for p in range(n1)]
    ones += [[(p, 1)] + ([(p + half, 1)] if p + half < n1 else []) for p in range(half)]
    twos = [(p, 0) for p in range(n2)] + [(p, 1) for p in range(n2)]
    threes = [[(p, 0)] for p in range(n3 + n4)]
    threes += [[(p, 1)] + ([(n3 + p, 1)] if p < n4 else []) for p in range(n3)]
    assert max(len(twos), len(threes)) <= len(ones)
    return ones, twos, threes


def put(ref, first, p, value):
    ref[first + p] = value


def batched(matrix, values, store, form=stacked, group=4):
    for p in range(0, len(values), group):
        some = values[p : p + group]
        out = mm(matrix, jnp.concatenate([form(v()) for v in some], axis=1))
        for q in range(len(some)):
            store(p + q, out[:, q * LANES : (q + 1) * LANES])


def z_rows(src, nz, planes, count):
    if nz == 2:
        blocks = [s[planes] for s in src]
    else:
        blocks = [src[0][s, planes] for s in range(nz)]
    his, los = zip(*[halves(b.reshape(count * b.shape[1], b.shape[2])) for b in blocks])
    return jnp.concatenate([h.astype(BF16) for h in his + los + his], axis=1)


def z0_own_kernel(q_ref, w_ref, g_ref):
    bx, by, bz = q_ref.shape
    chunk = 8

    def step(c, carry):
        planes = pl.ds(c * chunk, chunk)
        hi, lo = halves(q_ref[planes].reshape(chunk * by, bz))
        lhs = jnp.concatenate([hi.astype(BF16), lo.astype(BF16)], axis=1)
        g_ref[planes] = mm(lhs, w_ref[0 : 2 * bz, :]).reshape(chunk, by, bz)
        return carry

    lax.fori_loop(0, bx // chunk, step, 0, unroll=4)


def z0_rest_kernel(idx_ref, g_in, q_ref, other_ref, w_ref, g0_ref, xa_ref, xb_ref):
    bx, by, bz = q_ref.shape
    chunk = 8

    def step(c, carry):
        planes = pl.ds(c * chunk, chunk)
        own = halves(q_ref[planes].reshape(chunk * by, bz))[0]
        hi, lo = halves(other_ref[planes].reshape(chunk * by, bz))
        lhs = jnp.concatenate([v.astype(BF16) for v in (own, hi, lo, hi)], axis=1)
        out = mm(lhs, w_ref[2 * bz :, :]).reshape(chunk, by, bz)
        g0_ref[planes] = g_in[planes] + out
        return carry

    lax.fori_loop(0, bx // chunk, step, 0, unroll=4)
    even = (idx_ref[0] % 2) == 0
    xa_ref[...] = g0_ref[pl.ds(jnp.where(even, bx - REACH, 0), REACH)]
    xb_ref[...] = g0_ref[pl.ds(jnp.where(even, 0, bx - REACH), REACH)]


def z0_kernel(nz, idx_ref, *refs):
    src = refs[: (2 if nz == 2 else 1)]
    w_ref, g0_ref, xa_ref, xb_ref = refs[len(src) :]
    bx, by, bz = g0_ref.shape
    chunk = 8

    def step(c, carry):
        planes = pl.ds(c * chunk, chunk)
        out = mm(z_rows(src, nz, planes, chunk), w_ref[...])
        g0_ref[planes] = out.reshape(chunk, by, bz)
        return carry

    lax.fori_loop(0, bx // chunk, step, 0, unroll=4)
    even = (idx_ref[0] % 2) == 0
    xa_ref[...] = g0_ref[pl.ds(jnp.where(even, bx - REACH, 0), REACH)]
    xb_ref[...] = g0_ref[pl.ds(jnp.where(even, 0, bx - REACH), REACH)]


def z_kernel(nx, nz, idx_ref, *refs):
    src = refs[: (2 if nz == 2 else 1)]
    w_ref, sy_ref, ma_ref, mb_ref, mc_ref, y1_ref, y2_ref, y34_ref = refs[
        len(src) : len(src) + 8
    ]
    g1, g2, x1, x2, x3, t1, t2, t3, x4 = refs[len(src) + 8 :]
    bx, by, bz = g1.shape
    dx, dy = idx_ref[0], idx_ref[1]
    chunk = 8

    def step(c, carry):
        planes = pl.ds(c * chunk, chunk)
        out = mm(z_rows(src, nz, planes, chunk), w_ref[...])
        g1[planes] = out[:, :LANES].reshape(chunk, by, bz)
        g2[planes] = out[:, LANES:].reshape(chunk, by, bz)
        return carry

    lax.fori_loop(0, bx // chunk, step, 0, unroll=4)
    place = (dx, nx)
    for source, first, second, third, fourth in (
        (g1, x1, x2, x3, None),
        (g2, t1, t2, t3, x4),
    ):
        restrict_planes(source, first, 1, bx >> 1, place)
        restrict_planes(first, second, 2, bx >> 2, place)
        restrict_planes(second, third, 3, bx >> 3, place)
        if fourth is not None:
            restrict_planes(third, fourth, 4, bx >> 4, place)
    padded = rows_padded(by)
    n3 = x3.shape[0]
    row0 = 0
    for l, (source, target, first) in enumerate(
        ((x1, y1_ref, 0), (x2, y2_ref, 0), (x3, y34_ref, 0), (x4, y34_ref, n3)), 1
    ):
        sy = sy_ref[dy, row0 : row0 + padded[l], :]
        planes = [functools.partial(lambda ref, p: ref[p], source, p) for p in range(source.shape[0])]
        batched(sy, planes, functools.partial(put, target, first))
        row0 += padded[l]
    off = lane_offsets(bz)
    even = (dy % 2) == 0
    n1, n2 = y1_ref.shape[0], y2_ref.shape[0]
    ones, twos, threes = y_slots(n1, n2, n3, y34_ref.shape[0] - n3)
    lane8, row8 = iota((8, LANES), 1), iota((8, LANES), 0)
    for m_ref, rightward in ((ma_ref, even), (mb_ref, jnp.logical_not(even))):
        start1 = pl.multiple_of(jnp.where(rightward, padded[1] - 16, 0), 8)
        start2 = pl.multiple_of(jnp.where(rightward, padded[2] - 16, 0), 8)

        def first(p, b):
            return y1_ref[p, pl.ds(start1 + 8 * b, 8), :]

        for s in range(m_ref.shape[0]):
            value = first(*ones[s][0])
            if len(ones[s]) == 2:
                value = jnp.where(row8 < 4, value, pltpu.roll(first(*ones[s][1]), 4, 0))
            if s < len(twos):
                p, b = twos[s]
                value = jnp.where(lane8 < off[2], value, y2_ref[p, pl.ds(start2 + 8 * b, 8), :])
            if s < len(threes):
                p, b = threes[s][0]
                three = y34_ref[p, 8 * b : 8 * b + 8, :]
                if len(threes[s]) == 2:
                    p, b = threes[s][1]
                    four = pltpu.roll(y34_ref[p, 8 * b : 8 * b + 8, :], 5, 0)
                    three = jnp.where(row8 < 5, three, four)
                value = jnp.where(lane8 < off[3], value, three)
            m_ref[s] = value
    lane = iota((16, LANES), 1)
    for p in range(4):
        value = y34_ref[p]
        for g in range(1, 4):
            moved = pltpu.roll(y34_ref[4 * g + p], LANES - 32 * g, 1)
            value = jnp.where(lane >= off[3] - 32 * (g - 1), value, moved)
        mc_ref[2 * p : 2 * p + 2] = value.reshape(2, 8, LANES)


def conv_own_kernel(ny, taps_ref, idx_ref, g_ref, h_ref, *ty_refs):
    bx, by, bz = g_ref.shape
    y_matrices(by, ny, ny * by, taps_ref, idx_ref, *ty_refs)

    def rows(t, carry):
        at = pl.ds(pl.multiple_of(t * 8, 8), 8)
        for i in range(bx):
            total = None
            for k in range(TAPS):
                j = i + k - REACH
                if 0 <= j < bx:
                    term = g_ref[j, at, :] * taps_ref[0, k]
                    total = term if total is None else total + term
            h_ref[i, at, :] = total
        return carry

    lax.fori_loop(0, by // 8, rows, 0)


def x_slots(n1, n2, rows1, rows2):
    whole = rows1 - 1
    free = [whole * p + b for p in range(n1) for b in range(rows2, whole)]
    twos = {}
    for q in range(n2):
        for b in range(rows2):
            slot = whole * q + b if q < n1 else free[(q - n1) * rows2 + b]
            twos[slot] = (q, b)
    return twos


def mid_kernel(nx, ny, taps_ref, idx_ref, h_in, xa, xb, ra, rb, rc, y1, y2, y34, *refs):
    ty1, ty2, ty3, ty4, h0, ya_ref, yb_ref, ma_ref, mb_ref, mc_ref, h1, h2, h3, h4, halo = refs
    bx, by, bz = h0.shape
    dx, dy = idx_ref[0], idx_ref[1]
    off = lane_offsets(bz)

    ones, twos, threes = y_slots(y1.shape[0], y2.shape[0], h3.shape[0], h4.shape[0])
    row8 = iota((8, LANES), 0)
    found = {}
    for l, slots in ((1, ones), (2, [[v] for v in twos]), (3, threes)):
        for s, held in enumerate(slots):
            for place, (p, b) in enumerate(held):
                used = 8 if b == 0 else {1: 3, 2: 5}.get(l, 5 if p < h3.shape[0] else 1)
                found[l, p, b] = (s, 0 if place == 0 else 4 if l == 1 else 3, used)

    def block(ref, l, p, b):
        s, turn, used = found[l, p, b]
        value = ref[s] if turn == 0 else pltpu.roll(ref[s], turn, 0)
        return value if used == 8 else jnp.where(row8 < used, value, 0.0)

    def got(ref, l, p):
        return jnp.concatenate([block(ref, l, p, 0), block(ref, l, p, 1)], axis=0)

    def joined(own, l, p):
        return jnp.concatenate([own[p], got(ra, l, p), got(rb, l, p)], axis=0)

    def gathered(p):
        if ny == 4:
            far = rc[2 * (p % 4) : 2 * (p % 4) + 2].reshape(16, LANES)
            if p >= 4:
                far = pltpu.roll(far, 32 * (p // 4), 1)
            parts = [y34[p], got(ra, 3, p), got(rb, 3, p), far]
        else:
            parts = [rc[s, p] for s in range(ny)]
        return jnp.concatenate(parts, axis=0)

    for own, ty, h, l in ((y1, ty1, h1, 1), (y2, ty2, h2, 2)):
        planes = [functools.partial(joined, own, l, p) for p in range(h.shape[0])]
        batched(ty[...], planes, functools.partial(put, h, 0))
    n3 = h3.shape[0]
    planes = [functools.partial(gathered, p) for p in range(y34.shape[0])]
    batched(ty3[...], planes[:n3], functools.partial(put, h3, 0))
    batched(ty4[...], planes[n3:], functools.partial(put, h4, 0))

    even = (dx % 2) == 0
    n2, n1 = h2.shape[0], REACH + 3
    each = h1.shape[1] // 8 - 1
    twos = x_slots(n1, n2, each + 1, h2.shape[1] // 8)
    half = -(-n1 // 2)
    lane = iota((8, LANES), 1)

    def block34(pp, b):
        ref, p = (h3, pp) if pp < n3 else (h4, pp - n3)
        return ref[p, 8 * b : 8 * b + 8, :]

    for m_ref, rightward in ((ma_ref, even), (mb_ref, jnp.logical_not(even))):
        start1 = jnp.where(rightward, (bx >> 1) - REACH, 0)
        for p in range(n1):
            for b in range(each):
                value = h1[start1 + p, 8 * b : 8 * b + 8, :]
                if each * p + b in twos:
                    q, bb = twos[each * p + b]
                    value = jnp.where(lane < off[2], value, h2[q, 8 * bb : 8 * bb + 8, :])
                if b < 2 and p < n3:
                    value = jnp.where(lane < off[3], value, block34(p, b))
                elif 2 <= b < 4 and p < h4.shape[0]:
                    value = jnp.where(lane < off[3], value, block34(n3 + p, b - 2))
                m_ref[each * p + b] = value
        for p in range(half):
            value = h1[start1 + p, 8 * each : 8 * each + 8, :]
            if p + half < n1:
                other = pltpu.roll(h1[start1 + p + half, 8 * each : 8 * each + 8, :], 4, 0)
                value = jnp.where(row8 < 4, value, other)
            m_ref[each * n1 + p] = value
    start2 = jnp.where(dx < 2, n2 - 5, 0)
    rows2 = h2.shape[1] // 8
    for s in range(16):
        near = block34(s // 2, s % 2)
        far = pltpu.roll(block34((16 + s) // 2, s % 2), LANES - 32, 1)
        value = jnp.where(lane >= off[3], near, far)
        if s < 5 * rows2:
            b = s % rows2
            two = pltpu.roll(h2[start2 + s // rows2, 8 * b : 8 * b + 8, :], 64, 1)
            value = jnp.where(lane >= off[3] - 32, value, two)
        mc_ref[s] = value

    halo[jnp.where(even, 1, 0)] = xa[...]
    partner = jnp.where(even, dx > 0, dx < nx - 1)
    halo[jnp.where(even, 0, 1)] = xb[...] * jnp.where(partner, 1.0, 0.0).astype(F32)

    def rows(t, carry):
        at = pl.ds(pl.multiple_of(t * 8, 8), 8)
        for i in range(REACH):
            low, high = h_in[i, at, :], h_in[bx - REACH + i, at, :]
            for m in range(i, REACH):
                low = low + halo[0, m, at, :] * taps_ref[0, m - i]
            for m in range(i + 1):
                high = high + halo[1, m, at, :] * taps_ref[0, 2 * REACH + m - i]
            h0[i, at, :] = low
            h0[bx - REACH + i, at, :] = high
        return carry

    lax.fori_loop(0, by // 8, rows, 0)
    even = (dy % 2) == 0
    for m_ref, rightward in ((ya_ref, even), (yb_ref, jnp.logical_not(even))):
        m_ref[...] = h0[:, pl.ds(pl.multiple_of(jnp.where(rightward, by - 8, 0), 8), 8), :]


def last_own_kernel(taps_ref, h0, h1, ty0, f0, f1):
    bx, by, bz = h0.shape

    def planes(c, carry):
        some = [functools.partial(lambda p: h0[p], 4 * c + q) for q in range(4)]
        batched(ty0[...], some, lambda q, value: put(f0, 4 * c, q, value))
        return carry

    lax.fori_loop(0, bx // 4, planes, 0, unroll=4)
    count = h1.shape[0]
    for i in range(count):
        total = None
        for k in range(TAPS):
            j = i + k - REACH
            if 0 <= j < count:
                term = h1[j] * taps_ref[3, k]
                total = term if total is None else total + term
        f1[i] = total


def last_kernel(nx, taps_ref, idx_ref, f0, f1o, h2, h3, h4, ya, yb, ra, rb, rc, *refs):
    tyh, py_ref, pz_ref, result, side, e2, e3, e4, f1, f2, f3, f4, out_ref, sem = refs[:14]
    stage = refs[14:]
    group = result.shape[0] // sem.shape[0]
    copies = [
        pltpu.make_async_copy(
            out_ref.at[c * group : (c + 1) * group], result.at[c * group : (c + 1) * group], sem.at[c]
        )
        for c in range(sem.shape[0])
    ]
    bx, by, bz = f0.shape
    dx, dy, dz = idx_ref[0], idx_ref[1], idx_ref[2]
    even = (dx % 2) == 0
    place = (dx, nx)
    padded = rows_padded(by)
    each = f1o.shape[1] // 8 - 1
    n1, n2, n3, n4 = REACH + 3, h2.shape[0], h3.shape[0], h4.shape[0]
    rows2 = h2.shape[1] // 8
    twos = {v: k for k, v in x_slots(n1, n2, each + 1, rows2).items()}
    half = -(-n1 // 2)

    partner = jnp.where(even, dx > 0, dx < nx - 1)
    okay = jnp.where(partner, 1.0, 0.0).astype(F32)
    for ref, place_of, scale in ((ra, jnp.where(even, 1, 0), None), (rb, jnp.where(even, 0, 1), okay)):
        for p in range(n1):
            final = ref[each * n1 + p % half]
            final = pltpu.roll(final, 4, 0) if p >= half else final
            value = jnp.concatenate(
                [ref[each * p : each * p + each].reshape(8 * each, LANES), final], axis=0
            )
            side[place_of, p] = value if scale is None else value * scale
    block = bx >> 1
    for r in range(f1.shape[0]):
        total, i = f1o[r], r - LOW[1]
        for m in range(n1):
            for s, j in ((0, m - REACH - 1), (1, block - 1 + m)):
                k = j - i + REACH
                if 0 <= k < TAPS:
                    total = total + side[s, m] * taps_ref[3, k]
        f1[r] = masked(total, i, block, place)

    def near(ref, l, p):
        if l == 2:
            return jnp.concatenate(
                [ref[twos[p, b]] for b in range(rows2)], axis=0
            )
        first = p * each + (0 if l == 3 else 2)
        return ref[first : first + 2].reshape(16, LANES)

    def far(l, p):
        if l == 2:
            value = rc[p * rows2 : (p + 1) * rows2].reshape(8 * rows2, LANES)
            return pltpu.roll(value, 64, 1)
        first = 2 * p if l == 3 else 2 * (n3 + p)
        value = rc[first % 16 : first % 16 + 2].reshape(16, LANES)
        return value if first < 16 else pltpu.roll(value, 32, 1)

    for e, h, l in ((e2, h2, 2), (e3, h3, 3), (e4, h4, 4)):
        e[...] = jnp.zeros_like(e)
        for b in range(nx):
            source = xor(dx, GATHER[b]) if nx == 4 else b
            at = source * (bx >> l) - LOW[l] + 12
            count = h.shape[0]
            if nx == 4 and b == 3 and l == 2:
                at, count = at + jnp.where(source < 2, n2 - 5, 0), 5
            for p in range(count):
                if nx != 4:
                    value = near(rc.at[b], l, p)
                else:
                    value = far(l, p) if b == 3 else near(rb, l, p) if b == 2 else h[p]
                    if b == 1:
                        value = near(ra, l, p)
                e[at + p] = e[at + p] + value
    for e, f, l in ((e2, f2, 2), (e3, f3, 3), (e4, f4, 4)):
        start = dx * (bx >> l) - LOW[l] - REACH + 12
        for r in range(f.shape[0]):
            total = e[start + r] * taps_ref[3 * l, 0]
            for k in range(1, TAPS):
                total = total + e[start + r + k] * taps_ref[3 * l, k]
            f[r] = masked(total, r - LOW[l], bx >> l, place)
    def strips(p):
        return jnp.concatenate([ya[p], yb[p]], axis=0)

    def add_strips(p, value):
        out_ref[p, 0:8] = f0[p, 0:8] + value[0:8]
        out_ref[p, 8 : by - 8] = f0[p, 8 : by - 8]
        out_ref[p, by - 8 : by] = f0[p, by - 8 : by] + value[8:16]

    batched(tyh[...], [functools.partial(strips, p) for p in range(bx)], add_strips)

    def doubled(value):
        return jnp.concatenate(halves(value), axis=0).astype(BF16)

    row0 = [sum(padded[:l]) for l in range(LEVELS)]
    for l, f, target in ((3, f4, f3), (2, f3, f2), (1, f2, f1), (0, f1, out_ref)):
        rows, k = padded[l], 2 * padded[l + 1]
        matrix = py_ref[dy, row0[l] : row0[l] + rows, :k]
        s1, s2 = stage[2 * l], stage[2 * l + 1]
        count = f.shape[0]
        planes = [functools.partial(lambda ref, p: ref[p], f, p) for p in range(count)]
        batched(matrix, planes, functools.partial(put, s1, 0), doubled)
        pz = jnp.concatenate([pz_ref[dz, l], pz_ref[dz, l]], axis=0)
        hi, lo = halves(s1[...].reshape(count * rows, LANES))
        both = jnp.concatenate([hi.astype(BF16), lo.astype(BF16)], axis=1)
        s2[...] = mm(both, pz).reshape(count, rows, LANES)
        for r in range(target.shape[0]):
            j = r - LOW[l]
            total = None
            for kk, w in CUBIC.items():
                if (j - kk) % 2 == 0:
                    p = (j - kk) // 2 + LOW[l + 1]
                    if 0 <= p < count:
                        term = s2[p] if w == 1.0 else s2[p] * w
                        total = term if total is None else total + term
            target[r] = target[r] + masked(total, j, bx >> l, place)
            if l == 0 and (r + 1) % group == 0:
                copies[r // group].start()
    for copy in copies:
        copy.wait()


def call(kernel, out_shape, args, n_smem, scratch=(), flops=0, aliases={}, limit=20, out_hbm=False):
    vmem, smem = pl.BlockSpec(memory_space=pltpu.VMEM), pl.BlockSpec(memory_space=pltpu.SMEM)
    anywhere = pl.BlockSpec(memory_space=pltpu.HBM)
    many = isinstance(out_shape, (tuple, list))
    return pl.pallas_call(
        kernel,
        out_shape=out_shape,
        in_specs=[smem] * n_smem + [vmem] * (len(args) - n_smem),
        out_specs=[vmem] * len(out_shape) if many else anywhere if out_hbm else vmem,
        scratch_shapes=scratch,
        input_output_aliases=aliases,
        cost_estimate=pl.CostEstimate(flops=flops, bytes_accessed=2**20, transcendentals=0),
        compiler_params=pltpu.CompilerParams(vmem_limit_bytes=limit * 2**20),
    )(*args)


def swaps(count, flip):
    return [(i, i ^ flip) for i in range(count)]


def middle_swaps(count):
    if count == 4:
        return swaps(count, 3)
    return [p for i in range(1, count - 1, 2) for p in ((i, i + 1), (i + 1, i))]


def per_device(charges, kernel_taps):
    nx, ny, nz = (lax.axis_size(a) for a in ("gx", "gy", "gz"))
    bx, by, bz = charges.shape
    assert bz == LANES and nx % 2 == 0 and ny % 2 == 0
    xs, ys, padded = sizes(bx), sizes(by), rows_padded(by)
    dx, dy, dz = (lax.axis_index(a) for a in ("gx", "gy", "gz"))
    taps = kernel_taps.reshape(3 * LEVELS, TAPS)
    idx = jnp.stack([dx, dy, dz]).astype(jnp.int32)

    def shape(*dims, dtype=F32):
        return jax.ShapeDtypeStruct(dims, dtype)

    def neighbours(count):
        return middle_swaps(count)

    if nz == 2:
        others = (lax.ppermute(charges, "gz", swaps(2, 1)),)
    else:
        others = (lax.all_gather(charges, "gz"),)
    in_y = [0, padded[1] + 32, padded[2] + 32, 16 * ny, 16 * ny]
    w0, w = call(
        functools.partial(setup_kernel, nz),
        [
            shape(3 * nz * bz, LANES, dtype=BF16),
            shape(3 * nz * bz, 2 * LANES, dtype=BF16),
        ],
        (taps, idx),
        2,
        flops=FLOPS,
    )
    sy = jnp.asarray(split_rows_const(ny * by, ny))
    sources = (charges, *others) if nz == 2 else others
    n34 = xs[3] + xs[4]
    face, coarse = shape(REACH, by, bz), shape(xs[1] + -(-xs[1] // 2), 8, LANES)
    plane = lambda n: pltpu.VMEM((n, by, bz), F32)
    if nz == 2:
        g0 = call(z0_own_kernel, shape(bx, by, bz), (charges, w0), 0, flops=FLOPS)
        g0, xa, xb = call(
            z0_rest_kernel,
            [shape(bx, by, bz), face, face],
            (idx, g0, *sources, w0),
            1,
            flops=10**8,
            aliases={1: 0},
        )
    else:
        g0, xa, xb = call(
            functools.partial(z0_kernel, nz),
            [shape(bx, by, bz), face, face],
            (idx, *sources, w0),
            1,
            flops=10**8,
        )
    xa = lax.ppermute(xa, "gx", swaps(nx, 1))
    xb = lax.ppermute(xb, "gx", neighbours(nx))
    ma, mb, mc, y1, y2, y34 = call(
        functools.partial(z_kernel, nx, nz),
        [
            coarse,
            coarse,
            shape(8, 8, LANES),
            shape(xs[1], padded[1], LANES),
            shape(xs[2], padded[2], LANES),
            shape(n34, 16, LANES),
        ],
        (idx, *sources, w, sy),
        1,
        [plane(bx), plane(bx), plane(xs[1]), plane(xs[2]), plane(xs[3])]
        + [plane(xs[1]), plane(xs[2]), plane(xs[3]), plane(xs[4])],
        flops=10**9,
    )
    ra = lax.ppermute(ma, "gy", swaps(ny, 1))
    rb = lax.ppermute(mb, "gy", middle_swaps(ny))
    rc = lax.ppermute(mc, "gy", swaps(ny, 2)) if ny == 4 else lax.all_gather(y34, "gy")
    h0, ty0, tyh, *ty = call(
        functools.partial(conv_own_kernel, ny),
        [
            shape(bx, by, bz),
            shape(by, 3 * by, dtype=BF16),
            shape(16, 48, dtype=BF16),
        ]
        + [shape(padded[l], 3 * in_y[l], dtype=BF16) for l in range(1, LEVELS)],
        (taps, idx, g0),
        2,
        flops=10**9,
    )
    n1, strip = REACH + 3, shape(bx, 8, LANES)
    coarse = shape((padded[1] // 8 - 1) * n1 + -(-n1 // 2), 8, LANES)
    h0, ya, yb, ma, mb, mc, h1, h2, h3, h4 = call(
        functools.partial(mid_kernel, nx, ny),
        [shape(bx, by, bz), strip, strip, coarse, coarse, shape(16, 8, LANES)]
        + [shape(xs[l], padded[l], LANES) for l in range(1, LEVELS)],
        (taps, idx, h0, xa, xb, ra, rb, rc, y1, y2, y34, *ty),
        2,
        [pltpu.VMEM((2, REACH, by, bz), F32)],
        flops=10**9,
        aliases={2: 0},
    )
    ra = lax.ppermute(ma, "gx", swaps(nx, 1))
    rb = lax.ppermute(mb, "gx", middle_swaps(nx))
    rc = lax.ppermute(mc, "gx", swaps(nx, 2)) if nx == 4 else lax.all_gather(ma, "gx")
    ya = lax.ppermute(ya, "gy", swaps(ny, 1))
    yb = lax.ppermute(yb, "gy", neighbours(ny))
    f0, f1 = call(
        last_own_kernel,
        [shape(bx, by, bz), shape(xs[1], padded[1], LANES)],
        (taps, h0, h1, ty0),
        1,
        flops=10**9,
    )
    py = jnp.asarray(prolong_rows_const(ny * by, ny))
    pz = jnp.asarray(prolong_lanes_const(nz * bz, nz))
    buf = lambda n, rows: pltpu.VMEM((n, rows, LANES), F32)
    return call(
        functools.partial(last_kernel, nx),
        shape(bx, by, bz),
        (taps, idx, f0, f1, h2, h3, h4, ya, yb, ra, rb, rc, tyh, py, pz),
        2,
        [pltpu.VMEM((2, REACH + 3, padded[1], LANES), F32)]
        + [buf((nx * bx >> l) + 24, padded[l]) for l in range(2, LEVELS)]
        + [buf(xs[l], padded[l]) for l in range(1, LEVELS)]
        + [buf(bx, by), pltpu.SemaphoreType.DMA((4,))]
        + [buf(xs[l + 1], padded[l]) for l in range(LEVELS - 1) for _ in range(2)],
        flops=10**9,
        out_hbm=True,
    )


def solution(mesh):
    in_specs = (P("gx", "gy", "gz"), P())
    out_specs = P("gx", "gy", "gz")
    return jax.shard_map(
        per_device, mesh=mesh, in_specs=in_specs, out_specs=out_specs, check_vma=False
    )
```

```python
import functools

import jax
import jax.numpy as jnp
import numpy as np
from jax import lax
from jax.experimental import pallas as pl
from jax.experimental.pallas import tpu as pltpu
from jax.sharding import PartitionSpec as P

LEVELS = 5
TAPS = 17
REACH = 8
LANES = 128
CUBIC = {-3: -0.0625, -1: 0.5625, 0: 1.0, 1: 0.5625, 3: -0.0625}
LOW = (0, 1, 2, 2, 2)
HIGH = (0, 2, 3, 3, 3)
F32 = jnp.float32
BF16 = jnp.bfloat16
GATHER = (0, 1, 3, 2)
FLOPS = 10**9


def sizes(block):
    return [block // 2**l + LOW[l] + HIGH[l] for l in range(LEVELS)]


def pad8(n):
    return -(-n // 8) * 8


def pad16(n):
    return -(-n // 16) * 16


def restrictions(whole):
    composite, out = np.eye(whole), [np.eye(whole)]
    for _ in range(1, LEVELS):
        fine = composite.shape[0]
        step = np.zeros((fine // 2, fine))
        for i in range(fine // 2):
            for k, w in CUBIC.items():
                if 0 <= 2 * i + k < fine:
                    step[i, 2 * i + k] = w
        composite = step @ composite
        out.append(composite)
    return out


def rows_padded(block):
    n = sizes(block)
    return [block] + [max(16, pad8(n[l])) for l in range(1, LEVELS)]


def lane_offsets(block):
    n = sizes(block)
    return [0, 0, n[1], n[1] + n[2], n[1] + n[2]]


def split_rows_const(whole, count):
    block = whole // count
    full, n, padded = restrictions(whole), sizes(block), rows_padded(block)
    out = np.zeros((count, sum(padded[1:]), block), np.float32)
    for d in range(count):
        row0 = 0
        for l in range(1, LEVELS):
            for r in range(n[l]):
                g = d * (block >> l) - LOW[l] + r
                if 0 <= g < whole >> l:
                    out[d, row0 + r] = full[l][g, d * block : (d + 1) * block]
            row0 += padded[l]
    hi = out.astype(BF16)
    lo = (out - hi.astype(np.float32)).astype(BF16)
    return np.concatenate([hi, hi, lo], axis=2)


def prolong_entries(whole, count, d, l):
    block = whole // count
    n = sizes(block)
    for i in range(n[l]):
        g_out = d * (block >> l) - LOW[l] + i
        for j in range(n[l + 1]):
            g_in = d * (block >> (l + 1)) - LOW[l + 1] + j
            ok = 0 <= g_out < whole >> l and 0 <= g_in < whole >> (l + 1)
            if ok and g_out - 2 * g_in in CUBIC:
                yield i, j, CUBIC[g_out - 2 * g_in]


def prolong_rows_const(whole, count):
    padded = rows_padded(whole // count)
    out = np.zeros((count, sum(padded[:4]), 2 * padded[1]), np.float32)
    for d in range(count):
        row0 = 0
        for l in range(LEVELS - 1):
            for i, j, w in prolong_entries(whole, count, d, l):
                out[d, row0 + i, j] = w
                out[d, row0 + i, padded[l + 1] + j] = w
            row0 += padded[l]
    return out.astype(BF16)


def prolong_lanes_const(whole, count):
    off = lane_offsets(whole // count)
    out = np.zeros((count, LEVELS - 1, LANES, LANES), np.float32)
    for d in range(count):
        for l in range(LEVELS - 1):
            for i, j, w in prolong_entries(whole, count, d, l):
                out[d, l, off[l + 1] + j, off[l] + i] = w
    return out.astype(BF16)


def toeplitz(taps_ref, row, g_in, g_out, mask):
    diff = g_in - g_out + REACH
    value = jnp.zeros(diff.shape, F32)
    for k in range(TAPS):
        value = jnp.where(diff == k, taps_ref[row, k], value)
    return jnp.where(mask, value, 0.0)


def iota(shape, axis):
    return lax.broadcasted_iota(jnp.int32, shape, axis)


def xor(a, b):
    return jnp.bitwise_xor(a, jnp.int32(b))


def halves(value):
    scaled = value * 65537.0
    hi = scaled - (scaled - value)
    return hi, value - hi


def mm(a, b):
    return jnp.dot(a, b, preferred_element_type=F32)


def spread(fine, coarse):
    k = fine - 2 * iota(fine.shape, 1)
    step = jnp.where(k == 0, 1.0, 0.0)
    step = jnp.where((k == 1) | (k == -1), 0.5625, step)
    step = jnp.where((k == 3) | (k == -3), -0.0625, step).astype(BF16)
    hi, lo = halves(coarse)
    low, rest = halves(lo)
    total = mm(step, rest.astype(BF16)) + mm(step, low.astype(BF16))
    return total + mm(step, hi.astype(BF16))


def setup_kernel(
    nz, taps_ref, idx_ref, w0_ref, w_ref
):
    bz = LANES
    whole_z = nz * bz
    dz = idx_ref[2]
    n, off = sizes(bz), lane_offsets(bz)
    below = None
    for l in range(LEVELS - 1, 0, -1):
        rows = whole_z >> l
        col = iota((rows, LANES), 1)
        g_out = dz * (bz >> l) - LOW[l] + col - off[l]
        mask = (col >= off[l]) & (col < off[l] + n[l]) & (g_out >= 0) & (g_out < rows)
        here = toeplitz(taps_ref, 3 * l + 2, iota((rows, LANES), 0), g_out, mask)
        none = jnp.zeros((rows, LANES), F32)
        here = jnp.concatenate([none, here] if l == LEVELS - 1 else [here, none], axis=1)
        if below is not None:
            here = here + spread(iota((rows, rows // 2), 0), below)
        below = here
    order = [dz, 1 - dz] if nz == 2 else list(range(nz))

    def store_rows(ref, j, value):
        hi, lo = halves(value)
        ref[j * bz : (j + 1) * bz] = hi.astype(BF16)
        ref[(nz + j) * bz : (nz + j + 1) * bz] = hi.astype(BF16)
        ref[(2 * nz + j) * bz : (2 * nz + j + 1) * bz] = lo.astype(BF16)

    row, col = iota((bz, bz), 0), iota((bz, bz), 1)
    if nz == 2:
        hi, lo = halves(toeplitz(taps_ref, 2, row, col, row >= 0))
        w0_ref[0:bz] = hi.astype(BF16)
        w0_ref[bz : 2 * bz] = hi.astype(BF16)
        w0_ref[2 * bz : 3 * bz] = lo.astype(BF16)
        hi, lo = halves(toeplitz(taps_ref, 2, (1 - 2 * dz) * bz + row, col, row >= 0))
        w0_ref[3 * bz : 4 * bz] = hi.astype(BF16)
        w0_ref[4 * bz : 5 * bz] = hi.astype(BF16)
        w0_ref[5 * bz : 6 * bz] = lo.astype(BF16)
    else:
        for j in range(nz):
            g_in, g_out = j * bz + row, dz * bz + col
            store_rows(w0_ref, j, toeplitz(taps_ref, 2, g_in, g_out, g_out >= 0))
    for j, source in enumerate(order):
        store_rows(w_ref, j, spread(source * bz + iota((bz, whole_z // 2), 0), below))


def y_matrices(by, ny, whole_y, taps_ref, idx_ref, ty0_ref, tyh_ref, *ty_refs):
    dy = idx_ref[1]
    even = (dy % 2) == 0
    sizes_y, padded = sizes(by), rows_padded(by)

    def column(shape):
        k = shape[1] // 3
        j = iota(shape, 1)
        return k, jnp.where(j >= 2 * k, j - 2 * k, jnp.where(j >= k, j - k, j))

    def store(ref, k, value):
        hi, lo = halves(value)
        ref[...] = jnp.where(iota(ref.shape, 1) < 2 * k, hi, lo).astype(BF16)

    def windows(l, j, own, window):
        block = by >> l
        right = (dy + 1) * block - LOW[l]
        left = (dy - 1) * block - LOW[l] + padded[l] - window
        base_a = jnp.where(even, right, left)
        base_b = jnp.where(even, left, right)
        second = jnp.where(j < own + window, base_a + j - own, base_b + j - own - window)
        return jnp.where(j < own, dy * block - LOW[l] + j, second)

    k, j = column(ty0_ref.shape)
    i = iota(ty0_ref.shape, 0)
    store(ty0_ref, k, toeplitz(taps_ref, 1, j, i, i >= 0))
    k, j = column(tyh_ref.shape)
    i = iota(tyh_ref.shape, 0)
    i = dy * by + jnp.where(i < 8, i, i + by - 16)
    g_in = windows(0, j, 0, 8)
    store(tyh_ref, k, toeplitz(taps_ref, 1, g_in, i, (g_in >= 0) & (g_in < whole_y)))
    for l, ty_ref in enumerate(ty_refs, 1):
        block = by >> l
        k, j = column(ty_ref.shape)
        if l < 3:
            g_in = windows(l, j, padded[l], 16)
        else:
            g_in = j
            for b in range(ny):
                source = xor(dy, GATHER[b]) if ny == 4 else b
                here = (j >= b * 16) & (j < (b + 1) * 16)
                g_in = jnp.where(here, source * block - LOW[l] + j - b * 16, g_in)
        i = iota(ty_ref.shape, 0)
        g_out = dy * block - LOW[l] + i
        mask = (i < sizes_y[l]) & (g_out >= 0) & (g_out < whole_y >> l)
        mask = mask & (g_in >= 0) & (g_in < whole_y >> l)
        store(ty_ref, k, toeplitz(taps_ref, 3 * l + 1, g_in, g_out, mask))


def masked(value, index, block, place):
    if 0 <= index < block:
        return value
    cell = place[0] * block + index
    inside = (cell >= 0) & (cell < place[1] * block)
    return value * jnp.where(inside, 1.0, 0.0).astype(F32)


def restrict_planes(src, dst, level, block_out, place):
    lo_in, count_in = LOW[level - 1], src.shape[0]
    for r in range(dst.shape[0]):
        i = r - LOW[level]
        total = None
        for k, w in CUBIC.items():
            p = 2 * i + k + lo_in
            if 0 <= p < count_in:
                term = src[p] if w == 1.0 else src[p] * w
                total = term if total is None else total + term
        dst[r] = masked(total, i, block_out, place)


def stacked(value):
    hi, lo = halves(value)
    return jnp.concatenate([hi, lo, hi], axis=0).astype(BF16)


def y_slots(n1, n2, n3, n4):
    half = -(-n1 // 2)
    ones = [[(p, 0)] for p in range(n1)]
    ones += [[(p, 1)] + ([(p + half, 1)] if p + half < n1 else []) for p in range(half)]
    twos = [(p, 0) for p in range(n2)] + [(p, 1) for p in range(n2)]
    threes = [[(p, 0)] for p in range(n3 + n4)]
    threes += [[(p, 1)] + ([(n3 + p, 1)] if p < n4 else []) for p in range(n3)]
    assert max(len(twos), len(threes)) <= len(ones)
    return ones, twos, threes


def put(ref, first, p, value):
    ref[first + p] = value


def batched(matrix, values, store, form=stacked, group=4):
    for p in range(0, len(values), group):
        some = values[p : p + group]
        out = mm(matrix, jnp.concatenate([form(v()) for v in some], axis=1))
        for q in range(len(some)):
            store(p + q, out[:, q * LANES : (q + 1) * LANES])


def z_rows(src, nz, planes, count):
    if nz == 2:
        blocks = [s[planes] for s in src]
    else:
        blocks = [src[0][s, planes] for s in range(nz)]
    his, los = zip(*[halves(b.reshape(count * b.shape[1], b.shape[2])) for b in blocks])
    return jnp.concatenate([h.astype(BF16) for h in his + los + his], axis=1)


def z0_own_kernel(q_ref, w_ref, g_ref):
    bx, by, bz = q_ref.shape
    chunk = 4

    def step(c, carry):
        planes = pl.ds(c * chunk, chunk)
        hi, lo = halves(q_ref[planes].reshape(chunk * by, bz))
        lhs = jnp.concatenate([hi.astype(BF16), lo.astype(BF16)], axis=1)
        g_ref[planes] = mm(lhs, w_ref[0 : 2 * bz, :]).reshape(chunk, by, bz)
        return carry

    lax.fori_loop(0, bx // chunk, step, 0, unroll=8)


def z0_rest_kernel(idx_ref, g_in, q_ref, other_ref, w_ref, g0_ref, xa_ref, xb_ref):
    bx, by, bz = q_ref.shape
    chunk = 4

    def step(c, carry):
        planes = pl.ds(c * chunk, chunk)
        own = halves(q_ref[planes].reshape(chunk * by, bz))[0]
        hi, lo = halves(other_ref[planes].reshape(chunk * by, bz))
        lhs = jnp.concatenate([v.astype(BF16) for v in (own, hi, lo, hi)], axis=1)
        out = mm(lhs, w_ref[2 * bz :, :]).reshape(chunk, by, bz)
        g0_ref[planes] = g_in[planes] + out
        return carry

    lax.fori_loop(0, bx // chunk, step, 0, unroll=8)
    even = (idx_ref[0] % 2) == 0
    xa_ref[...] = g0_ref[pl.ds(jnp.where(even, bx - REACH, 0), REACH)]
    xb_ref[...] = g0_ref[pl.ds(jnp.where(even, 0, bx - REACH), REACH)]


def z0_kernel(nz, idx_ref, *refs):
    src = refs[: (2 if nz == 2 else 1)]
    w_ref, g0_ref, xa_ref, xb_ref = refs[len(src) :]
    bx, by, bz = g0_ref.shape
    chunk = 4

    def step(c, carry):
        planes = pl.ds(c * chunk, chunk)
        out = mm(z_rows(src, nz, planes, chunk), w_ref[...])
        g0_ref[planes] = out.reshape(chunk, by, bz)
        return carry

    lax.fori_loop(0, bx // chunk, step, 0, unroll=8)
    even = (idx_ref[0] % 2) == 0
    xa_ref[...] = g0_ref[pl.ds(jnp.where(even, bx - REACH, 0), REACH)]
    xb_ref[...] = g0_ref[pl.ds(jnp.where(even, 0, bx - REACH), REACH)]


def z_kernel(nx, nz, idx_ref, *refs):
    src = refs[: (2 if nz == 2 else 1)]
    w_ref, sy_ref, ma_ref, mb_ref, mc_ref, y1_ref, y2_ref, y34_ref = refs[
        len(src) : len(src) + 8
    ]
    g1, g2, x1, x2, x3, t1, t2, t3, x4 = refs[len(src) + 8 :]
    bx, by, bz = g1.shape
    dx, dy = idx_ref[0], idx_ref[1]
    chunk = 4

    def step(c, carry):
        planes = pl.ds(c * chunk, chunk)
        out = mm(z_rows(src, nz, planes, chunk), w_ref[...])
        g1[planes] = out[:, :LANES].reshape(chunk, by, bz)
        g2[planes] = out[:, LANES:].reshape(chunk, by, bz)
        return carry

    lax.fori_loop(0, bx // chunk, step, 0, unroll=8)
    place = (dx, nx)
    for source, first, second, third, fourth in (
        (g1, x1, x2, x3, None),
        (g2, t1, t2, t3, x4),
    ):
        restrict_planes(source, first, 1, bx >> 1, place)
        restrict_planes(first, second, 2, bx >> 2, place)
        restrict_planes(second, third, 3, bx >> 3, place)
        if fourth is not None:
            restrict_planes(third, fourth, 4, bx >> 4, place)
    padded = rows_padded(by)
    n3 = x3.shape[0]
    row0 = 0
    for l, (source, target, first) in enumerate(
        ((x1, y1_ref, 0), (x2, y2_ref, 0), (x3, y34_ref, 0), (x4, y34_ref, n3)), 1
    ):
        sy = sy_ref[dy, row0 : row0 + padded[l], :]
        planes = [functools.partial(lambda ref, p: ref[p], source, p) for p in range(source.shape[0])]
        batched(sy, planes, functools.partial(put, target, first))
        row0 += padded[l]
    off = lane_offsets(bz)
    even = (dy % 2) == 0
    n1, n2 = y1_ref.shape[0], y2_ref.shape[0]
    ones, twos, threes = y_slots(n1, n2, n3, y34_ref.shape[0] - n3)
    lane8, row8 = iota((8, LANES), 1), iota((8, LANES), 0)
    for m_ref, rightward in ((ma_ref, even), (mb_ref, jnp.logical_not(even))):
        start1 = pl.multiple_of(jnp.where(rightward, padded[1] - 16, 0), 8)
        start2 = pl.multiple_of(jnp.where(rightward, padded[2] - 16, 0), 8)

        def first(p, b):
            return y1_ref[p, pl.ds(start1 + 8 * b, 8), :]

        for s in range(m_ref.shape[0]):
            value = first(*ones[s][0])
            if len(ones[s]) == 2:
                value = jnp.where(row8 < 4, value, pltpu.roll(first(*ones[s][1]), 4, 0))
            if s < len(twos):
                p, b = twos[s]
                value = jnp.where(lane8 < off[2], value, y2_ref[p, pl.ds(start2 + 8 * b, 8), :])
            if s < len(threes):
                p, b = threes[s][0]
                three = y34_ref[p, 8 * b : 8 * b + 8, :]
                if len(threes[s]) == 2:
                    p, b = threes[s][1]
                    four = pltpu.roll(y34_ref[p, 8 * b : 8 * b + 8, :], 5, 0)
                    three = jnp.where(row8 < 5, three, four)
                value = jnp.where(lane8 < off[3], value, three)
            m_ref[s] = value
    lane = iota((16, LANES), 1)
    for p in range(4):
        value = y34_ref[p]
        for g in range(1, 4):
            moved = pltpu.roll(y34_ref[4 * g + p], LANES - 32 * g, 1)
            value = jnp.where(lane >= off[3] - 32 * (g - 1), value, moved)
        mc_ref[2 * p : 2 * p + 2] = value.reshape(2, 8, LANES)


def conv_own_kernel(ny, taps_ref, idx_ref, g_ref, h_ref, *ty_refs):
    bx, by, bz = g_ref.shape
    y_matrices(by, ny, ny * by, taps_ref, idx_ref, *ty_refs)

    def rows(t, carry):
        at = pl.ds(pl.multiple_of(t * 8, 8), 8)
        for i in range(bx):
            total = None
            for k in range(TAPS):
                j = i + k - REACH
                if 0 <= j < bx:
                    term = g_ref[j, at, :] * taps_ref[0, k]
                    total = term if total is None else total + term
            h_ref[i, at, :] = total
        return carry

    lax.fori_loop(0, by // 8, rows, 0)


def x_slots(n1, n2, rows1, rows2):
    whole = rows1 - 1
    free = [whole * p + b for p in range(n1) for b in range(rows2, whole)]
    twos = {}
    for q in range(n2):
        for b in range(rows2):
            slot = whole * q + b if q < n1 else free[(q - n1) * rows2 + b]
            twos[slot] = (q, b)
    return twos


def mid_kernel(nx, ny, taps_ref, idx_ref, h_in, xa, xb, ra, rb, rc, y1, y2, y34, *refs):
    ty1, ty2, ty3, ty4, h0, ya_ref, yb_ref, ma_ref, mb_ref, mc_ref, h1, h2, h3, h4, halo = refs
    bx, by, bz = h0.shape
    dx, dy = idx_ref[0], idx_ref[1]
    off = lane_offsets(bz)

    ones, twos, threes = y_slots(y1.shape[0], y2.shape[0], h3.shape[0], h4.shape[0])
    row8 = iota((8, LANES), 0)
    found = {}
    for l, slots in ((1, ones), (2, [[v] for v in twos]), (3, threes)):
        for s, held in enumerate(slots):
            for place, (p, b) in enumerate(held):
                used = 8 if b == 0 else {1: 3, 2: 5}.get(l, 5 if p < h3.shape[0] else 1)
                found[l, p, b] = (s, 0 if place == 0 else 4 if l == 1 else 3, used)

    def block(ref, l, p, b):
        s, turn, used = found[l, p, b]
        value = ref[s] if turn == 0 else pltpu.roll(ref[s], turn, 0)
        return value if used == 8 else jnp.where(row8 < used, value, 0.0)

    def got(ref, l, p):
        return jnp.concatenate([block(ref, l, p, 0), block(ref, l, p, 1)], axis=0)

    def joined(own, l, p):
        return jnp.concatenate([own[p], got(ra, l, p), got(rb, l, p)], axis=0)

    def gathered(p):
        if ny == 4:
            far = rc[2 * (p % 4) : 2 * (p % 4) + 2].reshape(16, LANES)
            if p >= 4:
                far = pltpu.roll(far, 32 * (p // 4), 1)
            parts = [y34[p], got(ra, 3, p), got(rb, 3, p), far]
        else:
            parts = [rc[s, p] for s in range(ny)]
        return jnp.concatenate(parts, axis=0)

    for own, ty, h, l in ((y1, ty1, h1, 1), (y2, ty2, h2, 2)):
        planes = [functools.partial(joined, own, l, p) for p in range(h.shape[0])]
        batched(ty[...], planes, functools.partial(put, h, 0))
    n3 = h3.shape[0]
    planes = [functools.partial(gathered, p) for p in range(y34.shape[0])]
    batched(ty3[...], planes[:n3], functools.partial(put, h3, 0))
    batched(ty4[...], planes[n3:], functools.partial(put, h4, 0))

    even = (dx % 2) == 0
    n2, n1 = h2.shape[0], REACH + 3
    each = h1.shape[1] // 8 - 1
    twos = x_slots(n1, n2, each + 1, h2.shape[1] // 8)
    half = -(-n1 // 2)
    lane = iota((8, LANES), 1)

    def block34(pp, b):
        ref, p = (h3, pp) if pp < n3 else (h4, pp - n3)
        return ref[p, 8 * b : 8 * b + 8, :]

    for m_ref, rightward in ((ma_ref, even), (mb_ref, jnp.logical_not(even))):
        start1 = jnp.where(rightward, (bx >> 1) - REACH, 0)
        for p in range(n1):
            for b in range(each):
                value = h1[start1 + p, 8 * b : 8 * b + 8, :]
                if each * p + b in twos:
                    q, bb = twos[each * p + b]
                    value = jnp.where(lane < off[2], value, h2[q, 8 * bb : 8 * bb + 8, :])
                if b < 2 and p < n3:
                    value = jnp.where(lane < off[3], value, block34(p, b))
                elif 2 <= b < 4 and p < h4.shape[0]:
                    value = jnp.where(lane < off[3], value, block34(n3 + p, b - 2))
                m_ref[each * p + b] = value
        for p in range(half):
            value = h1[start1 + p, 8 * each : 8 * each + 8, :]
            if p + half < n1:
                other = pltpu.roll(h1[start1 + p + half, 8 * each : 8 * each + 8, :], 4, 0)
                value = jnp.where(row8 < 4, value, other)
            m_ref[each * n1 + p] = value
    start2 = jnp.where(dx < 2, n2 - 5, 0)
    rows2 = h2.shape[1] // 8
    for s in range(16):
        near = block34(s // 2, s % 2)
        far = pltpu.roll(block34((16 + s) // 2, s % 2), LANES - 32, 1)
        value = jnp.where(lane >= off[3], near, far)
        if s < 5 * rows2:
            b = s % rows2
            two = pltpu.roll(h2[start2 + s // rows2, 8 * b : 8 * b + 8, :], 64, 1)
            value = jnp.where(lane >= off[3] - 32, value, two)
        mc_ref[s] = value

    halo[jnp.where(even, 1, 0)] = xa[...]
    partner = jnp.where(even, dx > 0, dx < nx - 1)
    halo[jnp.where(even, 0, 1)] = xb[...] * jnp.where(partner, 1.0, 0.0).astype(F32)

    def rows(t, carry):
        at = pl.ds(pl.multiple_of(t * 8, 8), 8)
        for i in range(REACH):
            low, high = h_in[i, at, :], h_in[bx - REACH + i, at, :]
            for m in range(i, REACH):
                low = low + halo[0, m, at, :] * taps_ref[0, m - i]
            for m in range(i + 1):
                high = high + halo[1, m, at, :] * taps_ref[0, 2 * REACH + m - i]
            h0[i, at, :] = low
            h0[bx - REACH + i, at, :] = high
        return carry

    lax.fori_loop(0, by // 8, rows, 0)
    even = (dy % 2) == 0
    for m_ref, rightward in ((ya_ref, even), (yb_ref, jnp.logical_not(even))):
        m_ref[...] = h0[:, pl.ds(pl.multiple_of(jnp.where(rightward, by - 8, 0), 8), 8), :]


def last_own_kernel(taps_ref, h0, h1, ty0, f0, f1):
    bx, by, bz = h0.shape

    def planes(c, carry):
        some = [functools.partial(lambda p: h0[p], 4 * c + q) for q in range(4)]
        batched(ty0[...], some, lambda q, value: put(f0, 4 * c, q, value))
        return carry

    lax.fori_loop(0, bx // 4, planes, 0, unroll=4)
    count = h1.shape[0]
    for i in range(count):
        total = None
        for k in range(TAPS):
            j = i + k - REACH
            if 0 <= j < count:
                term = h1[j] * taps_ref[3, k]
                total = term if total is None else total + term
        f1[i] = total


def last_kernel(nx, taps_ref, idx_ref, f0, f1o, h2, h3, h4, ya, yb, ra, rb, rc, *refs):
    tyh, py_ref, pz_ref, result, side, e2, e3, e4, f1, f2, f3, f4, out_ref, sem = refs[:14]
    stage = refs[14:]
    group = result.shape[0] // sem.shape[0]
    copies = [
        pltpu.make_async_copy(
            out_ref.at[c * group : (c + 1) * group], result.at[c * group : (c + 1) * group], sem.at[c]
        )
        for c in range(sem.shape[0])
    ]
    bx, by, bz = f0.shape
    dx, dy, dz = idx_ref[0], idx_ref[1], idx_ref[2]
    even = (dx % 2) == 0
    place = (dx, nx)
    padded = rows_padded(by)
    each = f1o.shape[1] // 8 - 1
    n1, n2, n3, n4 = REACH + 3, h2.shape[0], h3.shape[0], h4.shape[0]
    rows2 = h2.shape[1] // 8
    twos = {v: k for k, v in x_slots(n1, n2, each + 1, rows2).items()}
    half = -(-n1 // 2)

    def near(ref, l, p):
        if l == 2:
            return jnp.concatenate(
                [ref[twos[p, b]] for b in range(rows2)], axis=0
            )
        first = p * each + (0 if l == 3 else 2)
        return ref[first : first + 2].reshape(16, LANES)

    def far(l, p):
        if l == 2:
            value = rc[p * rows2 : (p + 1) * rows2].reshape(8 * rows2, LANES)
            return pltpu.roll(value, 64, 1)
        first = 2 * p if l == 3 else 2 * (n3 + p)
        value = rc[first % 16 : first % 16 + 2].reshape(16, LANES)
        return value if first < 16 else pltpu.roll(value, 32, 1)

    for e, h, l in ((e2, h2, 2), (e3, h3, 3), (e4, h4, 4)):
        e[...] = jnp.zeros_like(e)
        for b in range(nx):
            source = xor(dx, GATHER[b]) if nx == 4 else b
            at = source * (bx >> l) - LOW[l] + 12
            count = h.shape[0]
            if nx == 4 and b == 3 and l == 2:
                at, count = at + jnp.where(source < 2, n2 - 5, 0), 5
            for p in range(count):
                if nx != 4:
                    value = near(rc.at[b], l, p)
                else:
                    value = far(l, p) if b == 3 else near(rb, l, p) if b == 2 else h[p]
                    if b == 1:
                        value = near(ra, l, p)
                e[at + p] = e[at + p] + value
    for e, f, l in ((e2, f2, 2), (e3, f3, 3), (e4, f4, 4)):
        start = dx * (bx >> l) - LOW[l] - REACH + 12
        for r in range(f.shape[0]):
            total = e[start + r] * taps_ref[3 * l, 0]
            for k in range(1, TAPS):
                total = total + e[start + r + k] * taps_ref[3 * l, k]
            f[r] = masked(total, r - LOW[l], bx >> l, place)
    def strips(p):
        return jnp.concatenate([ya[p], yb[p]], axis=0)

    def add_strips(p, value):
        out_ref[p, 0:8] = f0[p, 0:8] + value[0:8]
        out_ref[p, 8 : by - 8] = f0[p, 8 : by - 8]
        out_ref[p, by - 8 : by] = f0[p, by - 8 : by] + value[8:16]

    batched(tyh[...], [functools.partial(strips, p) for p in range(bx)], add_strips)

    def doubled(value):
        return jnp.concatenate(halves(value), axis=0).astype(BF16)

    row0 = [sum(padded[:l]) for l in range(LEVELS)]
    def middle():
        partner = jnp.where(even, dx > 0, dx < nx - 1)
        okay = jnp.where(partner, 1.0, 0.0).astype(F32)
        for ref, place_of, scale in ((ra, jnp.where(even, 1, 0), None), (rb, jnp.where(even, 0, 1), okay)):
            for p in range(n1):
                final = ref[each * n1 + p % half]
                final = pltpu.roll(final, 4, 0) if p >= half else final
                value = jnp.concatenate(
                    [ref[each * p : each * p + each].reshape(8 * each, LANES), final], axis=0
                )
                side[place_of, p] = value if scale is None else value * scale
        block = bx >> 1
        for r in range(f1.shape[0]):
            total, i = f1o[r], r - LOW[1]
            for m in range(n1):
                for s, j in ((0, m - REACH - 1), (1, block - 1 + m)):
                    k = j - i + REACH
                    if 0 <= k < TAPS:
                        total = total + side[s, m] * taps_ref[3, k]
            f1[r] = masked(total, i, block, place)

    for l, f, target in ((3, f4, f3), (2, f3, f2), (1, f2, f1), (0, f1, out_ref)):
        if l == 1:
            middle()
        rows, k = padded[l], 2 * padded[l + 1]
        matrix = py_ref[dy, row0[l] : row0[l] + rows, :k]
        s1, s2 = stage[2 * l], stage[2 * l + 1]
        count = f.shape[0]
        planes = [functools.partial(lambda ref, p: ref[p], f, p) for p in range(count)]
        batched(matrix, planes, functools.partial(put, s1, 0), doubled)
        pz = jnp.concatenate([pz_ref[dz, l], pz_ref[dz, l]], axis=0)
        hi, lo = halves(s1[...].reshape(count * rows, LANES))
        both = jnp.concatenate([hi.astype(BF16), lo.astype(BF16)], axis=1)
        s2[...] = mm(both, pz).reshape(count, rows, LANES)
        for r in range(target.shape[0]):
            j = r - LOW[l]
            total = None
            for kk, w in CUBIC.items():
                if (j - kk) % 2 == 0:
                    p = (j - kk) // 2 + LOW[l + 1]
                    if 0 <= p < count:
                        term = s2[p] if w == 1.0 else s2[p] * w
                        total = term if total is None else total + term
            target[r] = target[r] + masked(total, j, bx >> l, place)
            if l == 0 and (r + 1) % group == 0:
                copies[r // group].start()
    for copy in copies:
        copy.wait()


def call(kernel, out_shape, args, n_smem, scratch=(), flops=0, aliases={}, limit=20, out_hbm=False):
    vmem, smem = pl.BlockSpec(memory_space=pltpu.VMEM), pl.BlockSpec(memory_space=pltpu.SMEM)
    anywhere = pl.BlockSpec(memory_space=pltpu.HBM)
    many = isinstance(out_shape, (tuple, list))
    return pl.pallas_call(
        kernel,
        out_shape=out_shape,
        in_specs=[smem] * n_smem + [vmem] * (len(args) - n_smem),
        out_specs=[vmem] * len(out_shape) if many else anywhere if out_hbm else vmem,
        scratch_shapes=scratch,
        input_output_aliases=aliases,
        cost_estimate=pl.CostEstimate(flops=flops, bytes_accessed=2**20, transcendentals=0),
        compiler_params=pltpu.CompilerParams(vmem_limit_bytes=limit * 2**20),
    )(*args)


def swaps(count, flip):
    return [(i, i ^ flip) for i in range(count)]


def middle_swaps(count):
    if count == 4:
        return swaps(count, 3)
    return [p for i in range(1, count - 1, 2) for p in ((i, i + 1), (i + 1, i))]


def per_device(charges, kernel_taps):
    nx, ny, nz = (lax.axis_size(a) for a in ("gx", "gy", "gz"))
    bx, by, bz = charges.shape
    assert bz == LANES and nx % 2 == 0 and ny % 2 == 0
    xs, ys, padded = sizes(bx), sizes(by), rows_padded(by)
    dx, dy, dz = (lax.axis_index(a) for a in ("gx", "gy", "gz"))
    taps = kernel_taps.reshape(3 * LEVELS, TAPS)
    idx = jnp.stack([dx, dy, dz]).astype(jnp.int32)

    def shape(*dims, dtype=F32):
        return jax.ShapeDtypeStruct(dims, dtype)

    def neighbours(count):
        return middle_swaps(count)

    if nz == 2:
        others = (lax.ppermute(charges, "gz", swaps(2, 1)),)
    else:
        others = (lax.all_gather(charges, "gz"),)
    in_y = [0, padded[1] + 32, padded[2] + 32, 16 * ny, 16 * ny]
    w0, w = call(
        functools.partial(setup_kernel, nz),
        [
            shape(3 * nz * bz, LANES, dtype=BF16),
            shape(3 * nz * bz, 2 * LANES, dtype=BF16),
        ],
        (taps, idx),
        2,
        flops=FLOPS,
    )
    sy = jnp.asarray(split_rows_const(ny * by, ny))
    sources = (charges, *others) if nz == 2 else others
    n34 = xs[3] + xs[4]
    face, coarse = shape(REACH, by, bz), shape(xs[1] + -(-xs[1] // 2), 8, LANES)
    plane = lambda n: pltpu.VMEM((n, by, bz), F32)
    if nz == 2:
        g0 = call(z0_own_kernel, shape(bx, by, bz), (charges, w0), 0, flops=FLOPS)
        g0, xa, xb = call(
            z0_rest_kernel,
            [shape(bx, by, bz), face, face],
            (idx, g0, *sources, w0),
            1,
            flops=10**8,
            aliases={1: 0},
        )
    else:
        g0, xa, xb = call(
            functools.partial(z0_kernel, nz),
            [shape(bx, by, bz), face, face],
            (idx, *sources, w0),
            1,
            flops=10**8,
        )
    xa = lax.ppermute(xa, "gx", swaps(nx, 1))
    xb = lax.ppermute(xb, "gx", neighbours(nx))
    ma, mb, mc, y1, y2, y34 = call(
        functools.partial(z_kernel, nx, nz),
        [
            coarse,
            coarse,
            shape(8, 8, LANES),
            shape(xs[1], padded[1], LANES),
            shape(xs[2], padded[2], LANES),
            shape(n34, 16, LANES),
        ],
        (idx, *sources, w, sy),
        1,
        [plane(bx), plane(bx), plane(xs[1]), plane(xs[2]), plane(xs[3])]
        + [plane(xs[1]), plane(xs[2]), plane(xs[3]), plane(xs[4])],
        flops=10**9,
    )
    ra = lax.ppermute(ma, "gy", swaps(ny, 1))
    rb = lax.ppermute(mb, "gy", middle_swaps(ny))
    rc = lax.ppermute(mc, "gy", swaps(ny, 2)) if ny == 4 else lax.all_gather(y34, "gy")
    h0, ty0, tyh, *ty = call(
        functools.partial(conv_own_kernel, ny),
        [
            shape(bx, by, bz),
            shape(by, 3 * by, dtype=BF16),
            shape(16, 48, dtype=BF16),
        ]
        + [shape(padded[l], 3 * in_y[l], dtype=BF16) for l in range(1, LEVELS)],
        (taps, idx, g0),
        2,
        flops=10**9,
    )
    n1, strip = REACH + 3, shape(bx, 8, LANES)
    coarse = shape((padded[1] // 8 - 1) * n1 + -(-n1 // 2), 8, LANES)
    h0, ya, yb, ma, mb, mc, h1, h2, h3, h4 = call(
        functools.partial(mid_kernel, nx, ny),
        [shape(bx, by, bz), strip, strip, coarse, coarse, shape(16, 8, LANES)]
        + [shape(xs[l], padded[l], LANES) for l in range(1, LEVELS)],
        (taps, idx, h0, xa, xb, ra, rb, rc, y1, y2, y34, *ty),
        2,
        [pltpu.VMEM((2, REACH, by, bz), F32)],
        flops=10**9,
        aliases={2: 0},
    )
    ra = lax.ppermute(ma, "gx", swaps(nx, 1))
    rb = lax.ppermute(mb, "gx", middle_swaps(nx))
    rc = lax.ppermute(mc, "gx", swaps(nx, 2)) if nx == 4 else lax.all_gather(ma, "gx")
    ya = lax.ppermute(ya, "gy", swaps(ny, 1))
    yb = lax.ppermute(yb, "gy", neighbours(ny))
    f0, f1 = call(
        last_own_kernel,
        [shape(bx, by, bz), shape(xs[1], padded[1], LANES)],
        (taps, h0, h1, ty0),
        1,
        flops=10**9,
    )
    py = jnp.asarray(prolong_rows_const(ny * by, ny))
    pz = jnp.asarray(prolong_lanes_const(nz * bz, nz))
    buf = lambda n, rows: pltpu.VMEM((n, rows, LANES), F32)
    return call(
        functools.partial(last_kernel, nx),
        shape(bx, by, bz),
        (taps, idx, f0, f1, h2, h3, h4, ya, yb, ra, rb, rc, tyh, py, pz),
        2,
        [pltpu.VMEM((2, REACH + 3, padded[1], LANES), F32)]
        + [buf((nx * bx >> l) + 24, padded[l]) for l in range(2, LEVELS)]
        + [buf(xs[l], padded[l]) for l in range(1, LEVELS)]
        + [buf(bx, by), pltpu.SemaphoreType.DMA((4,))]
        + [buf(xs[l + 1], padded[l]) for l in range(LEVELS - 1) for _ in range(2)],
        flops=10**9,
        out_hbm=True,
    )


def solution(mesh):
    in_specs = (P("gx", "gy", "gz"), P())
    out_specs = P("gx", "gy", "gz")
    return jax.shard_map(
        per_device, mesh=mesh, in_specs=in_specs, out_specs=out_specs, check_vma=False
    )
```
